256 devices in a mesh: tile: 32 (over z_lo, y, core), img: 8 (over x, z_hi).
Axes of the slice: x: 4, y: 4, z: 8 (z_hi: 2, z_lo: 4; z = z_hi * 4 + z_lo), core: 2. Of those that a mesh axis runs over, the one named last changes fastest.
Arguments:
- tower: bfloat16 [8, 64, 128, 256], P('img', 'tile'), may hold values from -6 to 6
- cls_weight: bfloat16 [720, 2304], replicated, may hold values from -0.125 to 0.125
- cls_bias: float32 [720], replicated, may hold values from -5.5 to -3.5
- box_weight: bfloat16 [36, 2304], replicated, may hold values from -0.125 to 0.125
- box_bias: float32 [36], replicated, may hold values from -0.5 to 0.5
- labels: int32 [8, 9, 64, 128], P('img', None, 'tile'), may hold values from -2 to 79, as said below
- target_index: int32 [8, 9, 64, 128], P('img', None, 'tile'), may hold values from 0 to 99
- boxes: float32 [8, 4, 100], P('img'), may hold values from -320 to 1344, as said below
Outputs:
- loss: float32 [], replicated
- cls_weight_grad: float32 [720, 2304], replicated
- cls_bias_grad: float32 [720], replicated
- box_weight_grad: float32 [36, 2304], replicated
- box_bias_grad: float32 [36], replicated
- tower_grad: bfloat16 [8, 64, 128, 256], P('img', 'tile')
The draws below stay inside these ranges and needn't reach their ends.
Inputs may be any that keep to these rules, and one draw needn't show every extreme that they name: `labels`: -1 marks background and -2 an ignored anchor, other values are classes; every image has at least one anchor with a class. `boxes`: x1 < x2 and y1 < y2 in every box; sides between 8 and 640 pixels.
All inputs are finite; a program needn't handle non-finite values.
Results may differ from the reference program's by a relative error of at most 0.0053.
Values may be sent and summed in bfloat16 or wider, within the bound.
A program may use at most 64 MiB of HBM per device.

```python
import jax
import jax.numpy as jnp
from jax import lax

CHANNELS = 256
CLASSES = 80
ANCHORS = 9
STRIDE = 8
COLUMNS = 128
MAX_BOXES = 100
ROWS = 64
IMAGES = 8


def draw_labels(key, part):
    dims = (IMAGES, ANCHORS, ROWS, COLUMNS)
    key_pick = jax.random.fold_in(key, 11)
    key_class = jax.random.fold_in(key, 12)
    rolled = jax.random.randint(key_pick, dims, 0, 1000)
    row_ids = lax.broadcasted_iota(jnp.int32, dims, 2)
    col_ids = lax.broadcasted_iota(jnp.int32, dims, 3)
    anchor_ids = lax.broadcasted_iota(jnp.int32, dims, 1)
    positive_limit = 30 + 60 * row_ids // ROWS
    ignore_limit = positive_limit + 50
    classes = jax.random.randint(key_class, dims, 0, CLASSES)
    labels = jnp.where(rolled < positive_limit, classes, jnp.where(rolled < ignore_limit, -2, -1))
    forced = (anchor_ids == 0) & (row_ids == 0) & (col_ids == 0)
    return jnp.where(forced, classes, labels).astype(jnp.int32)


def draw_boxes(key, part):
    dims = (IMAGES, MAX_BOXES)
    centre_x = jax.random.uniform(jax.random.fold_in(key, 21), dims, jnp.float32, 0.0, COLUMNS * STRIDE * 1.0)
    centre_y = jax.random.uniform(jax.random.fold_in(key, 22), dims, jnp.float32, 0.0, ROWS * STRIDE * 1.0)
    widths = jnp.exp(jax.random.uniform(jax.random.fold_in(key, 23), dims, jnp.float32, jnp.log(16.0), jnp.log(512.0)))
    heights = jnp.exp(jax.random.uniform(jax.random.fold_in(key, 24), dims, jnp.float32, jnp.log(16.0), jnp.log(512.0)))
    corners = jnp.stack([centre_x - 0.5 * widths, centre_y - 0.5 * heights, centre_x + 0.5 * widths, centre_y + 0.5 * heights], axis=1)
    return corners.astype(jnp.float32)


def place_ends(result, stream_key, smallest, high):
    place = [jax.random.randint(jax.random.fold_in(stream_key, axis), (), 0, length) for axis, length in enumerate(result.shape)]
    widest = result.shape.index(max(result.shape))
    next_to = place[:widest] + [(place[widest] + 1) % result.shape[widest]] + place[widest + 1:]
    return result.at[tuple(place)].set(smallest).at[tuple(next_to)].set(high)


def levels(rng, shape, shards, smallest, high):
    loudness, own = 1.0, jax.random.fold_in(rng, 6)
    for position, blocks in shards:
        steps = jnp.exp(jax.random.uniform(jax.random.fold_in(own, position), (blocks,), jnp.float32, smallest / len(shards), high / len(shards)))
        loudness = loudness * jnp.repeat(steps, shape[position] // blocks).reshape([-1 if axis == position else 1 for axis in range(len(shape))])
    return loudness


def noise(rng, shape, spread, most, split=(), dtype=jnp.bfloat16):
    loudness = levels(rng, shape, split, -0.22, 0.18) if split else 1.0
    values = jax.random.normal(rng, shape, jnp.float32) * spread * loudness
    return jnp.minimum(jnp.maximum(values, -most), most).astype(dtype)


def setup_inputs(seed: int = 0) -> dict:
    arg_keys = jax.random.split(jax.random.key(seed), 9)
    return {
        "tower": noise(arg_keys[0], (IMAGES, ROWS, COLUMNS, CHANNELS), 1.0, 6.0, ((0, 8), (1, 32))),
        "cls_weight": noise(arg_keys[1], (ANCHORS * CLASSES, 9 * CHANNELS), (9 * CHANNELS) ** -0.5, 0.125),
        "cls_bias": jnp.clip(jax.random.uniform(arg_keys[2], (ANCHORS * CLASSES,), jnp.float32, -5.5, -3.5), -5.5, -3.5),
        "box_weight": noise(arg_keys[3], (ANCHORS * 4, 9 * CHANNELS), (9 * CHANNELS) ** -0.5, 0.125),
        "box_bias": jnp.clip(jax.random.uniform(arg_keys[4], (ANCHORS * 4,), jnp.float32, -0.5, 0.5), -0.5, 0.5),
        "labels": draw_labels(jax.random.fold_in(arg_keys[8], 71), 0),
        "target_index": place_ends(jax.random.randint(arg_keys[6], (IMAGES, ANCHORS, ROWS, COLUMNS), 0, MAX_BOXES), jax.random.fold_in(arg_keys[6], 1), 0, MAX_BOXES - 1).astype(jnp.int32),
        "boxes": draw_boxes(jax.random.fold_in(arg_keys[8], 71), 0),
    }


FOCAL_ALPHA = 0.25
NORM_EPS = 1e-06

def build_patches(extended):
    rows_here = extended.shape[1] - 2
    columns = extended.shape[2]
    padded = jnp.pad(extended, ((0, 0), (0, 0), (1, 1), (0, 0)))
    pieces = []
    for row_tap in range(3):
        for col_tap in range(3):
            pieces.append(padded[:, row_tap:row_tap + rows_here, col_tap:col_tap + columns, :])
    return jnp.concatenate(pieces, axis=3)

def taps_back(dpatch, rows_lo, rows_out):
    images_here, rows_in, columns, width_all = dpatch.shape
    channels = width_all // 9
    pieces = dpatch.reshape(images_here, rows_in, columns, 9, channels)
    accumulated = jnp.zeros((images_here, rows_in + 2, columns + 2, channels), jnp.float32)
    for row_tap in range(3):
        for col_tap in range(3):
            accumulated = accumulated.at[:, row_tap:row_tap + rows_in, col_tap:col_tap + columns, :].add(pieces[:, :, :, row_tap * 3 + col_tap, :])
    return accumulated[:, rows_lo:rows_lo + rows_out, 1:columns + 1, :]

def head_terms(logits, deltas, labels, target_index, boxes, first_row):
    images_here = labels.shape[0]
    rows_here = labels.shape[2]
    columns = labels.shape[3]
    scores = logits.reshape(ANCHORS, CLASSES, images_here, rows_here, columns)
    assigned = jnp.transpose(labels, (1, 0, 2, 3))
    classes = lax.broadcasted_iota(jnp.int32, (1, CLASSES, 1, 1, 1), 1)
    target = (assigned[:, None] == classes).astype(jnp.float32)
    counted = (assigned >= -1).astype(jnp.float32)[:, None]
    probability = jax.nn.sigmoid(scores)
    hit_term = -FOCAL_ALPHA * (1.0 - probability) * (1.0 - probability) * jax.nn.log_sigmoid(scores)
    miss_term = -(1.0 - FOCAL_ALPHA) * probability * probability * jax.nn.log_sigmoid(-scores)
    focal_sum = jnp.sum(counted * (target * hit_term + (1.0 - target) * miss_term))
    offsets = deltas.reshape(ANCHORS, 4, images_here, rows_here, columns)
    anchor_ids = lax.broadcasted_iota(jnp.int32, (ANCHORS, 1, 1, 1), 0)
    scale_step = (anchor_ids // 3).astype(jnp.float32)
    ratio_step = (anchor_ids % 3 - 1).astype(jnp.float32)
    anchor_base = 4.0 * STRIDE * jnp.exp2(scale_step / 3.0)
    anchor_w = anchor_base * jnp.exp2(-ratio_step / 2.0)
    anchor_h = anchor_base * jnp.exp2(ratio_step / 2.0)
    row_ids = first_row + lax.broadcasted_iota(jnp.int32, (1, 1, rows_here, 1), 2)
    col_ids = lax.broadcasted_iota(jnp.int32, (1, 1, 1, columns), 3)
    centre_y = (row_ids.astype(jnp.float32) + 0.5) * STRIDE
    centre_x = (col_ids.astype(jnp.float32) + 0.5) * STRIDE
    middle_x = centre_x + offsets[:, 0] * anchor_w
    middle_y = centre_y + offsets[:, 1] * anchor_h
    pred_width = anchor_w * jnp.exp(offsets[:, 2])
    pred_height = anchor_h * jnp.exp(offsets[:, 3])
    pred_left = middle_x - 0.5 * pred_width
    pred_right = middle_x + 0.5 * pred_width
    pred_top = middle_y - 0.5 * pred_height
    pred_bottom = middle_y + 0.5 * pred_height
    flat_index = target_index.reshape(images_here, -1)
    picked = jnp.take_along_axis(boxes, jnp.broadcast_to(flat_index[:, None, :], (images_here, 4, flat_index.shape[1])), axis=2)
    picked = jnp.transpose(picked.reshape(images_here, 4, ANCHORS, rows_here, columns), (1, 2, 0, 3, 4))
    true_left, true_top, true_right, true_bottom = (picked[0], picked[1], picked[2], picked[3])
    crossing_w = jnp.maximum(jnp.minimum(pred_right, true_right) - jnp.maximum(pred_left, true_left), 0.0)
    crossing_h = jnp.maximum(jnp.minimum(pred_bottom, true_bottom) - jnp.maximum(pred_top, true_top), 0.0)
    crossing = crossing_w * crossing_h
    union_area = pred_width * pred_height + (true_right - true_left) * (true_bottom - true_top) - crossing
    outer_w = jnp.maximum(pred_right, true_right) - jnp.minimum(pred_left, true_left)
    outer_h = jnp.maximum(pred_bottom, true_bottom) - jnp.minimum(pred_top, true_top)
    outer_area = outer_w * outer_h
    giou_value = crossing / union_area - (outer_area - union_area) / outer_area
    positive = (assigned >= 0).astype(jnp.float32)
    giou_sum = jnp.sum(positive * (1.0 - giou_value))
    return (focal_sum, giou_sum)

def reference(tower, cls_weight, cls_bias, box_weight, box_bias, labels, target_index, boxes):
    weight_all = jnp.concatenate([cls_weight, box_weight], axis=0)
    bias_all = jnp.concatenate([cls_bias, box_bias])
    split_at = cls_weight.shape[0]

    def one_image(carry, inputs):
        weight_sum, bias_sum, focal_total, giou_total, positives = carry
        image, image_labels, image_index, image_boxes = inputs
        extended = jnp.pad(image[None], ((0, 0), (1, 1), (0, 0), (0, 0)))
        patches = build_patches(extended)
        flat_patches = patches.reshape(-1, patches.shape[3])
        outputs = lax.dot_general(weight_all, flat_patches, (((1,), (1,)), ((), ())), preferred_element_type=jnp.float32)
        outputs = (outputs + bias_all[:, None]).reshape(weight_all.shape[0], 1, ROWS, COLUMNS)

        def loss_pair(scores, offsets):
            return head_terms(scores, offsets, image_labels[None], image_index[None], image_boxes[None], 0)
        loss_terms, pullback = jax.vjp(loss_pair, outputs[:split_at], outputs[split_at:])
        grad_scores, grad_offsets = pullback((jnp.ones((), jnp.float32), jnp.ones((), jnp.float32)))
        grad_out = jnp.concatenate([grad_scores, grad_offsets], axis=0)
        grad_low = grad_out.astype(jnp.bfloat16)
        grad_flat = grad_low.reshape(grad_low.shape[0], -1)
        weight_sum = weight_sum + jnp.dot(grad_flat, flat_patches, preferred_element_type=jnp.float32)
        bias_sum = bias_sum + lax.optimization_barrier(jnp.sum(grad_out, axis=(1, 2, 3)))
        dpatch = lax.dot_general(grad_flat, weight_all, (((0,), (0,)), ((), ())), preferred_element_type=jnp.float32)
        dpatch = dpatch.reshape(1, ROWS, COLUMNS, weight_all.shape[1])
        image_grad = taps_back(dpatch, 1, ROWS)[0].astype(jnp.bfloat16)
        positives = positives + jnp.sum((image_labels >= 0).astype(jnp.float32))
        focal_total = focal_total + loss_terms[0]
        giou_total = giou_total + loss_terms[1]
        return ((weight_sum, bias_sum, focal_total, giou_total, positives), image_grad)
    initial = (jnp.zeros(weight_all.shape, jnp.float32), jnp.zeros(bias_all.shape, jnp.float32), jnp.zeros((), jnp.float32), jnp.zeros((), jnp.float32), jnp.zeros((), jnp.float32))
    finals, tower_grad = lax.scan(one_image, initial, (tower, labels, target_index, boxes))
    weight_sum, bias_sum, focal_total, giou_total, positives = finals
    loss = (focal_total + giou_total) / positives
    entries = weight_all.shape[0] * (weight_all.shape[1] + 1)
    squares = jnp.sum(weight_sum * weight_sum) + jnp.sum(bias_sum * bias_sum)
    scale = lax.rsqrt(squares / entries + NORM_EPS)
    weight_norm = weight_sum * scale
    bias_norm = bias_sum * scale
    return (loss, weight_norm[:split_at], bias_norm[:split_at], weight_norm[split_at:], bias_norm[split_at:], tower_grad)
```

```python
import functools

import jax
import jax.numpy as jnp
import numpy as np
from jax import lax
from jax.experimental import pallas as pl
from jax.experimental.pallas import tpu as pltpu
from jax.sharding import PartitionSpec as P

CLASSES = 80
ANCHORS = 9
STRIDE = 8
FOCAL_ALPHA = 0.25
NORM_EPS = 1e-06

RING = 4
CLS = ANCHORS * CLASSES
OUTS = CLS + 4 * ANCHORS
PAD_OUTS = 768
TAPS = 9
DEPTH = 256
WIDTH = TAPS * DEPTH
HALF = WIDTH // 2
COLS = 128
BLOCK = PAD_OUTS // (RING * RING)
SPLIT = 640
BF16 = jnp.bfloat16
F32 = jnp.float32
MESH = pl.DeviceIdType.MESH


def flip(i):
    return i + 1 - 2 * (i % 2)


class Links:
    def __init__(self, send, recv):
        self.send, self.recv, self.used, self.sent = send, recv, 0, []

    def make(self, src, dst, device):
        i = self.used
        self.used += 1
        return pltpu.make_async_remote_copy(
            src_ref=src,
            dst_ref=dst,
            send_sem=self.send.at[i],
            recv_sem=self.recv.at[i],
            device_id=device,
            device_id_type=MESH,
        )

    def push(self, src, dst, device):
        copy = self.make(src, dst, device)
        copy.start()
        self.sent.append(copy)
        return copy

    def drain(self):
        for copy in self.sent:
            copy.wait_send()


def anchor_sizes():
    ids = np.arange(ANCHORS)
    base = np.float32(4.0 * STRIDE) * np.exp2((ids // 3).astype(np.float32) / np.float32(3.0))
    ratio = (ids % 3 - 1).astype(np.float32) / np.float32(2.0)
    return (base * np.exp2(-ratio)).astype(np.float32), (base * np.exp2(ratio)).astype(np.float32)


def box_terms(offsets, assigned, corners, first_row):
    shape = assigned.shape
    ids = lax.broadcasted_iota(jnp.int32, shape, 0)
    lanes = lax.broadcasted_iota(jnp.int32, shape, 1)
    widths, heights = anchor_sizes()
    anchor_w = jnp.zeros(shape, F32)
    anchor_h = jnp.zeros(shape, F32)
    for a in range(ANCHORS):
        anchor_w = jnp.where(ids == a, float(widths[a]), anchor_w)
        anchor_h = jnp.where(ids == a, float(heights[a]), anchor_h)
    second = (lanes >= COLS).astype(jnp.int32)
    centre_y = ((first_row + second).astype(F32) + 0.5) * STRIDE
    centre_x = ((lanes - COLS * second).astype(F32) + 0.5) * STRIDE
    true_left, true_top, true_right, true_bottom = corners
    positive = (assigned >= 0).astype(F32)

    def each(o0, o1, o2, o3):
        middle_x = centre_x + o0 * anchor_w
        middle_y = centre_y + o1 * anchor_h
        pred_width = anchor_w * jnp.exp(o2)
        pred_height = anchor_h * jnp.exp(o3)
        pred_left = middle_x - 0.5 * pred_width
        pred_right = middle_x + 0.5 * pred_width
        pred_top = middle_y - 0.5 * pred_height
        pred_bottom = middle_y + 0.5 * pred_height
        crossing_w = jnp.maximum(
            jnp.minimum(pred_right, true_right) - jnp.maximum(pred_left, true_left), 0.0
        )
        crossing_h = jnp.maximum(
            jnp.minimum(pred_bottom, true_bottom) - jnp.maximum(pred_top, true_top), 0.0
        )
        crossing = crossing_w * crossing_h
        union_area = (
            pred_width * pred_height
            + (true_right - true_left) * (true_bottom - true_top)
            - crossing
        )
        outer_w = jnp.maximum(pred_right, true_right) - jnp.minimum(pred_left, true_left)
        outer_h = jnp.maximum(pred_bottom, true_bottom) - jnp.minimum(pred_top, true_top)
        outer_area = outer_w * outer_h
        giou_value = crossing / union_area - (outer_area - union_area) / outer_area
        return positive * (1.0 - giou_value)

    values, pullback = jax.vjp(each, *offsets)
    return values, pullback(jnp.ones(shape, F32)), positive


def shifted(value, tap):
    if tap == 1:
        return value
    rows = lax.broadcasted_iota(jnp.int32, value.shape, 0)
    if tap == 0:
        return jnp.where(rows == 0, 0.0, pltpu.roll(value, 1, 0))
    return jnp.where(rows == COLS - 1, 0.0, pltpu.roll(value, COLS - 1, 0))


def step_kernel(
    zl_count, zh_count,
    tower, wc_hbm, wb, bias, labels, tindex, boxes,
    r_out, s_out, tg_out,
    w, wbs, patches, halo, outs, gf, glow, boxy, acc, send_c, recv_c,
    a1s, a1r, a2s, a2r, accb, b1s0, b1r0, b2s0, b2r0, b1s1, b1r1, b2s1, b2r1,
    zf, zs, zr, zg, sc, sx, sy, sz, dpatch, edge_s, edge_r,
    wsem, send, recv,
):
    t = lax.axis_index("tile")
    m = lax.axis_index("img")
    tiles = zl_count * RING * 2
    nz = zl_count * zh_count
    c = t % 2
    y = (t // 2) % RING
    x = m // zh_count
    z = (m % zh_count) * zl_count + t // (2 * RING)

    def at(x_, y_, z_, c_):
        return {
            "tile": (z_ % zl_count) * (2 * RING) + y_ * 2 + c_,
            "img": x_ * zh_count + z_ // zl_count,
        }

    a = x + c * (y - x)
    b = y + c * (x - y)

    def ring(a_, b_):
        return at(a_ + c * (b_ - a_), b_ + c * (a_ - b_), z, c)

    sibling = at(x, y, z, 1 - c)
    above = {"tile": t - 1, "img": m}
    below = {"tile": t + 1, "img": m}
    links = Links(send, recv)

    load = pltpu.make_async_copy(wc_hbm, w, wsem)
    load.start()

    barrier = pltpu.get_barrier_semaphore()

    def greet(device):
        pl.semaphore_signal(barrier, inc=1, device_id=device, device_id_type=MESH)

    greet(sibling)
    for k in range(1, RING):
        greet(at((x + k) % RING, y, z, c))
        greet(at(x, (y + k) % RING, z, c))
    for k in range(1, nz):
        greet(at(x, y, (z + k) % nz, c))

    @pl.when(t > 0)
    def _():
        greet(above)

    @pl.when(t < tiles - 1)
    def _():
        greet(below)

    wanted = jnp.concatenate([tindex[0, :, 0, :], tindex[0, :, 1, :]], axis=1)

    def pick(n, found):
        hit = wanted == n
        return tuple(jnp.where(hit, boxes[0, j, n], found[j]) for j in range(4))

    zero = jnp.zeros(wanted.shape, F32)
    corners = lax.fori_loop(0, boxes.shape[2], pick, (zero, zero, zero, zero))
    wbs[...] = jnp.zeros(wbs.shape, BF16)
    wbs[0 : 4 * ANCHORS, :] = wb[...]

    def fill(row, ext):
        value = row.astype(F32)
        for col_tap in range(3):
            piece = shifted(value, col_tap).astype(BF16)
            for here in range(2):
                row_tap = ext - here
                if 0 <= row_tap <= 2:
                    for part in range(2):
                        k = (3 * row_tap + col_tap) * DEPTH + part * COLS
                        patches[k // HALF, here * COLS : (here + 1) * COLS,
                                k % HALF : k % HALF + COLS] = piece[:, part * COLS : (part + 1) * COLS]

    fill(tower[0, 0], 1)
    fill(tower[0, 1], 2)

    greeted = 1 + 2 * (RING - 1) + nz - 1
    pl.semaphore_wait(
        barrier, greeted + (t > 0).astype(jnp.int32) + (t < tiles - 1).astype(jnp.int32)
    )

    halo_up = links.make(tower.at[0, 0], halo.at[1], above)
    halo_down = links.make(tower.at[0, 1], halo.at[0], below)

    @pl.when(t > 0)
    def _():
        halo_up.start()

    @pl.when(t < tiles - 1)
    def _():
        halo_down.start()

    @pl.when(t == 0)
    def _():
        halo[0] = jnp.zeros(halo.shape[1:], BF16)

    @pl.when(t == tiles - 1)
    def _():
        halo[1] = jnp.zeros(halo.shape[1:], BF16)

    load.wait()

    @pl.when(t < tiles - 1)
    def _():
        halo_up.wait_recv()

    @pl.when(t > 0)
    def _():
        halo_down.wait_recv()

    fill(halo[0], 0)
    fill(halo[1], 3)

    nt = (((1,), (1,)), ((), ()))

    def product(lhs, rhs):
        return lax.dot_general(lhs, rhs, nt, preferred_element_type=F32)

    bias_col = jnp.transpose(jnp.broadcast_to(bias[...], (8, PAD_OUTS)))[:, 0:1]
    outs[0:CLS, :] = (
        product(w[:, 0:HALF], patches[0]) + product(w[:, HALF:WIDTH], patches[1]) + bias_col[0:CLS]
    )
    outs[CLS:PAD_OUTS, :] = (
        product(wbs[:, 0:HALF], patches[0])
        + product(wbs[:, HALF:WIDTH], patches[1])
        + bias_col[CLS:PAD_OUTS]
    )

    class_ids = lax.broadcasted_iota(jnp.int32, (CLASSES, COLS), 0)

    def focal(anchor, total):
        rows = pl.ds(pl.multiple_of(anchor * CLASSES, CLASSES), CLASSES)
        for here in range(2):
            lanes = slice(here * COLS, (here + 1) * COLS)
            score = outs[rows, lanes]
            label = labels[0, anchor, here : here + 1, :]
            hit = jnp.broadcast_to(label, (CLASSES, COLS)) == class_ids
            counted = (label >= -1).astype(F32)
            side = jnp.where(hit, score, -score)
            small = jnp.exp(-jnp.abs(score))
            inverse = 1.0 / (1.0 + small)
            log_p = jnp.minimum(side, 0.0) - jnp.log1p(small)
            right = side >= 0
            p = jnp.where(right, inverse, small * inverse)
            miss = jnp.where(right, small * inverse, inverse)
            alpha = jnp.where(hit, FOCAL_ALPHA, FOCAL_ALPHA - 1.0) * counted
            weight = alpha * miss * miss
            grad = weight * (2.0 * p * log_p - miss)
            value = -jnp.abs(weight) * log_p
            gf[rows, lanes] = grad
            glow[rows, lanes] = grad.astype(BF16)
            total = total + jnp.sum(value.reshape(CLASSES // 8, 8, COLS), axis=0)
        return total

    focal_sum = lax.fori_loop(0, ANCHORS, focal, jnp.zeros((8, COLS), F32))

    assigned = jnp.concatenate([labels[0, :, 0, :], labels[0, :, 1, :]], axis=1)
    for here in range(2):
        boxy[here] = outs[CLS:PAD_OUTS, here * COLS : (here + 1) * COLS]
    offsets = [
        jnp.concatenate([boxy[here, pl.ds(j, ANCHORS, stride=4), :] for here in range(2)], axis=1)
        for j in range(4)
    ]
    giou, offset_grads, positive = box_terms(offsets, assigned, corners, 2 * t)
    boxy[...] = jnp.zeros(boxy.shape, F32)
    for here in range(2):
        lanes = slice(here * COLS, (here + 1) * COLS)
        for j in range(4):
            boxy[here, pl.ds(j, ANCHORS, stride=4), :] = offset_grads[j][:, lanes]
        gf[CLS:PAD_OUTS, lanes] = boxy[here]
    glow[CLS:PAD_OUTS, :] = gf[CLS:PAD_OUTS, :].astype(BF16)

    send_to_core = []
    for k in range(RING):
        rows = slice(k * RING * BLOCK, (k + 1) * RING * BLOCK)
        part = jnp.dot(glow[rows, :], patches[1 - c], preferred_element_type=F32)
        send_c[k] = part.astype(BF16).reshape(RING, BLOCK, HALF)
        send_to_core.append(links.push(send_c.at[k], recv_c.at[k], sibling))

    sums = lax.dot_general(
        jnp.ones((8, 2 * COLS), F32), gf[...], nt,
        precision=lax.Precision.HIGHEST, preferred_element_type=F32,
    )
    lane = lax.broadcasted_iota(jnp.int32, (1, COLS), 1)
    mine = jnp.zeros((8, COLS), F32)
    rows8 = lax.broadcasted_iota(jnp.int32, (8, COLS), 0)
    for k in range(PAD_OUTS // COLS):
        mine = jnp.where(rows8 == k, sums[:, k * COLS : (k + 1) * COLS], mine)
    scalars = (jnp.sum(focal_sum), jnp.sum(giou), jnp.sum(positive))
    for k, value in enumerate(scalars):
        mine = jnp.where((rows8 == 6) & (lane == k), value, mine)
    sc[c] = mine
    small_c = links.push(sc.at[c], sc.at[c], sibling)

    def own(k, carry):
        rows = pl.ds(pl.multiple_of(k * RING * BLOCK, RING * BLOCK), RING * BLOCK)
        part = jnp.dot(glow[rows, :], patches[c], preferred_element_type=F32)
        acc[k] = part.reshape(RING, BLOCK, HALF)
        return carry

    lax.fori_loop(0, RING, own, 0)

    small_c.wait_recv()
    sx[x] = sc[0] + sc[1]
    small_x = [
        links.push(sx.at[x], sx.at[x], at((x + k) % RING, y, z, c)) for k in range(1, RING)
    ]
    for copy in send_to_core:
        copy.wait_recv()

    def pair(quarter, j):
        return acc[quarter, j] + recv_c[quarter, j].astype(F32)

    steps_a = ((flip(a), 3 - a), (3 - a, flip(a)))
    first = {}
    for which in (1, 0):
        for s in range(2):
            near, far = steps_a[s]
            back = (3 - near, flip(near))[s]
            quarter = back if which else near
            for j in range(2):
                a1s[s, which, j] = pair(quarter, 2 * s + j).astype(BF16)
            first[s, which] = links.push(a1s.at[s, which], a1r.at[s, which], ring(near, b))

    tn = (((0,), (0,)), ((), ()))
    dpatch[...] = lax.dot_general(
        glow[0:CLS, :], w[...], tn, preferred_element_type=F32
    ) + lax.dot_general(glow[CLS:PAD_OUTS, :], wbs[...], tn, preferred_element_type=F32)

    def reach(row_tap, here):
        total = None
        for col_tap in range(3):
            k = (3 * row_tap + col_tap) * DEPTH
            piece = shifted(dpatch[here * COLS : (here + 1) * COLS, k : k + DEPTH], 2 - col_tap)
            total = piece if total is None else total + piece
        return total

    edge_s[0] = reach(0, 0)
    edge_s[1] = reach(2, 1)
    edge_up = links.make(edge_s.at[0], edge_r.at[1], above)
    edge_down = links.make(edge_s.at[1], edge_r.at[0], below)

    @pl.when(t > 0)
    def _():
        edge_up.start()

    @pl.when(t < tiles - 1)
    def _():
        edge_down.start()

    @pl.when(t == 0)
    def _():
        edge_r[0] = jnp.zeros(edge_r.shape[1:], F32)

    @pl.when(t == tiles - 1)
    def _():
        edge_r[1] = jnp.zeros(edge_r.shape[1:], F32)

    second = []
    for s in range(2):
        near, far = steps_a[s]
        first[s, 1].wait_recv()
        for j in range(2):
            a2s[s, j] = (pair(far, 2 * s + j) + a1r[s, 1, j].astype(F32)).astype(BF16)
        second.append(links.push(a2s.at[s], a2r.at[s], ring(far, b)))

    for copy in small_x:
        copy.wait_recv()
    sy[y] = (sx[0] + sx[1]) + (sx[2] + sx[3])
    small_y = [
        links.push(sy.at[y], sy.at[y], at(x, (y + k) % RING, z, c)) for k in range(1, RING)
    ]

    tg_own = (reach(1, 0) + reach(0, 1), reach(2, 0) + reach(1, 1))

    @pl.when(t < tiles - 1)
    def _():
        edge_up.wait_recv()

    @pl.when(t > 0)
    def _():
        edge_down.wait_recv()

    for here in range(2):
        tg_out[0, here] = (tg_own[here] + edge_r[here]).astype(BF16)

    for s in range(2):
        first[s, 0].wait_recv()
        second[s].wait_recv()
        for j in range(2):
            accb[2 * s + j] = (
                pair(a, 2 * s + j) + a1r[s, 0, j].astype(F32) + a2r[s, j].astype(F32)
            )

    steps_b = ((flip(b), 3 - b), (3 - b, flip(b)))
    bufs = ((b1s0, b1r0, b2s0, b2r0, slice(0, SPLIT)), (b1s1, b1r1, b2s1, b2r1, slice(SPLIT, HALF)))
    first = {}
    for which in (1, 0):
        for s in range(2):
            near, far = steps_b[s]
            back = (3 - near, flip(near))[s]
            quarter = back if which else near
            s1, r1, s2, r2, cols = bufs[s]
            s1[which] = accb[quarter, :, cols].astype(BF16)
            first[s, which] = links.push(s1.at[which], r1.at[which], ring(a, near))
    second = []
    for s in range(2):
        near, far = steps_b[s]
        s1, r1, s2, r2, cols = bufs[s]
        first[s, 1].wait_recv()
        s2[...] = (accb[far, :, cols] + r1[1].astype(F32)).astype(BF16)
        second.append(links.push(s2, r2, ring(a, far)))
    for copy in small_y:
        copy.wait_recv()
    sz[z] = (sy[0] + sy[1]) + (sy[2] + sy[3])
    small_z = [
        links.push(sz.at[z], sz.at[z], at(x, y, (z + k) % nz, c)) for k in range(1, nz)
    ]
    per = zf.shape[1] // 8
    groups = BLOCK // 8
    zf[...] = jnp.zeros(zf.shape, F32)
    for s in range(2):
        s1, r1, s2, r2, cols = bufs[s]
        first[s, 0].wait_recv()
        second[s].wait_recv()
        done = accb[b, :, cols] + r1[0].astype(F32) + r2[...].astype(F32)
        for k in range(cols.start // COLS, cols.stop // COLS):
            at_col = k * COLS - cols.start
            for g in range(groups):
                n = k * groups + g
                zf[n // per, (n % per) * 8 : (n % per) * 8 + 8, :] = done[
                    g * 8 : g * 8 + 8, at_col : at_col + COLS
                ]

    zs[...] = zf[...].astype(BF16)
    turns = [
        links.push(zs.at[(z + k) % nz], zr.at[z], at(x, y, (z + k) % nz, c)) for k in range(1, nz)
    ]
    total = zf[z]
    for k in range(1, nz):
        turns[k - 1].wait_recv()
        total = total + zr[(z + nz - k) % nz].astype(F32)
    zg[z] = total.astype(BF16)
    turns = [
        links.push(zg.at[z], zg.at[z], at(x, y, (z + k) % nz, c)) for k in range(1, nz)
    ]
    for copy in turns:
        copy.wait_recv()
    zf[...] = zg[...].astype(F32)
    for k in range(HALF // COLS):
        pieces = []
        for g in range(groups):
            n = k * groups + g
            pieces.append(zf[n // per, (n % per) * 8 : (n % per) * 8 + 8, :])
        r_out[c, a, b, :, k * COLS : (k + 1) * COLS] = jnp.concatenate(pieces, axis=0).astype(BF16)

    def wrap(i):
        return (i + RING) % RING

    top, bottom = slice(0, 32), slice(32, BLOCK)
    shared = []

    def share(a_, b_):
        shared.append(links.push(r_out.at[c, a_, b_], r_out.at[c, a_, b_], sibling))

    def along_a(b_):
        block = r_out.at[c, a, b_]
        return (
            links.push(block, block, ring(wrap(a + 1), b)),
            links.push(block, block, ring(wrap(a - 1), b)),
        )

    block = r_out.at[c, a, b]
    to_next = links.push(block, block, ring(a, wrap(b + 1)))
    to_last = links.push(block, block, ring(a, wrap(b - 1)))
    wide = [along_a(b)]
    share(a, b)
    to_next.wait_recv()
    block = r_out.at[c, a, wrap(b - 1), top]
    on_next = links.push(block, block, ring(a, wrap(b + 1)))
    wide.append(along_a(wrap(b - 1)))
    share(a, wrap(b - 1))
    to_last.wait_recv()
    block = r_out.at[c, a, wrap(b + 1), bottom]
    on_last = links.push(block, block, ring(a, wrap(b - 1)))
    wide.append(along_a(wrap(b + 1)))
    share(a, wrap(b + 1))
    on_next.wait_recv()
    on_last.wait_recv()
    wide.append(along_a(wrap(b + 2)))
    share(a, wrap(b + 2))

    order = (b, wrap(b - 1), wrap(b + 1), wrap(b + 2))
    rest = []
    for k, b_ in enumerate(order):
        wide[k][0].wait_recv()
        if k < 2:
            block = r_out.at[c, wrap(a - 1), b_]
            rest.append(links.push(block, block, ring(wrap(a + 1), b)))
        share(wrap(a - 1), b_)
        wide[k][1].wait_recv()
        if k >= 2:
            block = r_out.at[c, wrap(a + 1), b_]
            rest.append(links.push(block, block, ring(wrap(a - 1), b)))
        share(wrap(a + 1), b_)
    for k, b_ in enumerate(order):
        rest[k].wait_recv()
        share(wrap(a + 2), b_)

    for copy in small_z:
        copy.wait_recv()
    whole = sz[0]
    for k in range(1, nz):
        whole = whole + sz[k]
    s_out[...] = whole

    for copy in shared:
        copy.wait_recv()
    links.drain()

    @pl.when(t > 0)
    def _():
        halo_up.wait_send()
        edge_up.wait_send()

    @pl.when(t < tiles - 1)
    def _():
        halo_down.wait_send()
        edge_down.wait_send()


def scale_kernel(r, s, cls_out, box_out, bias_out, stage, sem):
    def squares(k, total):
        for h in range(2):
            value = r[h, k // RING, k % RING].astype(F32)
            value = value * value
            value = jnp.sum(value.reshape(BLOCK // 8, 8, HALF), axis=0)
            for j in range(HALF // COLS):
                total = total + value[:, j * COLS : (j + 1) * COLS]
        return total

    total = lax.fori_loop(0, RING * RING, squares, jnp.zeros((8, COLS), F32))
    rows8 = lax.broadcasted_iota(jnp.int32, (8, COLS), 0)
    bias = jnp.where(rows8 < PAD_OUTS // COLS, s[...], 0.0)
    total = jnp.sum(total + bias * bias, keepdims=True)
    scale = lax.rsqrt(total / (OUTS * (WIDTH + 1)) + NORM_EPS)
    bias_out[...] = bias * scale

    slots = stage.shape[0]
    count = CLS // BLOCK

    def store(k):
        return pltpu.make_async_copy(
            stage.at[k % slots],
            cls_out.at[pl.ds(pl.multiple_of(k * BLOCK, BLOCK), BLOCK)],
            sem.at[k % slots],
        )

    def chunk(k, carry):
        @pl.when(k >= slots)
        def _():
            store(k - slots).wait()

        for h in range(2):
            stage[k % slots, :, h * HALF : (h + 1) * HALF] = (
                r[h, k // RING, k % RING].astype(F32) * scale
            )
        store(k).start()
        return carry

    lax.fori_loop(0, count, chunk, 0)
    for h in range(2):
        box_out[:, h * HALF : (h + 1) * HALF] = (
            r[h, RING - 1, RING - 1].astype(F32) * scale
        )[0 : 4 * ANCHORS]
    for k in range(count - slots, count):
        store(k).wait()


def per_device(
    zl_count, zh_count, tower, cls_weight, cls_bias, box_weight, box_bias, labels, target_index, boxes
):
    nz = zl_count * zh_count
    tiles8 = BLOCK // 8 * (HALF // COLS)
    per = -(-tiles8 // nz) * 8
    bias = jnp.concatenate([cls_bias, box_bias, jnp.zeros((PAD_OUTS - OUTS,), F32)])[None]
    vmem = pl.BlockSpec(memory_space=pltpu.VMEM)
    copies = 100 + 4 * nz

    def buf(*shape, dtype=BF16):
        return pltpu.VMEM(shape, dtype)

    r, s, tower_grad = pl.pallas_call(
        functools.partial(step_kernel, zl_count, zh_count),
        out_shape=(
            jax.ShapeDtypeStruct((2, RING, RING, BLOCK, HALF), BF16),
            jax.ShapeDtypeStruct((8, COLS), F32),
            jax.ShapeDtypeStruct(tower.shape, BF16),
        ),
        in_specs=[
            vmem,
            pl.BlockSpec(memory_space=pl.ANY),
            vmem, vmem, vmem, vmem,
            pl.BlockSpec(memory_space=pltpu.SMEM),
        ],
        out_specs=(vmem, vmem, vmem),
        scratch_shapes=[
            buf(CLS, WIDTH),
            buf(PAD_OUTS - CLS, WIDTH),
            buf(2, 2 * COLS, HALF),
            buf(2, COLS, DEPTH),
            buf(PAD_OUTS, 2 * COLS, dtype=F32),
            buf(PAD_OUTS, 2 * COLS, dtype=F32),
            buf(PAD_OUTS, 2 * COLS),
            buf(2, PAD_OUTS - CLS, COLS, dtype=F32),
            buf(RING, RING, BLOCK, HALF, dtype=F32),
            buf(RING, RING, BLOCK, HALF),
            buf(RING, RING, BLOCK, HALF),
            buf(2, 2, 2, BLOCK, HALF),
            buf(2, 2, 2, BLOCK, HALF),
            buf(2, 2, BLOCK, HALF),
            buf(2, 2, BLOCK, HALF),
            buf(RING, BLOCK, HALF, dtype=F32),
            buf(2, BLOCK, SPLIT),
            buf(2, BLOCK, SPLIT),
            buf(BLOCK, SPLIT),
            buf(BLOCK, SPLIT),
            buf(2, BLOCK, HALF - SPLIT),
            buf(2, BLOCK, HALF - SPLIT),
            buf(BLOCK, HALF - SPLIT),
            buf(BLOCK, HALF - SPLIT),
            buf(nz, per, COLS, dtype=F32),
            buf(nz, per, COLS),
            buf(nz, per, COLS),
            buf(nz, per, COLS),
            buf(2, 8, COLS, dtype=F32),
            buf(RING, 8, COLS, dtype=F32),
            buf(RING, 8, COLS, dtype=F32),
            buf(nz, 8, COLS, dtype=F32),
            buf(2 * COLS, WIDTH, dtype=F32),
            buf(2, COLS, DEPTH, dtype=F32),
            buf(2, COLS, DEPTH, dtype=F32),
            pltpu.SemaphoreType.DMA,
            pltpu.SemaphoreType.DMA((copies,)),
            pltpu.SemaphoreType.DMA((copies,)),
        ],
        compiler_params=pltpu.CompilerParams(
            collective_id=0, has_side_effects=True, vmem_limit_bytes=56 * 2**20
        ),
        name="step",
    )(tower, cls_weight, box_weight, bias, labels, target_index, boxes)

    cls_grad, box_grad, bias_grad = pl.pallas_call(
        scale_kernel,
        out_shape=(
            jax.ShapeDtypeStruct((CLS, WIDTH), F32),
            jax.ShapeDtypeStruct((4 * ANCHORS, WIDTH), F32),
            jax.ShapeDtypeStruct((8, COLS), F32),
        ),
        in_specs=[vmem, vmem],
        out_specs=(pl.BlockSpec(memory_space=pl.ANY), vmem, vmem),
        scratch_shapes=[
            buf(4, BLOCK, WIDTH, dtype=F32),
            pltpu.SemaphoreType.DMA((4,)),
        ],
        compiler_params=pltpu.CompilerParams(vmem_limit_bytes=40 * 2**20),
        name="scale",
    )(r, s)
    flat = bias_grad.reshape(-1)
    loss = (s[6, 0] + s[6, 1]) / s[6, 2]
    return loss, cls_grad, flat[:CLS], box_grad, flat[CLS:OUTS], tower_grad


def solution(mesh):
    zl_count = mesh.shape["tile"] // (2 * RING)
    zh_count = mesh.shape["img"] // RING
    placed = (
        P("img", "tile", None, None),
        P(),
        P(),
        P(),
        P(),
        P("img", None, "tile", None),
        P("img", None, "tile", None),
        P("img", None, None),
    )
    return jax.shard_map(
        functools.partial(per_device, zl_count, zh_count),
        mesh=mesh,
        in_specs=placed,
        out_specs=(P(), P(), P(), P(), P(), P("img", "tile", None, None)),
        check_vma=False,
    )
```

```python
import functools

import jax
import jax.numpy as jnp
import numpy as np
from jax import lax
from jax.experimental import pallas as pl
from jax.experimental.pallas import tpu as pltpu
from jax.sharding import PartitionSpec as P

CLASSES = 80
ANCHORS = 9
STRIDE = 8
FOCAL_ALPHA = 0.25
NORM_EPS = 1e-06

RING = 4
CLS = ANCHORS * CLASSES
OUTS = CLS + 4 * ANCHORS
PAD_OUTS = 768
TAPS = 9
DEPTH = 256
WIDTH = TAPS * DEPTH
HALF = WIDTH // 2
COLS = 128
BLOCK = PAD_OUTS // (RING * RING)
SPLIT = 640
BF16 = jnp.bfloat16
F32 = jnp.float32
MESH = pl.DeviceIdType.MESH


def flip(i):
    return i + 1 - 2 * (i % 2)


class Links:
    def __init__(self, send, recv):
        self.send, self.recv, self.used, self.sent = send, recv, 0, []

    def make(self, src, dst, device):
        i = self.used
        self.used += 1
        return pltpu.make_async_remote_copy(
            src_ref=src,
            dst_ref=dst,
            send_sem=self.send.at[i],
            recv_sem=self.recv.at[i],
            device_id=device,
            device_id_type=MESH,
        )

    def push(self, src, dst, device):
        copy = self.make(src, dst, device)
        copy.start()
        self.sent.append(copy)
        return copy

    def drain(self):
        for copy in self.sent:
            copy.wait_send()


def anchor_sizes():
    ids = np.arange(ANCHORS)
    base = np.float32(4.0 * STRIDE) * np.exp2((ids // 3).astype(np.float32) / np.float32(3.0))
    ratio = (ids % 3 - 1).astype(np.float32) / np.float32(2.0)
    return (base * np.exp2(-ratio)).astype(np.float32), (base * np.exp2(ratio)).astype(np.float32)


def box_terms(offsets, assigned, corners, first_row):
    shape = assigned.shape
    ids = lax.broadcasted_iota(jnp.int32, shape, 0)
    lanes = lax.broadcasted_iota(jnp.int32, shape, 1)
    widths, heights = anchor_sizes()
    anchor_w = jnp.zeros(shape, F32)
    anchor_h = jnp.zeros(shape, F32)
    for a in range(ANCHORS):
        anchor_w = jnp.where(ids == a, float(widths[a]), anchor_w)
        anchor_h = jnp.where(ids == a, float(heights[a]), anchor_h)
    second = (lanes >= COLS).astype(jnp.int32)
    centre_y = ((first_row + second).astype(F32) + 0.5) * STRIDE
    centre_x = ((lanes - COLS * second).astype(F32) + 0.5) * STRIDE
    true_left, true_top, true_right, true_bottom = corners
    positive = (assigned >= 0).astype(F32)

    def each(o0, o1, o2, o3):
        middle_x = centre_x + o0 * anchor_w
        middle_y = centre_y + o1 * anchor_h
        pred_width = anchor_w * jnp.exp(o2)
        pred_height = anchor_h * jnp.exp(o3)
        pred_left = middle_x - 0.5 * pred_width
        pred_right = middle_x + 0.5 * pred_width
        pred_top = middle_y - 0.5 * pred_height
        pred_bottom = middle_y + 0.5 * pred_height
        crossing_w = jnp.maximum(
            jnp.minimum(pred_right, true_right) - jnp.maximum(pred_left, true_left), 0.0
        )
        crossing_h = jnp.maximum(
            jnp.minimum(pred_bottom, true_bottom) - jnp.maximum(pred_top, true_top), 0.0
        )
        crossing = crossing_w * crossing_h
        union_area = (
            pred_width * pred_height
            + (true_right - true_left) * (true_bottom - true_top)
            - crossing
        )
        outer_w = jnp.maximum(pred_right, true_right) - jnp.minimum(pred_left, true_left)
        outer_h = jnp.maximum(pred_bottom, true_bottom) - jnp.minimum(pred_top, true_top)
        outer_area = outer_w * outer_h
        giou_value = crossing / union_area - (outer_area - union_area) / outer_area
        return positive * (1.0 - giou_value)

    values, pullback = jax.vjp(each, *offsets)
    return values, pullback(jnp.ones(shape, F32)), positive


def shifted(value, tap):
    if tap == 1:
        return value
    rows = lax.broadcasted_iota(jnp.int32, value.shape, 0)
    if tap == 0:
        return jnp.where(rows == 0, 0.0, pltpu.roll(value, 1, 0))
    return jnp.where(rows == COLS - 1, 0.0, pltpu.roll(value, COLS - 1, 0))


def step_kernel(
    zl_count, zh_count,
    tower, wc_hbm, wb, cls_bias, box_bias, labels, tindex, boxes,
    r_out, q_out, s_out, tg_out,
    w, wbs, bias_row, patches, halo, outs, gf, glow, boxy, acc, send_c, recv_c,
    a1s, a1r, a2s, a2r, accb, b1s0, b1r0, b2s0, b2r0, b1s1, b1r1, b2s1, b2r1,
    zf, zs, zr, zg, small, sz, dpatch, edge_s, edge_r,
    wsem, ready, send, recv,
):
    t = lax.axis_index("tile")
    m = lax.axis_index("img")
    tiles = zl_count * RING * 2
    nz = zl_count * zh_count
    c = t % 2
    y = (t // 2) % RING
    x = m // zh_count
    z = (m % zh_count) * zl_count + t // (2 * RING)

    def at(x_, y_, z_, c_):
        return {
            "tile": (z_ % zl_count) * (2 * RING) + y_ * 2 + c_,
            "img": x_ * zh_count + z_ // zl_count,
        }

    a = x + c * (y - x)
    b = y + c * (x - y)

    def ring(a_, b_):
        return at(a_ + c * (b_ - a_), b_ + c * (a_ - b_), z, c)

    sibling = at(x, y, z, 1 - c)
    above = {"tile": t - 1, "img": m}
    below = {"tile": t + 1, "img": m}
    links = Links(send, recv)

    load = pltpu.make_async_copy(wc_hbm, w, wsem)
    load.start()

    barrier = pltpu.get_barrier_semaphore()

    def greet(device):
        pl.semaphore_signal(barrier, inc=1, device_id=device, device_id_type=MESH)

    greet(sibling)
    for near in (flip(a), 3 - a):
        greet(ring(near, b))
    for near in (flip(b), 3 - b):
        greet(ring(a, near))
    beside_z = (at(x, y, (z + 1) % nz, c), at(x, y, (z + nz - 1) % nz, c))
    for device in beside_z:
        greet(device)

    @pl.when(t > 0)
    def _():
        greet(above)

    @pl.when(t < tiles - 1)
    def _():
        greet(below)

    wanted = jnp.concatenate([tindex[0, :, 0, :], tindex[0, :, 1, :]], axis=1)

    def pick(n, found):
        hit = wanted == n
        return tuple(jnp.where(hit, boxes[0, j, n], found[j]) for j in range(4))

    zero = jnp.zeros(wanted.shape, F32)
    corners = lax.fori_loop(0, boxes.shape[2], pick, (zero, zero, zero, zero))
    wbs[...] = jnp.zeros(wbs.shape, BF16)
    wbs[0 : 4 * ANCHORS, :] = wb[...]

    def fill(row, ext):
        value = row.astype(F32)
        for col_tap in range(3):
            piece = shifted(value, col_tap).astype(BF16)
            for here in range(2):
                row_tap = ext - here
                if 0 <= row_tap <= 2:
                    for part in range(2):
                        k = (3 * row_tap + col_tap) * DEPTH + part * COLS
                        patches[k // HALF, here * COLS : (here + 1) * COLS,
                                k % HALF : k % HALF + COLS] = piece[:, part * COLS : (part + 1) * COLS]

    fill(tower[0, 0], 1)
    fill(tower[0, 1], 2)

    greeted = 1 + 4 + 2
    pl.semaphore_wait(
        barrier, greeted + (t > 0).astype(jnp.int32) + (t < tiles - 1).astype(jnp.int32)
    )

    rounds = nz // 2 - 1

    def tell(k):
        if k < rounds:
            for device in beside_z:
                pl.semaphore_signal(ready.at[k], inc=1, device_id=device, device_id_type=MESH)

    def hear(k):
        if k < rounds:
            pl.semaphore_wait(ready.at[k], 2)
            tell(k + 1)

    tell(0)

    halo_up = links.make(tower.at[0, 0], halo.at[1], above)
    halo_down = links.make(tower.at[0, 1], halo.at[0], below)

    @pl.when(t > 0)
    def _():
        halo_up.start()

    @pl.when(t < tiles - 1)
    def _():
        halo_down.start()

    @pl.when(t == 0)
    def _():
        halo[0] = jnp.zeros(halo.shape[1:], BF16)

    @pl.when(t == tiles - 1)
    def _():
        halo[1] = jnp.zeros(halo.shape[1:], BF16)

    nt = (((1,), (1,)), ((), ()))

    def product(lhs, rhs):
        return lax.dot_general(lhs, rhs, nt, preferred_element_type=F32)

    def column(values):
        wide = jnp.broadcast_to(values, (8, values.shape[1]))
        return jnp.transpose(wide)[:, 0:1]

    edge = 3 * DEPTH
    patches[0, 0:COLS, 0:edge] = jnp.zeros((COLS, edge), BF16)
    patches[1, COLS : 2 * COLS, HALF - edge : HALF] = jnp.zeros((COLS, edge), BF16)
    bias_row[0:1, 0:CLS] = cls_bias[...].reshape(1, CLS)
    bias_row[0:1, CLS:OUTS] = box_bias[...].reshape(1, OUTS - CLS)
    bias_row[0:1, OUTS:PAD_OUTS] = jnp.zeros((1, PAD_OUTS - OUTS), F32)
    bias_col = column(bias_row[0:1, :])
    load.wait()
    for lhs, rows in ((w, slice(0, CLS)), (wbs, slice(CLS, PAD_OUTS))):
        outs[rows, :] = (
            product(lhs[:, 0:HALF], patches[0])
            + product(lhs[:, HALF:WIDTH], patches[1])
            + bias_col[rows]
        )

    @pl.when(t < tiles - 1)
    def _():
        halo_up.wait_recv()

    @pl.when(t > 0)
    def _():
        halo_down.wait_recv()

    fill(halo[0], 0)
    fill(halo[1], 3)
    for lhs, rows in ((w, slice(0, CLS)), (wbs, slice(CLS, PAD_OUTS))):
        outs[rows, 0:COLS] += product(lhs[:, 0:edge], patches[0, 0:COLS, 0:edge])
        outs[rows, COLS : 2 * COLS] += product(
            lhs[:, WIDTH - edge : WIDTH], patches[1, COLS : 2 * COLS, HALF - edge : HALF]
        )
    hear(0)

    class_ids = lax.broadcasted_iota(jnp.int32, (CLASSES, COLS), 0)

    def focal(anchor, total):
        rows = pl.ds(pl.multiple_of(anchor * CLASSES, CLASSES), CLASSES)
        for here in range(2):
            lanes = slice(here * COLS, (here + 1) * COLS)
            score = outs[rows, lanes]
            label = labels[0, anchor, here : here + 1, :]
            hit = jnp.broadcast_to(label, (CLASSES, COLS)) == class_ids
            counted = (label >= -1).astype(F32)
            side = jnp.where(hit, score, -score)
            small = jnp.exp(-jnp.abs(score))
            inverse = 1.0 / (1.0 + small)
            log_p = jnp.minimum(side, 0.0) - jnp.log1p(small)
            right = side >= 0
            p = jnp.where(right, inverse, small * inverse)
            miss = jnp.where(right, small * inverse, inverse)
            alpha = jnp.where(hit, FOCAL_ALPHA, FOCAL_ALPHA - 1.0) * counted
            weight = alpha * miss * miss
            grad = weight * (2.0 * p * log_p - miss)
            value = -jnp.abs(weight) * log_p
            gf[rows, lanes] = grad
            glow[rows, lanes] = grad.astype(BF16)
            total = total + jnp.sum(value.reshape(CLASSES // 8, 8, COLS), axis=0)
        return total

    focal_sum = lax.fori_loop(0, ANCHORS, focal, jnp.zeros((8, COLS), F32))

    assigned = jnp.concatenate([labels[0, :, 0, :], labels[0, :, 1, :]], axis=1)
    for here in range(2):
        boxy[here] = outs[CLS:PAD_OUTS, here * COLS : (here + 1) * COLS]
    offsets = [
        jnp.concatenate([boxy[here, pl.ds(j, ANCHORS, stride=4), :] for here in range(2)], axis=1)
        for j in range(4)
    ]
    giou, offset_grads, positive = box_terms(offsets, assigned, corners, 2 * t)
    boxy[...] = jnp.zeros(boxy.shape, F32)
    for here in range(2):
        lanes = slice(here * COLS, (here + 1) * COLS)
        for j in range(4):
            boxy[here, pl.ds(j, ANCHORS, stride=4), :] = offset_grads[j][:, lanes]
        gf[CLS:PAD_OUTS, lanes] = boxy[here]
    glow[CLS:PAD_OUTS, :] = gf[CLS:PAD_OUTS, :].astype(BF16)

    hear(1)

    send_to_core = []
    for k in range(RING):
        rows = slice(k * RING * BLOCK, (k + 1) * RING * BLOCK)
        part = jnp.dot(glow[rows, :], patches[1 - c], preferred_element_type=F32)
        send_c[k] = part.astype(BF16).reshape(RING, BLOCK, HALF)
        send_to_core.append(links.push(send_c.at[k], recv_c.at[k], sibling))

    def own(k, carry):
        rows = pl.ds(pl.multiple_of(k * RING * BLOCK, RING * BLOCK), RING * BLOCK)
        part = jnp.dot(glow[rows, :], patches[c], preferred_element_type=F32)
        acc[k] = part.reshape(RING, BLOCK, HALF)
        return carry

    lax.fori_loop(0, RING, own, 0)

    hear(2)
    for copy in send_to_core:
        copy.wait_recv()

    def pair(quarter, j):
        return acc[quarter, j] + recv_c[quarter, j].astype(F32)

    steps_a = ((flip(a), 3 - a), (3 - a, flip(a)))
    first = {}
    for which in (1, 0):
        for s in range(2):
            near, far = steps_a[s]
            back = (3 - near, flip(near))[s]
            quarter = back if which else near
            for j in range(2):
                a1s[s, which, j] = pair(quarter, 2 * s + j).astype(BF16)
            first[s, which] = links.push(a1s.at[s, which], a1r.at[s, which], ring(near, b))

    tn = (((0,), (0,)), ((), ()))
    dpatch[...] = lax.dot_general(
        glow[0:CLS, :], w[...], tn, preferred_element_type=F32
    ) + lax.dot_general(glow[CLS:PAD_OUTS, :], wbs[...], tn, preferred_element_type=F32)

    sums = lax.dot_general(
        jnp.ones((8, 2 * COLS), F32), gf[...], nt,
        precision=lax.Precision.HIGHEST, preferred_element_type=F32,
    )
    lane = lax.broadcasted_iota(jnp.int32, (1, COLS), 1)
    mine = jnp.zeros((8, COLS), F32)
    rows8 = lax.broadcasted_iota(jnp.int32, (8, COLS), 0)
    for k in range(PAD_OUTS // COLS):
        mine = jnp.where(rows8 == k, sums[:, k * COLS : (k + 1) * COLS], mine)
    scalars = (jnp.sum(focal_sum), jnp.sum(giou), jnp.sum(positive))
    for k, value in enumerate(scalars):
        mine = jnp.where((rows8 == 6) & (lane == k), value, mine)
    stages = (sibling,) + tuple(ring(n, b) for n in (flip(a), 3 - a)) + tuple(
        ring(a, n) for n in (flip(b), 3 - b)
    )
    doubling = []

    def double(k):
        if k == 0:
            small[0, 0] = mine
        else:
            doubling[k - 1].wait_recv()
            small[k, 0] = small[k - 1, 0] + small[k - 1, 1]
        doubling.append(links.push(small.at[k, 0], small.at[k, 1], stages[k]))

    double(0)

    def reach(row_tap, here):
        total = None
        for col_tap in range(3):
            k = (3 * row_tap + col_tap) * DEPTH
            piece = shifted(dpatch[here * COLS : (here + 1) * COLS, k : k + DEPTH], 2 - col_tap)
            total = piece if total is None else total + piece
        return total

    edge_s[0] = reach(0, 0)
    edge_s[1] = reach(2, 1)
    edge_up = links.make(edge_s.at[0], edge_r.at[1], above)
    edge_down = links.make(edge_s.at[1], edge_r.at[0], below)

    @pl.when(t > 0)
    def _():
        edge_up.start()

    @pl.when(t < tiles - 1)
    def _():
        edge_down.start()

    @pl.when(t == 0)
    def _():
        edge_r[0] = jnp.zeros(edge_r.shape[1:], F32)

    @pl.when(t == tiles - 1)
    def _():
        edge_r[1] = jnp.zeros(edge_r.shape[1:], F32)

    second = []
    for s in range(2):
        near, far = steps_a[s]
        first[s, 1].wait_recv()
        for j in range(2):
            a2s[s, j] = (pair(far, 2 * s + j) + a1r[s, 1, j].astype(F32)).astype(BF16)
        second.append(links.push(a2s.at[s], a2r.at[s], ring(far, b)))

    double(1)

    tg_own = (reach(1, 0) + reach(0, 1), reach(2, 0) + reach(1, 1))

    @pl.when(t < tiles - 1)
    def _():
        edge_up.wait_recv()

    @pl.when(t > 0)
    def _():
        edge_down.wait_recv()

    for here in range(2):
        tg_out[0, here] = (tg_own[here] + edge_r[here]).astype(BF16)

    for s in range(2):
        first[s, 0].wait_recv()
        second[s].wait_recv()
        for j in range(2):
            accb[2 * s + j] = (
                pair(a, 2 * s + j) + a1r[s, 0, j].astype(F32) + a2r[s, j].astype(F32)
            )

    double(2)

    steps_b = ((flip(b), 3 - b), (3 - b, flip(b)))
    bufs = ((b1s0, b1r0, b2s0, b2r0, slice(0, SPLIT)), (b1s1, b1r1, b2s1, b2r1, slice(SPLIT, HALF)))
    first = {}
    for which in (1, 0):
        for s in range(2):
            near, far = steps_b[s]
            back = (3 - near, flip(near))[s]
            quarter = back if which else near
            s1, r1, s2, r2, cols = bufs[s]
            s1[which] = accb[quarter, :, cols].astype(BF16)
            first[s, which] = links.push(s1.at[which], r1.at[which], ring(a, near))
    second = []
    for s in range(2):
        near, far = steps_b[s]
        s1, r1, s2, r2, cols = bufs[s]
        first[s, 1].wait_recv()
        s2[...] = (accb[far, :, cols] + r1[1].astype(F32)).astype(BF16)
        second.append(links.push(s2, r2, ring(a, far)))
    double(3)
    per = zf.shape[1] // 8
    groups = BLOCK // 8
    zf[...] = jnp.zeros(zf.shape, F32)
    for s in range(2):
        s1, r1, s2, r2, cols = bufs[s]
        first[s, 0].wait_recv()
        second[s].wait_recv()
        done = accb[b, :, cols] + r1[0].astype(F32) + r2[...].astype(F32)
        for k in range(cols.start // COLS, cols.stop // COLS):
            at_col = k * COLS - cols.start
            for g in range(groups):
                n = k * groups + g
                zf[n // per, (n % per) * 8 : (n % per) * 8 + 8, :] = done[
                    g * 8 : g * 8 + 8, at_col : at_col + COLS
                ]

    zs[...] = zf[...].astype(BF16)
    turns = [
        links.push(zs.at[(z + k) % nz], zr.at[z], at(x, y, (z + k) % nz, c)) for k in range(1, nz)
    ]
    double(4)
    total = zf[z]
    for k in range(1, nz):
        turns[k - 1].wait_recv()
        total = total + zr[(z + nz - k) % nz].astype(F32)
    zg[z] = total.astype(BF16)
    turns = [
        links.push(zg.at[z], zg.at[z], at(x, y, (z + k) % nz, c)) for k in range(1, nz)
    ]
    doubling[4].wait_recv()
    sz[z] = small[4, 0] + small[4, 1]
    small_z = [
        links.push(sz.at[z], sz.at[z], at(x, y, (z + k) % nz, c)) for k in range(1, nz)
    ]
    for copy in turns:
        copy.wait_recv()
    zf[...] = zg[...].astype(F32)
    for k in range(HALF // COLS):
        pieces = []
        for g in range(groups):
            n = k * groups + g
            pieces.append(zf[n // per, (n % per) * 8 : (n % per) * 8 + 8, :])
        r_out[c, a, b, :, k * COLS : (k + 1) * COLS] = jnp.concatenate(pieces, axis=0).astype(BF16)

    def wrap(i):
        return (i + RING) % RING

    top, bottom = slice(0, 32), slice(32, BLOCK)
    shared = []

    def square(h, a_, b_):
        value = r_out[h, a_, b_].astype(F32)
        value = jnp.sum((value * value).reshape(BLOCK // 8, 8, HALF), axis=0)
        total = value[:, 0:COLS]
        for j in range(1, HALF // COLS):
            total = total + value[:, j * COLS : (j + 1) * COLS]
        q_out[h, a_, b_] = total

    def share(a_, b_):
        shared.append(links.push(r_out.at[c, a_, b_], r_out.at[c, a_, b_], sibling))
        square(c, a_, b_)

    def along_a(b_):
        block = r_out.at[c, a, b_]
        return (
            links.push(block, block, ring(wrap(a + 1), b)),
            links.push(block, block, ring(wrap(a - 1), b)),
        )

    block = r_out.at[c, a, b]
    to_next = links.push(block, block, ring(a, wrap(b + 1)))
    to_last = links.push(block, block, ring(a, wrap(b - 1)))
    wide = [along_a(b)]
    share(a, b)
    to_next.wait_recv()
    block = r_out.at[c, a, wrap(b - 1), top]
    on_next = links.push(block, block, ring(a, wrap(b + 1)))
    wide.append(along_a(wrap(b - 1)))
    share(a, wrap(b - 1))
    to_last.wait_recv()
    block = r_out.at[c, a, wrap(b + 1), bottom]
    on_last = links.push(block, block, ring(a, wrap(b - 1)))
    wide.append(along_a(wrap(b + 1)))
    share(a, wrap(b + 1))
    on_next.wait_recv()
    on_last.wait_recv()
    wide.append(along_a(wrap(b + 2)))
    share(a, wrap(b + 2))

    order = (b, wrap(b - 1), wrap(b + 1), wrap(b + 2))
    rest = []
    for k, b_ in enumerate(order):
        wide[k][0].wait_recv()
        if k < 2:
            block = r_out.at[c, wrap(a - 1), b_]
            rest.append(links.push(block, block, ring(wrap(a + 1), b)))
        share(wrap(a - 1), b_)
        wide[k][1].wait_recv()
        if k >= 2:
            block = r_out.at[c, wrap(a + 1), b_]
            rest.append(links.push(block, block, ring(wrap(a - 1), b)))
        share(wrap(a + 1), b_)
    for k, b_ in enumerate(order):
        rest[k].wait_recv()
        share(wrap(a + 2), b_)

    for copy in small_z:
        copy.wait_recv()
    whole = sz[0]
    for k in range(1, nz):
        whole = whole + sz[k]
    s_out[...] = whole

    for copy in shared:
        copy.wait_recv()

    def other(k, carry):
        square(1 - c, k // RING, k % RING)
        return carry

    lax.fori_loop(0, RING * RING, other, 0)
    links.drain()

    @pl.when(t > 0)
    def _():
        halo_up.wait_send()
        edge_up.wait_send()

    @pl.when(t < tiles - 1)
    def _():
        halo_down.wait_send()
        edge_down.wait_send()


def scale_kernel(r, q, s, tg, cls_out, box_out, loss_out, cls_bias_out, box_bias_out, tg_out, stage, sem):
    slots = stage.shape[0]
    tower_copy = pltpu.make_async_copy(tg, tg_out, sem.at[slots])
    tower_copy.start()
    rows8 = lax.broadcasted_iota(jnp.int32, (8, COLS), 0)
    bias = jnp.where(rows8 < PAD_OUTS // COLS, s[...], 0.0)
    total = bias * bias
    for k in range(2 * RING * RING):
        total = total + q[k // (RING * RING), k // RING % RING, k % RING]
    total = jnp.sum(total, keepdims=True)
    scale = lax.rsqrt(total / (OUTS * (WIDTH + 1)) + NORM_EPS)
    bias = bias * scale
    cls_bias_out[...] = bias
    at_row, at_lane = CLS // COLS, CLS % COLS
    box_bias_out[...] = pltpu.roll(bias, COLS - at_lane, 1)[at_row : at_row + 1]
    loss_out[...] = (s[6:7, 0:1] + s[6:7, 1:2]) / s[6:7, 2:3]

    count = CLS // BLOCK

    def store(k):
        return pltpu.make_async_copy(
            stage.at[k % slots],
            cls_out.at[pl.ds(pl.multiple_of(k * BLOCK, BLOCK), BLOCK)],
            sem.at[k % slots],
        )

    def chunk(k, carry):
        @pl.when(k >= slots)
        def _():
            store(k - slots).wait()

        for h in range(2):
            stage[k % slots, :, h * HALF : (h + 1) * HALF] = (
                r[h, k // RING, k % RING].astype(F32) * scale
            )
        store(k).start()
        return carry

    lax.fori_loop(0, count, chunk, 0)
    for h in range(2):
        box_out[:, h * HALF : (h + 1) * HALF] = (
            r[h, RING - 1, RING - 1].astype(F32) * scale
        )[0 : 4 * ANCHORS]
    for k in range(count - slots, count):
        store(k).wait()
    tower_copy.wait()


def per_device(
    zl_count, zh_count, tower, cls_weight, cls_bias, box_weight, box_bias, labels, target_index, boxes
):
    nz = zl_count * zh_count
    tiles8 = BLOCK // 8 * (HALF // COLS)
    per = -(-tiles8 // nz) * 8
    vmem = pl.BlockSpec(memory_space=pltpu.VMEM)
    copies = 100 + 4 * nz

    def buf(*shape, dtype=BF16):
        return pltpu.VMEM(shape, dtype)

    r, q, s, tower_grad = pl.pallas_call(
        functools.partial(step_kernel, zl_count, zh_count),
        out_shape=(
            buf(2, RING, RING, BLOCK, HALF),
            buf(2, RING, RING, 8, COLS, dtype=F32),
            buf(8, COLS, dtype=F32),
            buf(*tower.shape),
        ),
        in_specs=[
            vmem,
            pl.BlockSpec(memory_space=pl.ANY),
            vmem, vmem, vmem, vmem, vmem,
            pl.BlockSpec(memory_space=pltpu.SMEM),
        ],
        out_specs=(vmem, vmem, vmem, vmem),
        scratch_shapes=[
            buf(CLS, WIDTH),
            buf(PAD_OUTS - CLS, WIDTH),
            buf(8, PAD_OUTS, dtype=F32),
            buf(2, 2 * COLS, HALF),
            buf(2, COLS, DEPTH),
            buf(PAD_OUTS, 2 * COLS, dtype=F32),
            buf(PAD_OUTS, 2 * COLS, dtype=F32),
            buf(PAD_OUTS, 2 * COLS),
            buf(2, PAD_OUTS - CLS, COLS, dtype=F32),
            buf(RING, RING, BLOCK, HALF, dtype=F32),
            buf(RING, RING, BLOCK, HALF),
            buf(RING, RING, BLOCK, HALF),
            buf(2, 2, 2, BLOCK, HALF),
            buf(2, 2, 2, BLOCK, HALF),
            buf(2, 2, BLOCK, HALF),
            buf(2, 2, BLOCK, HALF),
            buf(RING, BLOCK, HALF, dtype=F32),
            buf(2, BLOCK, SPLIT),
            buf(2, BLOCK, SPLIT),
            buf(BLOCK, SPLIT),
            buf(BLOCK, SPLIT),
            buf(2, BLOCK, HALF - SPLIT),
            buf(2, BLOCK, HALF - SPLIT),
            buf(BLOCK, HALF - SPLIT),
            buf(BLOCK, HALF - SPLIT),
            buf(nz, per, COLS, dtype=F32),
            buf(nz, per, COLS),
            buf(nz, per, COLS),
            buf(nz, per, COLS),
            buf(5, 2, 8, COLS, dtype=F32),
            buf(nz, 8, COLS, dtype=F32),
            buf(2 * COLS, WIDTH, dtype=F32),
            buf(2, COLS, DEPTH, dtype=F32),
            buf(2, COLS, DEPTH, dtype=F32),
            pltpu.SemaphoreType.DMA,
            pltpu.SemaphoreType.REGULAR((max(nz // 2 - 1, 1),)),
            pltpu.SemaphoreType.DMA((copies,)),
            pltpu.SemaphoreType.DMA((copies,)),
        ],
        compiler_params=pltpu.CompilerParams(
            collective_id=0, has_side_effects=True, vmem_limit_bytes=56 * 2**20
        ),
        name="step",
    )(tower, cls_weight, box_weight, cls_bias, box_bias, labels, target_index, boxes)

    hbm = pl.BlockSpec(memory_space=pl.ANY)
    cls_grad, box_grad, loss, cls_bias_grad, box_bias_grad, tower_grad = pl.pallas_call(
        scale_kernel,
        out_shape=(
            jax.ShapeDtypeStruct((CLS, WIDTH), F32),
            jax.ShapeDtypeStruct((OUTS - CLS, WIDTH), F32),
            jax.ShapeDtypeStruct((1, 1), F32),
            jax.ShapeDtypeStruct((8, COLS), F32),
            jax.ShapeDtypeStruct((1, COLS), F32),
            jax.ShapeDtypeStruct(tower.shape, BF16),
        ),
        in_specs=[vmem, vmem, vmem, vmem],
        out_specs=(hbm, vmem, vmem, vmem, vmem, hbm),
        scratch_shapes=[
            buf(4, BLOCK, WIDTH, dtype=F32),
            pltpu.SemaphoreType.DMA((5,)),
        ],
        compiler_params=pltpu.CompilerParams(vmem_limit_bytes=40 * 2**20),
        name="scale",
    )(r, q, s, tower_grad)
    return (
        loss.reshape(()),
        cls_grad,
        cls_bias_grad.reshape(-1)[:CLS],
        box_grad,
        box_bias_grad.reshape(-1)[: OUTS - CLS],
        tower_grad,
    )


def solution(mesh):
    zl_count = mesh.shape["tile"] // (2 * RING)
    zh_count = mesh.shape["img"] // RING
    placed = (
        P("img", "tile", None, None),
        P(),
        P(),
        P(),
        P(),
        P("img", None, "tile", None),
        P("img", None, "tile", None),
        P("img", None, None),
    )
    return jax.shard_map(
        functools.partial(per_device, zl_count, zh_count),
        mesh=mesh,
        in_specs=placed,
        out_specs=(P(), P(), P(), P(), P(), P("img", "tile", None, None)),
        check_vma=False,
    )
```

```python
import functools

import jax
import jax.numpy as jnp
import numpy as np
from jax import lax
from jax.experimental import pallas as pl
from jax.experimental.pallas import tpu as pltpu
from jax.sharding import PartitionSpec as P

CLASSES = 80
ANCHORS = 9
STRIDE = 8
FOCAL_ALPHA = 0.25
NORM_EPS = 1e-06

RING = 4
IN_FLIGHT = 40
RECEIVES = 74
GROUPS = 9
CLS = ANCHORS * CLASSES
OUTS = CLS + 4 * ANCHORS
PAD_OUTS = 768
TAPS = 9
DEPTH = 256
WIDTH = TAPS * DEPTH
HALF = WIDTH // 2
COLS = 128
BLOCK = PAD_OUTS // (RING * RING)
STREAMS = ((0, 640, 384), (640, 1152, 256))
BF16 = jnp.bfloat16
F32 = jnp.float32
MESH = pl.DeviceIdType.MESH


def flip(i):
    return i + 1 - 2 * (i % 2)


class Links:
    def __init__(self, send, recv):
        self.send, self.recv = send, recv
        self.sends = self.recvs = 0
        self.sent, self.groups = [], []

    def make(self, src, dst, device, pair=None):
        send_id, recv_id = self.pair() if pair is None else pair
        return pltpu.make_async_remote_copy(
            src_ref=src,
            dst_ref=dst,
            send_sem=self.send.at[send_id],
            recv_sem=self.recv.at[recv_id],
            device_id=device,
            device_id_type=MESH,
        )

    def pair(self):
        self.sends += 1
        self.recvs += 1
        return IN_FLIGHT + self.sends - 1, self.recvs - 1

    def push(self, src, dst, device):
        slot = len(self.sent) % IN_FLIGHT
        if len(self.sent) >= IN_FLIGHT:
            self.sent[-IN_FLIGHT].wait_send()
        self.recvs += 1
        copy = self.make(src, dst, device, (slot, self.recvs - 1))
        copy.start()
        self.sent.append(copy)
        return copy

    def group(self, whole, device):
        pair = self.pair()
        both = self.make(whole, whole, device, pair)
        self.groups.append(both)

        def start(src, dst, to):
            self.make(src, dst, to, pair).start()

        return start, both.wait_recv

    def drain(self):
        for copy in self.sent[-IN_FLIGHT:]:
            copy.wait_send()
        for both in self.groups:
            both.wait_send()


def anchor_sizes():
    ids = np.arange(ANCHORS)
    base = np.float32(4.0 * STRIDE) * np.exp2((ids // 3).astype(np.float32) / np.float32(3.0))
    ratio = (ids % 3 - 1).astype(np.float32) / np.float32(2.0)
    return (base * np.exp2(-ratio)).astype(np.float32), (base * np.exp2(ratio)).astype(np.float32)


def box_terms(offsets, assigned, corners, first_row):
    shape = assigned.shape
    ids = lax.broadcasted_iota(jnp.int32, shape, 0)
    lanes = lax.broadcasted_iota(jnp.int32, shape, 1)
    widths, heights = anchor_sizes()
    anchor_w = jnp.zeros(shape, F32)
    anchor_h = jnp.zeros(shape, F32)
    for a in range(ANCHORS):
        anchor_w = jnp.where(ids == a, float(widths[a]), anchor_w)
        anchor_h = jnp.where(ids == a, float(heights[a]), anchor_h)
    second = (lanes >= COLS).astype(jnp.int32)
    centre_y = ((first_row + second).astype(F32) + 0.5) * STRIDE
    centre_x = ((lanes - COLS * second).astype(F32) + 0.5) * STRIDE
    true_left, true_top, true_right, true_bottom = corners
    positive = (assigned >= 0).astype(F32)

    def each(o0, o1, o2, o3):
        middle_x = centre_x + o0 * anchor_w
        middle_y = centre_y + o1 * anchor_h
        pred_width = anchor_w * jnp.exp(o2)
        pred_height = anchor_h * jnp.exp(o3)
        pred_left = middle_x - 0.5 * pred_width
        pred_right = middle_x + 0.5 * pred_width
        pred_top = middle_y - 0.5 * pred_height
        pred_bottom = middle_y + 0.5 * pred_height
        crossing_w = jnp.maximum(
            jnp.minimum(pred_right, true_right) - jnp.maximum(pred_left, true_left), 0.0
        )
        crossing_h = jnp.maximum(
            jnp.minimum(pred_bottom, true_bottom) - jnp.maximum(pred_top, true_top), 0.0
        )
        crossing = crossing_w * crossing_h
        union_area = (
            pred_width * pred_height
            + (true_right - true_left) * (true_bottom - true_top)
            - crossing
        )
        outer_w = jnp.maximum(pred_right, true_right) - jnp.minimum(pred_left, true_left)
        outer_h = jnp.maximum(pred_bottom, true_bottom) - jnp.minimum(pred_top, true_top)
        outer_area = outer_w * outer_h
        giou_value = crossing / union_area - (outer_area - union_area) / outer_area
        return positive * (1.0 - giou_value)

    values, pullback = jax.vjp(each, *offsets)
    return values, pullback(jnp.ones(shape, F32)), positive


def shifted(value, tap):
    if tap == 1:
        return value
    rows = lax.broadcasted_iota(jnp.int32, value.shape, 0)
    if tap == 0:
        return jnp.where(rows == 0, 0.0, pltpu.roll(value, 1, 0))
    return jnp.where(rows == COLS - 1, 0.0, pltpu.roll(value, COLS - 1, 0))


def step_kernel(
    zl_count, zh_count,
    tower, wc_hbm, wb, cls_bias, box_bias, labels, tindex, boxes,
    r_out0, r_out1, q_out, s_out, tg_out,
    w, wbs, bias_row, ext, patches, beside, outs, gf, glow, theirs, boxy,
    small, sz, dpatch, edge_s, edge_r,
    wsem, ready, send, recv, *per_stream,
):
    t = lax.axis_index("tile")
    m = lax.axis_index("img")
    tiles = zl_count * RING * 2
    nz = zl_count * zh_count
    c = t % 2
    y = (t // 2) % RING
    x = m // zh_count
    z = (m % zh_count) * zl_count + t // (2 * RING)

    def at(x_, y_, z_, c_):
        return {
            "tile": (z_ % zl_count) * (2 * RING) + y_ * 2 + c_,
            "img": x_ * zh_count + z_ // zl_count,
        }

    a = x + c * (y - x)
    b = y + c * (x - y)

    def ring(a_, b_):
        return at(a_ + c * (b_ - a_), b_ + c * (a_ - b_), z, c)

    sibling = at(x, y, z, 1 - c)
    outer = {"tile": t + 2 * c - 1, "img": m}
    has_outer = jnp.where(c == 0, t > 0, t < tiles - 1)
    links = Links(send, recv)

    load = pltpu.make_async_copy(wc_hbm, w, wsem)
    load.start()

    barrier = pltpu.get_barrier_semaphore()

    def greet(device):
        pl.semaphore_signal(barrier, inc=1, device_id=device, device_id_type=MESH)

    greet(sibling)
    for near in (flip(a), 3 - a):
        greet(ring(near, b))
    for near in (flip(b), 3 - b):
        greet(ring(a, near))
    beside_z = (at(x, y, (z + 1) % nz, c), at(x, y, (z + nz - 1) % nz, c))
    for device in beside_z:
        greet(device)

    @pl.when(has_outer)
    def _():
        greet(outer)

    wanted = jnp.concatenate([tindex[0, :, 0, :], tindex[0, :, 1, :]], axis=1)

    def pick(n, found):
        hit = wanted == n
        return tuple(jnp.where(hit, boxes[0, j, n], found[j]) for j in range(4))

    zero = jnp.zeros(wanted.shape, F32)
    corners = lax.fori_loop(0, boxes.shape[2], pick, (zero, zero, zero, zero))
    wbs[...] = jnp.zeros(wbs.shape, BF16)
    wbs[0 : 4 * ANCHORS, :] = wb[...]

    def fill(row, place, halves, put):
        value = row.astype(F32)
        for col_tap in range(3):
            piece = shifted(value, col_tap).astype(BF16)
            for here in range(2):
                row_tap = place - here
                if 0 <= row_tap <= 2:
                    for part in range(2):
                        k = (3 * row_tap + col_tap) * DEPTH + part * COLS
                        if k // HALF in halves:
                            put(
                                k // HALF,
                                slice(here * COLS, (here + 1) * COLS),
                                slice(k % HALF, k % HALF + COLS),
                                piece[:, part * COLS : (part + 1) * COLS],
                            )

    def put_own(half, rows, cols, value):
        patches[half, rows, cols] = value

    def put_beside(half, rows, cols, value):
        beside[rows, cols] = value

    for here in range(2):
        ext[1 + 2 * c + here] = tower[0, here]
        fill(tower[0, here], 1 + here, (0, 1), put_own)

    pl.semaphore_wait(barrier, 1 + 4 + 2 + has_outer.astype(jnp.int32))

    rounds = nz // 2 - 1

    def tell(k):
        if k < rounds:
            for device in beside_z:
                pl.semaphore_signal(ready.at[k], inc=1, device_id=device, device_id_type=MESH)

    def hear(k):
        if k < rounds:
            pl.semaphore_wait(ready.at[k], 2)
            tell(k + 1)

    halo = links.make(tower.at[0, c], ext.at[5 * (1 - c)], outer)

    @pl.when(has_outer)
    def _():
        halo.start()

    @pl.when(jnp.logical_not(has_outer))
    def _():
        ext[5 * c] = jnp.zeros(ext.shape[1:], BF16)

    rows_across = links.push(tower.at[0], ext.at[pl.ds(1 + 2 * c, 2)], sibling)
    tell(0)

    nt = (((1,), (1,)), ((), ()))

    def product(lhs, rhs):
        return lax.dot_general(lhs, rhs, nt, preferred_element_type=F32)

    def column(values):
        wide = jnp.broadcast_to(values, (8, values.shape[1]))
        return jnp.transpose(wide)[:, 0:1]

    edge = 3 * DEPTH
    patches[0, 0:COLS, 0:edge] = jnp.zeros((COLS, edge), BF16)
    patches[1, COLS : 2 * COLS, HALF - edge : HALF] = jnp.zeros((COLS, edge), BF16)
    bias_row[0:1, 0:CLS] = cls_bias[...].reshape(1, CLS)
    bias_row[0:1, CLS:OUTS] = box_bias[...].reshape(1, OUTS - CLS)
    bias_row[0:1, OUTS:PAD_OUTS] = jnp.zeros((1, PAD_OUTS - OUTS), F32)
    bias_col = column(bias_row[0:1, :])
    load.wait()
    for lhs, rows in ((w, slice(0, CLS)), (wbs, slice(CLS, PAD_OUTS))):
        outs[rows, :] = (
            product(lhs[:, 0:HALF], patches[0])
            + product(lhs[:, HALF:WIDTH], patches[1])
            + bias_col[rows]
        )

    rows_across.wait_recv()

    @pl.when(has_outer)
    def _():
        halo.wait_recv()

    outer_across = links.push(ext.at[5 * c], ext.at[5 * c], sibling)
    fill(ext[2 * c], 0, (0, 1), put_own)
    fill(ext[2 * c + 3], 3, (0, 1), put_own)
    for lhs, rows in ((w, slice(0, CLS)), (wbs, slice(CLS, PAD_OUTS))):
        outs[rows, 0:COLS] += product(lhs[:, 0:edge], patches[0, 0:COLS, 0:edge])
        outs[rows, COLS : 2 * COLS] += product(
            lhs[:, WIDTH - edge : WIDTH], patches[1, COLS : 2 * COLS, HALF - edge : HALF]
        )
    hear(0)

    class_ids = lax.broadcasted_iota(jnp.int32, (CLASSES, COLS), 0)

    def focal(anchor, total):
        rows = pl.ds(pl.multiple_of(anchor * CLASSES, CLASSES), CLASSES)
        for here in range(2):
            lanes = slice(here * COLS, (here + 1) * COLS)
            score = outs[rows, lanes]
            label = labels[0, anchor, here : here + 1, :]
            hit = jnp.broadcast_to(label, (CLASSES, COLS)) == class_ids
            counted = (label >= -1).astype(F32)
            side = jnp.where(hit, score, -score)
            small_e = jnp.exp(-jnp.abs(score))
            inverse = 1.0 / (1.0 + small_e)
            log_p = jnp.minimum(side, 0.0) - jnp.log1p(small_e)
            right = side >= 0
            p = jnp.where(right, inverse, small_e * inverse)
            miss = jnp.where(right, small_e * inverse, inverse)
            alpha = jnp.where(hit, FOCAL_ALPHA, FOCAL_ALPHA - 1.0) * counted
            weight = alpha * miss * miss
            grad = weight * (2.0 * p * log_p - miss)
            value = -jnp.abs(weight) * log_p
            gf[rows, lanes] = grad
            glow[rows, lanes] = grad.astype(BF16)
            total = total + jnp.sum(value.reshape(CLASSES // 8, 8, COLS), axis=0)
        return total

    focal_sum = lax.fori_loop(0, ANCHORS, focal, jnp.zeros((8, COLS), F32))

    assigned = jnp.concatenate([labels[0, :, 0, :], labels[0, :, 1, :]], axis=1)
    for here in range(2):
        boxy[here] = outs[CLS:PAD_OUTS, here * COLS : (here + 1) * COLS]
    offsets = [
        jnp.concatenate([boxy[here, pl.ds(j, ANCHORS, stride=4), :] for here in range(2)], axis=1)
        for j in range(4)
    ]
    giou, offset_grads, positive = box_terms(offsets, assigned, corners, 2 * t)
    boxy[...] = jnp.zeros(boxy.shape, F32)
    for here in range(2):
        lanes = slice(here * COLS, (here + 1) * COLS)
        for j in range(4):
            boxy[here, pl.ds(j, ANCHORS, stride=4), :] = offset_grads[j][:, lanes]
        gf[CLS:PAD_OUTS, lanes] = boxy[here]
    glow[CLS:PAD_OUTS, :] = gf[CLS:PAD_OUTS, :].astype(BF16)
    glow_across = links.push(glow, theirs, sibling)

    streams = []
    each = len(per_stream) // len(STREAMS)
    for k, (start, stop, cut) in enumerate(STREAMS):
        streams.append(((r_out0, r_out1)[k], start, stop, cut, *per_stream[k * each : (k + 1) * each]))
    for _, start, stop, _, acc, *_ in streams:
        part = jnp.dot(glow[...], patches[c, :, start:stop], preferred_element_type=F32)
        acc[...] = part.reshape(acc.shape)
    hear(1)
    outer_across.wait_recv()
    for half in range(2):

        @pl.when(c == half)
        def _():
            for place in range(4):
                fill(ext[2 * (1 - half) + place], place, (half,), put_beside)

    glow_across.wait_recv()

    def wrap(i):
        return (i + RING) % RING

    top, bottom = slice(0, 32), slice(32, BLOCK)
    groups = BLOCK // 8
    shared = []

    def square(k, h, a_, b_):
        r = streams[k][0]
        value = r[h, a_, b_].astype(F32)
        value = jnp.sum((value * value).reshape(groups, 8, value.shape[1]), axis=0)
        total = value[:, 0:COLS]
        for j in range(1, value.shape[1] // COLS):
            total = total + value[:, j * COLS : (j + 1) * COLS]
        q_out[k, h, a_, b_] = total

    def stream(
        number, r, start, stop, cut,
        acc, a1s, a1r, a2s, a2r, accb, b1s0, b1r0, b2s0, b2r0, b1s1, b1r1, b2s1, b2r1,
        zf, zs, zr, zg,
    ):
        width = stop - start
        part = jnp.dot(theirs[...], beside[:, start:stop], preferred_element_type=F32)
        acc[...] += part.reshape(acc.shape)

        steps = ((flip(a), 3 - a), (3 - a, flip(a)))
        first = {}
        for which in (1, 0):
            for s in range(2):
                near, far = steps[s]
                back = (3 - near, flip(near))[s]
                quarter = back if which else near
                for j in range(2):
                    a1s[s, which, j] = acc[quarter, 2 * s + j].astype(BF16)
                first[s, which] = links.push(a1s.at[s, which], a1r.at[s, which], ring(near, b))
        yield

        second = []
        for s in range(2):
            near, far = steps[s]
            first[s, 1].wait_recv()
            for j in range(2):
                a2s[s, j] = (acc[far, 2 * s + j] + a1r[s, 1, j].astype(F32)).astype(BF16)
            second.append(links.push(a2s.at[s], a2r.at[s], ring(far, b)))
        yield

        for s in range(2):
            first[s, 0].wait_recv()
            second[s].wait_recv()
            for j in range(2):
                accb[2 * s + j] = (
                    acc[a, 2 * s + j] + a1r[s, 0, j].astype(F32) + a2r[s, j].astype(F32)
                )

        steps = ((flip(b), 3 - b), (3 - b, flip(b)))
        bufs = (
            (b1s0, b1r0, b2s0, b2r0, slice(0, cut)),
            (b1s1, b1r1, b2s1, b2r1, slice(cut, width)),
        )
        first = {}
        for which in (1, 0):
            for s in range(2):
                near, far = steps[s]
                back = (3 - near, flip(near))[s]
                quarter = back if which else near
                s1, r1, s2, r2, cols = bufs[s]
                s1[which] = accb[quarter, :, cols].astype(BF16)
                first[s, which] = links.push(s1.at[which], r1.at[which], ring(a, near))
        yield

        second = []
        for s in range(2):
            near, far = steps[s]
            s1, r1, s2, r2, cols = bufs[s]
            first[s, 1].wait_recv()
            s2[...] = (accb[far, :, cols] + r1[1].astype(F32)).astype(BF16)
            second.append(links.push(s2, r2, ring(a, far)))
        yield

        per = zf.shape[1] // 8
        zf[...] = jnp.zeros(zf.shape, F32)
        for s in range(2):
            s1, r1, s2, r2, cols = bufs[s]
            first[s, 0].wait_recv()
            second[s].wait_recv()
            done = accb[b, :, cols] + r1[0].astype(F32) + r2[...].astype(F32)
            for k in range(cols.start // COLS, cols.stop // COLS):
                at_col = k * COLS - cols.start
                for g in range(groups):
                    n = k * groups + g
                    zf[n // per, (n % per) * 8 : (n % per) * 8 + 8, :] = done[
                        g * 8 : g * 8 + 8, at_col : at_col + COLS
                    ]

        zs[...] = zf[...].astype(BF16)
        turn, arrived = links.group(zr.at[pl.ds(0, nz - 1)], beside_z[0])
        for k in range(1, nz):
            turn(zs.at[(z + k) % nz], zr.at[z], at(x, y, (z + k) % nz, c))
        yield

        arrived()
        total = zf[z]
        for k in range(1, nz):
            total = total + zr[(z + nz - k) % nz].astype(F32)
        zg[z] = total.astype(BF16)
        turn, arrived = links.group(zg.at[pl.ds(0, nz - 1)], beside_z[0])
        for k in range(1, nz):
            turn(zg.at[z], zg.at[z], at(x, y, (z + k) % nz, c))
        yield

        arrived()
        zf[...] = zg[...].astype(F32)
        for k in range(width // COLS):
            pieces = []
            for g in range(groups):
                n = k * groups + g
                pieces.append(zf[n // per, (n % per) * 8 : (n % per) * 8 + 8, :])
            r[c, a, b, :, k * COLS : (k + 1) * COLS] = jnp.concatenate(pieces, axis=0).astype(BF16)

        across, all_across = links.group(r.at[1 - c], sibling)
        shared.append(all_across)

        def share(a_, b_):
            across(r.at[c, a_, b_], r.at[c, a_, b_], sibling)
            square(number, c, a_, b_)

        def along_a(b_):
            block = r.at[c, a, b_]
            return (
                links.push(block, block, ring(wrap(a + 1), b)),
                links.push(block, block, ring(wrap(a - 1), b)),
            )

        block = r.at[c, a, b]
        to_next = links.push(block, block, ring(a, wrap(b + 1)))
        to_last = links.push(block, block, ring(a, wrap(b - 1)))
        wide = [along_a(b)]
        share(a, b)
        yield

        to_next.wait_recv()
        block = r.at[c, a, wrap(b - 1), top]
        on_next = links.push(block, block, ring(a, wrap(b + 1)))
        wide.append(along_a(wrap(b - 1)))
        share(a, wrap(b - 1))
        to_last.wait_recv()
        block = r.at[c, a, wrap(b + 1), bottom]
        on_last = links.push(block, block, ring(a, wrap(b - 1)))
        wide.append(along_a(wrap(b + 1)))
        share(a, wrap(b + 1))
        yield

        on_next.wait_recv()
        on_last.wait_recv()
        wide.append(along_a(wrap(b + 2)))
        share(a, wrap(b + 2))
        yield

        order = (b, wrap(b - 1), wrap(b + 1), wrap(b + 2))
        rest = []
        for k, b_ in enumerate(order):
            wide[k][0].wait_recv()
            if k < 2:
                block = r.at[c, wrap(a - 1), b_]
                rest.append(links.push(block, block, ring(wrap(a + 1), b)))
            share(wrap(a - 1), b_)
            wide[k][1].wait_recv()
            if k >= 2:
                block = r.at[c, wrap(a + 1), b_]
                rest.append(links.push(block, block, ring(wrap(a - 1), b)))
            share(wrap(a + 1), b_)
            yield
        for k, b_ in enumerate(order):
            rest[k].wait_recv()
            share(wrap(a + 2), b_)
            yield

    going = [stream(k, *refs) for k, refs in enumerate(streams)]

    def step():
        for one in going:
            next(one, None)

    step()
    hear(2)

    tn = (((0,), (0,)), ((), ()))
    dpatch[...] = lax.dot_general(
        glow[0:CLS, :], w[...], tn, preferred_element_type=F32
    ) + lax.dot_general(glow[CLS:PAD_OUTS, :], wbs[...], tn, preferred_element_type=F32)

    def reach(row_tap, here):
        total = None
        for col_tap in range(3):
            k = (3 * row_tap + col_tap) * DEPTH
            piece = shifted(dpatch[here * COLS : (here + 1) * COLS, k : k + DEPTH], 2 - col_tap)
            total = piece if total is None else total + piece
        return total

    edge_s[0] = reach(0, 0)
    edge_s[1] = reach(2, 1)
    edge_out = links.make(edge_s.at[c], edge_r.at[1 - c], outer)
    edge_in = links.push(edge_s.at[1 - c], edge_r.at[c], sibling)

    @pl.when(has_outer)
    def _():
        edge_out.start()

    @pl.when(jnp.logical_not(has_outer))
    def _():
        edge_r[c] = jnp.zeros(edge_r.shape[1:], F32)

    sums = lax.dot_general(
        jnp.ones((8, 2 * COLS), F32), gf[...], nt,
        precision=lax.Precision.HIGHEST, preferred_element_type=F32,
    )
    lane = lax.broadcasted_iota(jnp.int32, (1, COLS), 1)
    mine = jnp.zeros((8, COLS), F32)
    rows8 = lax.broadcasted_iota(jnp.int32, (8, COLS), 0)
    for k in range(PAD_OUTS // COLS):
        mine = jnp.where(rows8 == k, sums[:, k * COLS : (k + 1) * COLS], mine)
    scalars = (jnp.sum(focal_sum), jnp.sum(giou), jnp.sum(positive))
    for k, value in enumerate(scalars):
        mine = jnp.where((rows8 == 6) & (lane == k), value, mine)
    stages = (sibling,) + tuple(ring(n, b) for n in (flip(a), 3 - a)) + tuple(
        ring(a, n) for n in (flip(b), 3 - b)
    )
    doubling = []

    def double(k):
        if k == 0:
            small[0, 0] = mine
        else:
            doubling[k - 1].wait_recv()
            small[k, 0] = small[k - 1, 0] + small[k - 1, 1]
        doubling.append(links.push(small.at[k, 0], small.at[k, 1], stages[k]))

    double(0)
    step()
    double(1)

    tg_own = (reach(1, 0) + reach(0, 1), reach(2, 0) + reach(1, 1))
    edge_in.wait_recv()

    @pl.when(has_outer)
    def _():
        edge_out.wait_recv()

    for here in range(2):
        tg_out[0, here] = (tg_own[here] + edge_r[here]).astype(BF16)

    step()
    double(2)
    step()
    double(3)
    step()
    double(4)
    step()
    doubling[4].wait_recv()
    sz[z] = small[4, 0] + small[4, 1]
    turn, small_arrived = links.group(sz.at[pl.ds(0, nz - 1)], beside_z[0])
    for k in range(1, nz):
        turn(sz.at[z], sz.at[z], at(x, y, (z + k) % nz, c))
    step()
    step()
    step()
    for _ in range(2 * RING + 1):
        step()

    small_arrived()
    whole = sz[0]
    for k in range(1, nz):
        whole = whole + sz[k]
    s_out[...] = whole

    for all_across in shared:
        all_across()

    def other(i, carry):
        for k in range(len(STREAMS)):
            square(k, 1 - c, i // RING, i % RING)
        return carry

    lax.fori_loop(0, RING * RING, other, 0)
    links.drain()

    @pl.when(has_outer)
    def _():
        halo.wait_send()
        edge_out.wait_send()


def scale_kernel(r0, r1, q, s, tg, cls_out, box_out, loss_out, cls_bias_out, box_bias_out, tg_out, stage, sem):
    slots = stage.shape[0]
    tower_copy = pltpu.make_async_copy(tg, tg_out, sem.at[slots])
    tower_copy.start()
    rows8 = lax.broadcasted_iota(jnp.int32, (8, COLS), 0)
    bias = jnp.where(rows8 < PAD_OUTS // COLS, s[...], 0.0)
    total = bias * bias
    for k in range(len(STREAMS)):
        for n in range(2 * RING * RING):
            total = total + q[k, n // (RING * RING), n // RING % RING, n % RING]
    total = jnp.sum(total, keepdims=True)
    scale = lax.rsqrt(total / (OUTS * (WIDTH + 1)) + NORM_EPS)
    bias = bias * scale
    cls_bias_out[...] = bias
    at_row, at_lane = CLS // COLS, CLS % COLS
    box_bias_out[...] = pltpu.roll(bias, COLS - at_lane, 1)[at_row : at_row + 1, 0 : OUTS - CLS]
    loss_out[...] = (s[6:7, 0:1] + s[6:7, 1:2]) / s[6:7, 2:3]

    count = CLS // BLOCK

    def store(k):
        return pltpu.make_async_copy(
            stage.at[k % slots],
            cls_out.at[pl.ds(pl.multiple_of(k * BLOCK, BLOCK), BLOCK)],
            sem.at[k % slots],
        )

    def chunk(k, carry):
        @pl.when(k >= slots)
        def _():
            store(k - slots).wait()

        for h in range(2):
            for r, (start, stop, _) in zip((r0, r1), STREAMS):
                stage[k % slots, :, h * HALF + start : h * HALF + stop] = (
                    r[h, k // RING, k % RING].astype(F32) * scale
                )
        store(k).start()
        return carry

    lax.fori_loop(0, count, chunk, 0)
    for h in range(2):
        for r, (start, stop, _) in zip((r0, r1), STREAMS):
            box_out[:, h * HALF + start : h * HALF + stop] = (
                r[h, RING - 1, RING - 1].astype(F32) * scale
            )[0 : 4 * ANCHORS]
    for k in range(count - slots, count):
        store(k).wait()
    tower_copy.wait()


def per_device(
    zl_count, zh_count, tower, cls_weight, cls_bias, box_weight, box_bias, labels, target_index, boxes
):
    nz = zl_count * zh_count
    vmem = pl.BlockSpec(memory_space=pltpu.VMEM)

    def buf(*shape, dtype=BF16):
        return pltpu.VMEM(shape, dtype)

    per_stream = []
    for start, stop, cut in STREAMS:
        width = stop - start
        per = -(-(BLOCK // 8 * (width // COLS)) // nz) * 8
        per_stream += [
            buf(RING, RING, BLOCK, width, dtype=F32),
            buf(2, 2, 2, BLOCK, width),
            buf(2, 2, 2, BLOCK, width),
            buf(2, 2, BLOCK, width),
            buf(2, 2, BLOCK, width),
            buf(RING, BLOCK, width, dtype=F32),
        ]
        for part in (cut, width - cut):
            per_stream += [buf(2, BLOCK, part)] * 2 + [buf(BLOCK, part)] * 2
        per_stream += [buf(nz, per, COLS, dtype=F32)] + [buf(nz, per, COLS)] * 3

    r0, r1, q, s, tower_grad = pl.pallas_call(
        functools.partial(step_kernel, zl_count, zh_count),
        out_shape=(
            buf(2, RING, RING, BLOCK, STREAMS[0][1] - STREAMS[0][0]),
            buf(2, RING, RING, BLOCK, STREAMS[1][1] - STREAMS[1][0]),
            buf(len(STREAMS), 2, RING, RING, 8, COLS, dtype=F32),
            buf(8, COLS, dtype=F32),
            buf(*tower.shape),
        ),
        in_specs=[
            vmem,
            pl.BlockSpec(memory_space=pl.ANY),
            vmem, vmem, vmem, vmem, vmem,
            pl.BlockSpec(memory_space=pltpu.SMEM),
        ],
        out_specs=(vmem, vmem, vmem, vmem, vmem),
        scratch_shapes=[
            buf(CLS, WIDTH),
            buf(PAD_OUTS - CLS, WIDTH),
            buf(8, PAD_OUTS, dtype=F32),
            buf(6, COLS, DEPTH),
            buf(2, 2 * COLS, HALF),
            buf(2 * COLS, HALF),
            buf(PAD_OUTS, 2 * COLS, dtype=F32),
            buf(PAD_OUTS, 2 * COLS, dtype=F32),
            buf(PAD_OUTS, 2 * COLS),
            buf(PAD_OUTS, 2 * COLS),
            buf(2, PAD_OUTS - CLS, COLS, dtype=F32),
            buf(5, 2, 8, COLS, dtype=F32),
            buf(nz, 8, COLS, dtype=F32),
            buf(2 * COLS, WIDTH, dtype=F32),
            buf(2, COLS, DEPTH, dtype=F32),
            buf(2, COLS, DEPTH, dtype=F32),
            pltpu.SemaphoreType.DMA,
            pltpu.SemaphoreType.REGULAR((max(nz // 2 - 1, 1),)),
            pltpu.SemaphoreType.DMA((IN_FLIGHT + GROUPS,)),
            pltpu.SemaphoreType.DMA((RECEIVES,)),
            *per_stream,
        ],
        compiler_params=pltpu.CompilerParams(
            collective_id=0, has_side_effects=True, vmem_limit_bytes=56 * 2**20
        ),
        name="step",
    )(tower, cls_weight, box_weight, cls_bias, box_bias, labels, target_index, boxes)

    hbm = pl.BlockSpec(memory_space=pl.ANY)
    cls_grad, box_grad, loss, cls_bias_grad, box_bias_grad, tower_grad = pl.pallas_call(
        scale_kernel,
        out_shape=(
            jax.ShapeDtypeStruct((CLS, WIDTH), F32),
            jax.ShapeDtypeStruct((OUTS - CLS, WIDTH), F32),
            jax.ShapeDtypeStruct((1, 1), F32),
            jax.ShapeDtypeStruct((8, COLS), F32),
            jax.ShapeDtypeStruct((1, OUTS - CLS), F32),
            jax.ShapeDtypeStruct(tower.shape, BF16),
        ),
        in_specs=[vmem, vmem, vmem, vmem, vmem],
        out_specs=(hbm, vmem, vmem, vmem, vmem, hbm),
        scratch_shapes=[
            buf(4, BLOCK, WIDTH, dtype=F32),
            pltpu.SemaphoreType.DMA((5,)),
        ],
        compiler_params=pltpu.CompilerParams(vmem_limit_bytes=40 * 2**20),
        name="scale",
    )(r0, r1, q, s, tower_grad)
    return (
        loss.reshape(()),
        cls_grad,
        cls_bias_grad.reshape(-1)[:CLS],
        box_grad,
        box_bias_grad.reshape(-1),
        tower_grad,
    )


def solution(mesh):
    zl_count = mesh.shape["tile"] // (2 * RING)
    zh_count = mesh.shape["img"] // RING
    placed = (
        P("img", "tile", None, None),
        P(),
        P(),
        P(),
        P(),
        P("img", None, "tile", None),
        P("img", None, "tile", None),
        P("img", None, None),
    )
    return jax.shard_map(
        functools.partial(per_device, zl_count, zh_count),
        mesh=mesh,
        in_specs=placed,
        out_specs=(P(), P(), P(), P(), P(), P("img", "tile", None, None)),
        check_vma=False,
    )
```

```python
import functools

import jax
import jax.numpy as jnp
import numpy as np
from jax import lax
from jax.experimental import pallas as pl
from jax.experimental.pallas import tpu as pltpu
from jax.sharding import PartitionSpec as P

CLASSES = 80
ANCHORS = 9
STRIDE = 8
FOCAL_ALPHA = 0.25
NORM_EPS = 1e-06

RING = 4
IN_FLIGHT = 40
RECEIVES = 62
GROUPS = 11
CLS = ANCHORS * CLASSES
OUTS = CLS + 4 * ANCHORS
PAD_OUTS = 768
TAPS = 9
DEPTH = 256
WIDTH = TAPS * DEPTH
HALF = WIDTH // 2
COLS = 128
BLOCK = PAD_OUTS // (RING * RING)
STREAMS = ((0, 640), (640, 1152))
BF16 = jnp.bfloat16
F32 = jnp.float32
MESH = pl.DeviceIdType.MESH


def flip(i):
    return i + 1 - 2 * (i % 2)


class Links:
    def __init__(self, send, recv):
        self.send, self.recv = send, recv
        self.sends = self.recvs = 0
        self.sent, self.groups = [], []

    def make(self, src, dst, device, pair=None):
        send_id, recv_id = self.pair() if pair is None else pair
        return pltpu.make_async_remote_copy(
            src_ref=src,
            dst_ref=dst,
            send_sem=self.send.at[send_id],
            recv_sem=self.recv.at[recv_id],
            device_id=device,
            device_id_type=MESH,
        )

    def pair(self):
        self.sends += 1
        self.recvs += 1
        return IN_FLIGHT + self.sends - 1, self.recvs - 1

    def push(self, src, dst, device):
        slot = len(self.sent) % IN_FLIGHT
        if len(self.sent) >= IN_FLIGHT:
            self.sent[-IN_FLIGHT].wait_send()
        self.recvs += 1
        copy = self.make(src, dst, device, (slot, self.recvs - 1))
        copy.start()
        self.sent.append(copy)
        return copy

    def group(self, whole, device):
        pair = self.pair()
        both = self.make(whole, whole, device, pair)
        self.groups.append(both)

        def start(src, dst, to):
            self.make(src, dst, to, pair).start()

        return start, both.wait_recv

    def drain(self):
        for copy in self.sent[-IN_FLIGHT:]:
            copy.wait_send()
        for both in self.groups:
            both.wait_send()


def anchor_sizes():
    ids = np.arange(ANCHORS)
    base = np.float32(4.0 * STRIDE) * np.exp2((ids // 3).astype(np.float32) / np.float32(3.0))
    ratio = (ids % 3 - 1).astype(np.float32) / np.float32(2.0)
    return (base * np.exp2(-ratio)).astype(np.float32), (base * np.exp2(ratio)).astype(np.float32)


def box_terms(offsets, assigned, corners, first_row):
    shape = assigned.shape
    ids = lax.broadcasted_iota(jnp.int32, shape, 0)
    lanes = lax.broadcasted_iota(jnp.int32, shape, 1)
    widths, heights = anchor_sizes()
    anchor_w = jnp.zeros(shape, F32)
    anchor_h = jnp.zeros(shape, F32)
    for a in range(ANCHORS):
        anchor_w = jnp.where(ids == a, float(widths[a]), anchor_w)
        anchor_h = jnp.where(ids == a, float(heights[a]), anchor_h)
    second = (lanes >= COLS).astype(jnp.int32)
    centre_y = ((first_row + second).astype(F32) + 0.5) * STRIDE
    centre_x = ((lanes - COLS * second).astype(F32) + 0.5) * STRIDE
    true_left, true_top, true_right, true_bottom = corners
    positive = (assigned >= 0).astype(F32)

    def each(o0, o1, o2, o3):
        middle_x = centre_x + o0 * anchor_w
        middle_y = centre_y + o1 * anchor_h
        pred_width = anchor_w * jnp.exp(o2)
        pred_height = anchor_h * jnp.exp(o3)
        pred_left = middle_x - 0.5 * pred_width
        pred_right = middle_x + 0.5 * pred_width
        pred_top = middle_y - 0.5 * pred_height
        pred_bottom = middle_y + 0.5 * pred_height
        crossing_w = jnp.maximum(
            jnp.minimum(pred_right, true_right) - jnp.maximum(pred_left, true_left), 0.0
        )
        crossing_h = jnp.maximum(
            jnp.minimum(pred_bottom, true_bottom) - jnp.maximum(pred_top, true_top), 0.0
        )
        crossing = crossing_w * crossing_h
        union_area = (
            pred_width * pred_height
            + (true_right - true_left) * (true_bottom - true_top)
            - crossing
        )
        outer_w = jnp.maximum(pred_right, true_right) - jnp.minimum(pred_left, true_left)
        outer_h = jnp.maximum(pred_bottom, true_bottom) - jnp.minimum(pred_top, true_top)
        outer_area = outer_w * outer_h
        giou_value = crossing / union_area - (outer_area - union_area) / outer_area
        return positive * (1.0 - giou_value)

    values, pullback = jax.vjp(each, *offsets)
    return values, pullback(jnp.ones(shape, F32)), positive


def shifted(value, tap):
    if tap == 1:
        return value
    rows = lax.broadcasted_iota(jnp.int32, value.shape, 0)
    if tap == 0:
        return jnp.where(rows == 0, 0.0, pltpu.roll(value, 1, 0))
    return jnp.where(rows == COLS - 1, 0.0, pltpu.roll(value, COLS - 1, 0))


def step_kernel(
    zl_count, zh_count,
    tower_in, wc_in, wb_in, cls_bias_in, box_bias_in, labels_in, tindex_in, boxes_in,
    r_out0, r_out1, q_out, s_out, tg_out,
    tower, w, wb, cls_bias, box_bias, labels, tindex, boxes,
    wbs, bias_row, ext, patches, beside, outs, gf, glow, theirs, boxy,
    small, sz, dpatch, edge_s, edge_r,
    load_sem, ready, across_b, send, recv, *per_stream,
):
    t = lax.axis_index("tile")
    m = lax.axis_index("img")
    tiles = zl_count * RING * 2
    nz = zl_count * zh_count
    c = t % 2
    y = (t // 2) % RING
    x = m // zh_count
    z = (m % zh_count) * zl_count + t // (2 * RING)

    def at(x_, y_, z_, c_):
        return {
            "tile": (z_ % zl_count) * (2 * RING) + y_ * 2 + c_,
            "img": x_ * zh_count + z_ // zl_count,
        }

    a = x + c * (y - x)
    b = y + c * (x - y)

    def ring(a_, b_):
        return at(a_ + c * (b_ - a_), b_ + c * (a_ - b_), z, c)

    sibling = at(x, y, z, 1 - c)
    outer = {"tile": t + 2 * c - 1, "img": m}
    has_outer = jnp.where(c == 0, t > 0, t < tiles - 1)
    links = Links(send, recv)

    barrier = pltpu.get_barrier_semaphore()

    def greet(device):
        pl.semaphore_signal(barrier, inc=1, device_id=device, device_id_type=MESH)

    greet(sibling)
    for near in (flip(a), 3 - a):
        greet(ring(near, b))
    for near in (flip(b), 3 - b):
        greet(ring(a, near))
    beside_z = (at(x, y, (z + 1) % nz, c), at(x, y, (z + nz - 1) % nz, c))
    for device in beside_z:
        greet(device)

    @pl.when(has_outer)
    def _():
        greet(outer)

    loads = [
        pltpu.make_async_copy(src, dst, load_sem.at[k])
        for k, (src, dst) in enumerate((
            (tindex_in, tindex), (boxes_in, boxes), (tower_in, tower), (wb_in, wb),
            (wc_in, w), (cls_bias_in, cls_bias), (box_bias_in, box_bias), (labels_in, labels),
        ))
    ]
    for load in loads:
        load.start()
    for load in loads[:4]:
        load.wait()

    wanted = jnp.concatenate([tindex[0, :, 0, :], tindex[0, :, 1, :]], axis=1)

    def pick(n, found):
        hit = wanted == n
        return tuple(jnp.where(hit, boxes[0, j, n], found[j]) for j in range(4))

    zero = jnp.zeros(wanted.shape, F32)
    corners = lax.fori_loop(0, boxes.shape[2], pick, (zero, zero, zero, zero))
    wbs[...] = jnp.zeros(wbs.shape, BF16)
    wbs[0 : 4 * ANCHORS, :] = wb[...]

    def fill(row, place, halves, put):
        value = row.astype(F32)
        for col_tap in range(3):
            piece = shifted(value, col_tap).astype(BF16)
            for here in range(2):
                row_tap = place - here
                if 0 <= row_tap <= 2:
                    for part in range(2):
                        k = (3 * row_tap + col_tap) * DEPTH + part * COLS
                        if k // HALF in halves:
                            put(
                                k // HALF,
                                slice(here * COLS, (here + 1) * COLS),
                                slice(k % HALF, k % HALF + COLS),
                                piece[:, part * COLS : (part + 1) * COLS],
                            )

    def put_own(half, rows, cols, value):
        patches[half, rows, cols] = value

    def put_beside(half, rows, cols, value):
        beside[rows, cols] = value

    for here in range(2):
        ext[1 + 2 * c + here] = tower[0, here]
        fill(tower[0, here], 1 + here, (0, 1), put_own)

    pl.semaphore_wait(barrier, 1 + 4 + 2 + has_outer.astype(jnp.int32))

    rounds = nz // 2 - 1

    def tell(k):
        if k < rounds:
            for device in beside_z:
                pl.semaphore_signal(ready.at[k], inc=1, device_id=device, device_id_type=MESH)

    def hear(k):
        if k < rounds:
            pl.semaphore_wait(ready.at[k], 2)
            tell(k + 1)

    halo = links.make(tower.at[0, c], ext.at[5 * (1 - c)], outer)

    @pl.when(has_outer)
    def _():
        halo.start()

    @pl.when(jnp.logical_not(has_outer))
    def _():
        ext[5 * c] = jnp.zeros(ext.shape[1:], BF16)

    rows_across = links.push(tower.at[0], ext.at[pl.ds(1 + 2 * c, 2)], sibling)
    tell(0)
    for near in (flip(b), 3 - b):
        pl.semaphore_signal(across_b, inc=1, device_id=ring(a, near), device_id_type=MESH)

    nt = (((1,), (1,)), ((), ()))

    def product(lhs, rhs):
        return lax.dot_general(lhs, rhs, nt, preferred_element_type=F32)

    def column(values):
        wide = jnp.broadcast_to(values, (8, values.shape[1]))
        return jnp.transpose(wide)[:, 0:1]

    edge = 3 * DEPTH
    patches[0, 0:COLS, 0:edge] = jnp.zeros((COLS, edge), BF16)
    patches[1, COLS : 2 * COLS, HALF - edge : HALF] = jnp.zeros((COLS, edge), BF16)
    for load in loads[4:]:
        load.wait()
    bias_row[0:1, 0:CLS] = cls_bias[...].reshape(1, CLS)
    bias_row[0:1, CLS:OUTS] = box_bias[...].reshape(1, OUTS - CLS)
    bias_row[0:1, OUTS:PAD_OUTS] = jnp.zeros((1, PAD_OUTS - OUTS), F32)
    bias_col = column(bias_row[0:1, :])
    for lhs, rows in ((w, slice(0, CLS)), (wbs, slice(CLS, PAD_OUTS))):
        outs[rows, :] = (
            product(lhs[:, 0:HALF], patches[0])
            + product(lhs[:, HALF:WIDTH], patches[1])
            + bias_col[rows]
        )

    rows_across.wait_recv()

    @pl.when(has_outer)
    def _():
        halo.wait_recv()

    outer_across = links.push(ext.at[5 * c], ext.at[5 * c], sibling)
    fill(ext[2 * c], 0, (0, 1), put_own)
    fill(ext[2 * c + 3], 3, (0, 1), put_own)
    for lhs, rows in ((w, slice(0, CLS)), (wbs, slice(CLS, PAD_OUTS))):
        outs[rows, 0:COLS] += product(lhs[:, 0:edge], patches[0, 0:COLS, 0:edge])
        outs[rows, COLS : 2 * COLS] += product(
            lhs[:, WIDTH - edge : WIDTH], patches[1, COLS : 2 * COLS, HALF - edge : HALF]
        )
    hear(0)

    class_ids = lax.broadcasted_iota(jnp.int32, (CLASSES, COLS), 0)

    def focal(anchor, total):
        rows = pl.ds(pl.multiple_of(anchor * CLASSES, CLASSES), CLASSES)
        for here in range(2):
            lanes = slice(here * COLS, (here + 1) * COLS)
            score = outs[rows, lanes]
            label = labels[0, anchor, here : here + 1, :]
            hit = jnp.broadcast_to(label, (CLASSES, COLS)) == class_ids
            counted = (label >= -1).astype(F32)
            side = jnp.where(hit, score, -score)
            small_e = jnp.exp(-jnp.abs(score))
            inverse = 1.0 / (1.0 + small_e)
            log_p = jnp.minimum(side, 0.0) - jnp.log1p(small_e)
            right = side >= 0
            p = jnp.where(right, inverse, small_e * inverse)
            miss = jnp.where(right, small_e * inverse, inverse)
            alpha = jnp.where(hit, FOCAL_ALPHA, FOCAL_ALPHA - 1.0) * counted
            weight = alpha * miss * miss
            grad = weight * (2.0 * p * log_p - miss)
            value = -jnp.abs(weight) * log_p
            gf[rows, lanes] = grad
            glow[rows, lanes] = grad.astype(BF16)
            total = total + jnp.sum(value.reshape(CLASSES // 8, 8, COLS), axis=0)
        return total

    focal_sum = lax.fori_loop(0, ANCHORS, focal, jnp.zeros((8, COLS), F32))

    assigned = jnp.concatenate([labels[0, :, 0, :], labels[0, :, 1, :]], axis=1)
    for here in range(2):
        boxy[here] = outs[CLS:PAD_OUTS, here * COLS : (here + 1) * COLS]
    offsets = [
        jnp.concatenate([boxy[here, pl.ds(j, ANCHORS, stride=4), :] for here in range(2)], axis=1)
        for j in range(4)
    ]
    giou, offset_grads, positive = box_terms(offsets, assigned, corners, 2 * t)
    boxy[...] = jnp.zeros(boxy.shape, F32)
    for here in range(2):
        lanes = slice(here * COLS, (here + 1) * COLS)
        for j in range(4):
            boxy[here, pl.ds(j, ANCHORS, stride=4), :] = offset_grads[j][:, lanes]
        gf[CLS:PAD_OUTS, lanes] = boxy[here]
    glow[CLS:PAD_OUTS, :] = gf[CLS:PAD_OUTS, :].astype(BF16)
    glow_across = links.push(glow, theirs, sibling)

    streams = []
    each = len(per_stream) // len(STREAMS)
    for k, (start, stop) in enumerate(STREAMS):
        streams.append(((r_out0, r_out1)[k], start, stop, *per_stream[k * each : (k + 1) * each]))
    for _, start, stop, acc, *_ in streams:
        part = jnp.dot(glow[...], patches[c, :, start:stop], preferred_element_type=F32)
        acc[...] = part.reshape(acc.shape)
    hear(1)
    outer_across.wait_recv()
    for half in range(2):

        @pl.when(c == half)
        def _():
            for place in range(4):
                fill(ext[2 * (1 - half) + place], place, (half,), put_beside)

    glow_across.wait_recv()

    def wrap(i):
        return (i + RING) % RING

    far_first = sorted(range(1, nz), key=lambda k: -min(k, nz - k))
    groups = BLOCK // 8
    shared = []

    def square(k, h, a_, b_):
        r = streams[k][0]
        value = r[h, a_, b_].astype(F32)
        value = jnp.sum((value * value).reshape(groups, 8, value.shape[1]), axis=0)
        total = value[:, 0:COLS]
        for j in range(1, value.shape[1] // COLS):
            total = total + value[:, j * COLS : (j + 1) * COLS]
        q_out[k, h, a_, b_] = total

    def stream(
        number, r, start, stop,
        acc, a1s, a1r, a2s, a2r, accb, b_s, b_r, zf, zs, zr, zg,
    ):
        width = stop - start
        part = jnp.dot(theirs[...], beside[:, start:stop], preferred_element_type=F32)
        acc[...] += part.reshape(acc.shape)

        steps = ((flip(a), 3 - a), (3 - a, flip(a)))
        first = {}
        for which in (1, 0):
            for s in range(2):
                near, far = steps[s]
                back = (3 - near, flip(near))[s]
                quarter = back if which else near
                for j in range(2):
                    a1s[s, which, j] = acc[quarter, 2 * s + j].astype(BF16)
                first[s, which] = links.push(a1s.at[s, which], a1r.at[s, which], ring(near, b))
        yield

        second = []
        for s in range(2):
            near, far = steps[s]
            first[s, 1].wait_recv()
            for j in range(2):
                a2s[s, j] = (acc[far, 2 * s + j] + a1r[s, 1, j].astype(F32)).astype(BF16)
            second.append(links.push(a2s.at[s], a2r.at[s], ring(far, b)))
        yield

        for s in range(2):
            first[s, 0].wait_recv()
            second[s].wait_recv()
            for j in range(2):
                accb[2 * s + j] = (
                    acc[a, 2 * s + j] + a1r[s, 0, j].astype(F32) + a2r[s, j].astype(F32)
                )

        turn, arrived = links.group(b_r, ring(a, wrap(b + 1)))
        for k in (2, 1, 3):
            b_s[k - 1] = accb[wrap(b + k)].astype(BF16)
            turn(b_s.at[k - 1], b_r.at[k - 1], ring(a, wrap(b + k)))
        yield

        per = zf.shape[1] // 8
        zf[...] = jnp.zeros(zf.shape, F32)
        arrived()
        done = accb[b] + b_r[0].astype(F32) + b_r[1].astype(F32) + b_r[2].astype(F32)
        for k in range(width // COLS):
            for g in range(groups):
                n = k * groups + g
                zf[n // per, (n % per) * 8 : (n % per) * 8 + 8, :] = done[
                    g * 8 : g * 8 + 8, k * COLS : (k + 1) * COLS
                ]

        zs[...] = zf[...].astype(BF16)
        turn, arrived = links.group(zr.at[pl.ds(0, nz - 1)], beside_z[0])
        for k in far_first:
            turn(zs.at[(z + k) % nz], zr.at[z], at(x, y, (z + k) % nz, c))
        yield

        arrived()
        total = zf[z]
        for k in range(1, nz):
            total = total + zr[(z + nz - k) % nz].astype(F32)
        zg[z] = total.astype(BF16)
        turn, arrived = links.group(zg.at[pl.ds(0, nz - 1)], beside_z[0])
        for k in far_first:
            turn(zg.at[z], zg.at[z], at(x, y, (z + k) % nz, c))
        yield

        arrived()
        zf[...] = zg[...].astype(F32)
        for k in range(width // COLS):
            pieces = []
            for g in range(groups):
                n = k * groups + g
                pieces.append(zf[n // per, (n % per) * 8 : (n % per) * 8 + 8, :])
            r[c, a, b, :, k * COLS : (k + 1) * COLS] = jnp.concatenate(pieces, axis=0).astype(BF16)

        across, all_across = links.group(r.at[1 - c], sibling)
        shared.append(all_across)

        def share(a_, b_):
            across(r.at[c, a_, b_], r.at[c, a_, b_], sibling)
            square(number, c, a_, b_)

        def along_a(b_):
            block = r.at[c, a, b_]
            return (
                links.push(block, block, ring(wrap(a + 1), b)),
                links.push(block, block, ring(wrap(a - 1), b)),
            )

        block = r.at[c, a, b]
        wide = [along_a(b)]
        to = {k: links.push(block, block, ring(a, wrap(b + k))) for k in (1, 3, 2)}
        share(a, b)
        yield

        for k in (1, 3):
            to[k].wait_recv()
            wide.append(along_a(wrap(b - k)))
            share(a, wrap(b - k))
        yield

        to[2].wait_recv()
        wide.append(along_a(wrap(b + 2)))
        share(a, wrap(b + 2))
        yield

        order = (b, wrap(b - 1), wrap(b + 1), wrap(b + 2))
        rest = []
        for k, b_ in enumerate(order):
            wide[k][0].wait_recv()
            if k < 2:
                block = r.at[c, wrap(a - 1), b_]
                rest.append(links.push(block, block, ring(wrap(a + 1), b)))
            share(wrap(a - 1), b_)
            wide[k][1].wait_recv()
            if k >= 2:
                block = r.at[c, wrap(a + 1), b_]
                rest.append(links.push(block, block, ring(wrap(a - 1), b)))
            share(wrap(a + 1), b_)
            yield
        for k, b_ in enumerate(order):
            rest[k].wait_recv()
            share(wrap(a + 2), b_)
            yield

    going = [stream(k, *refs) for k, refs in enumerate(streams)]

    def step():
        for one in going:
            next(one, None)

    step()
    hear(2)

    tn = (((0,), (0,)), ((), ()))
    dpatch[...] = lax.dot_general(
        glow[0:CLS, :], w[...], tn, preferred_element_type=F32
    ) + lax.dot_general(glow[CLS:PAD_OUTS, :], wbs[...], tn, preferred_element_type=F32)

    def reach(row_tap, here):
        total = None
        for col_tap in range(3):
            k = (3 * row_tap + col_tap) * DEPTH
            piece = shifted(dpatch[here * COLS : (here + 1) * COLS, k : k + DEPTH], 2 - col_tap)
            total = piece if total is None else total + piece
        return total

    edge_s[0] = reach(0, 0)
    edge_s[1] = reach(2, 1)
    edge_out = links.make(edge_s.at[c], edge_r.at[1 - c], outer)
    edge_in = links.push(edge_s.at[1 - c], edge_r.at[c], sibling)

    @pl.when(has_outer)
    def _():
        edge_out.start()

    @pl.when(jnp.logical_not(has_outer))
    def _():
        edge_r[c] = jnp.zeros(edge_r.shape[1:], F32)

    sums = lax.dot_general(
        jnp.ones((8, 2 * COLS), F32), gf[...], nt,
        precision=lax.Precision.HIGHEST, preferred_element_type=F32,
    )
    lane = lax.broadcasted_iota(jnp.int32, (1, COLS), 1)
    mine = jnp.zeros((8, COLS), F32)
    rows8 = lax.broadcasted_iota(jnp.int32, (8, COLS), 0)
    for k in range(PAD_OUTS // COLS):
        mine = jnp.where(rows8 == k, sums[:, k * COLS : (k + 1) * COLS], mine)
    scalars = (jnp.sum(focal_sum), jnp.sum(giou), jnp.sum(positive))
    for k, value in enumerate(scalars):
        mine = jnp.where((rows8 == 6) & (lane == k), value, mine)
    stages = (sibling,) + tuple(ring(n, b) for n in (flip(a), 3 - a)) + tuple(
        ring(a, n) for n in (flip(b), 3 - b)
    )
    doubling = []

    def double(k):
        if k == 0:
            small[0, 0] = mine
        else:
            doubling[k - 1].wait_recv()
            small[k, 0] = small[k - 1, 0] + small[k - 1, 1]
        doubling.append(links.push(small.at[k, 0], small.at[k, 1], stages[k]))

    double(0)
    step()
    double(1)

    tg_own = (reach(1, 0) + reach(0, 1), reach(2, 0) + reach(1, 1))
    edge_in.wait_recv()

    @pl.when(has_outer)
    def _():
        edge_out.wait_recv()

    for here in range(2):
        tg_out[0, here] = (tg_own[here] + edge_r[here]).astype(BF16)

    pl.semaphore_wait(across_b, 2)
    step()
    double(2)
    step()
    double(3)
    step()
    double(4)
    step()
    doubling[4].wait_recv()
    sz[z] = small[4, 0] + small[4, 1]
    turn, small_arrived = links.group(sz.at[pl.ds(0, nz - 1)], beside_z[0])
    for k in far_first:
        turn(sz.at[z], sz.at[z], at(x, y, (z + k) % nz, c))
    step()
    step()
    for _ in range(2 * RING + 1):
        step()

    small_arrived()
    whole = sz[0]
    for k in range(1, nz):
        whole = whole + sz[k]
    s_out[...] = whole

    for all_across in shared:
        all_across()

    def other(i, carry):
        for k in range(len(STREAMS)):
            square(k, 1 - c, i // RING, i % RING)
        return carry

    lax.fori_loop(0, RING * RING, other, 0)
    links.drain()

    @pl.when(has_outer)
    def _():
        halo.wait_send()
        edge_out.wait_send()


def scale_kernel(r0, r1, q, s, tg, cls_out, box_out, loss_out, cls_bias_out, box_bias_out, tg_out, stage, sem):
    slots = stage.shape[0]
    tower_copy = pltpu.make_async_copy(tg, tg_out, sem.at[slots])
    tower_copy.start()
    rows8 = lax.broadcasted_iota(jnp.int32, (8, COLS), 0)
    bias = jnp.where(rows8 < PAD_OUTS // COLS, s[...], 0.0)
    total = bias * bias
    for k in range(len(STREAMS)):
        for n in range(2 * RING * RING):
            total = total + q[k, n // (RING * RING), n // RING % RING, n % RING]
    total = jnp.sum(total, keepdims=True)
    scale = lax.rsqrt(total / (OUTS * (WIDTH + 1)) + NORM_EPS)
    bias = bias * scale
    cls_bias_out[...] = bias
    at_row, at_lane = CLS // COLS, CLS % COLS
    box_bias_out[...] = pltpu.roll(bias, COLS - at_lane, 1)[at_row : at_row + 1, 0 : OUTS - CLS]
    loss_out[...] = (s[6:7, 0:1] + s[6:7, 1:2]) / s[6:7, 2:3]

    count = CLS // BLOCK

    def store(k):
        return pltpu.make_async_copy(
            stage.at[k % slots],
            cls_out.at[pl.ds(pl.multiple_of(k * BLOCK, BLOCK), BLOCK)],
            sem.at[k % slots],
        )

    def chunk(k, carry):
        @pl.when(k >= slots)
        def _():
            store(k - slots).wait()

        for h in range(2):
            for r, (start, stop) in zip((r0, r1), STREAMS):
                stage[k % slots, :, h * HALF + start : h * HALF + stop] = (
                    r[h, k // RING, k % RING].astype(F32) * scale
                )
        store(k).start()
        return carry

    lax.fori_loop(0, count, chunk, 0)
    for h in range(2):
        for r, (start, stop) in zip((r0, r1), STREAMS):
            box_out[:, h * HALF + start : h * HALF + stop] = (
                r[h, RING - 1, RING - 1].astype(F32) * scale
            )[0 : 4 * ANCHORS]
    for k in range(count - slots, count):
        store(k).wait()
    tower_copy.wait()


def per_device(
    zl_count, zh_count, tower, cls_weight, cls_bias, box_weight, box_bias, labels, target_index, boxes
):
    nz = zl_count * zh_count
    vmem = pl.BlockSpec(memory_space=pltpu.VMEM)
    hbm = pl.BlockSpec(memory_space=pl.ANY)

    def buf(*shape, dtype=BF16):
        return pltpu.VMEM(shape, dtype)

    per_stream = []
    for start, stop in STREAMS:
        width = stop - start
        per = -(-(BLOCK // 8 * (width // COLS)) // nz) * 8
        per_stream += [
            buf(RING, RING, BLOCK, width, dtype=F32),
            buf(2, 2, 2, BLOCK, width),
            buf(2, 2, 2, BLOCK, width),
            buf(2, 2, BLOCK, width),
            buf(2, 2, BLOCK, width),
            buf(RING, BLOCK, width, dtype=F32),
        ]
        per_stream += [buf(RING - 1, BLOCK, width)] * 2
        per_stream += [buf(nz, per, COLS, dtype=F32)] + [buf(nz, per, COLS)] * 3

    r0, r1, q, s, tower_grad = pl.pallas_call(
        functools.partial(step_kernel, zl_count, zh_count),
        out_shape=(
            buf(2, RING, RING, BLOCK, STREAMS[0][1] - STREAMS[0][0]),
            buf(2, RING, RING, BLOCK, STREAMS[1][1] - STREAMS[1][0]),
            buf(len(STREAMS), 2, RING, RING, 8, COLS, dtype=F32),
            buf(8, COLS, dtype=F32),
            buf(*tower.shape),
        ),
        in_specs=[hbm] * 8,
        out_specs=(vmem, vmem, vmem, vmem, vmem),
        scratch_shapes=[
            buf(*tower.shape),
            buf(CLS, WIDTH),
            buf(*box_weight.shape),
            buf(*cls_bias.shape, dtype=F32),
            buf(*box_bias.shape, dtype=F32),
            buf(*labels.shape, dtype=jnp.int32),
            buf(*target_index.shape, dtype=jnp.int32),
            pltpu.SMEM(boxes.shape, F32),
            buf(PAD_OUTS - CLS, WIDTH),
            buf(8, PAD_OUTS, dtype=F32),
            buf(6, COLS, DEPTH),
            buf(2, 2 * COLS, HALF),
            buf(2 * COLS, HALF),
            buf(PAD_OUTS, 2 * COLS, dtype=F32),
            buf(PAD_OUTS, 2 * COLS, dtype=F32),
            buf(PAD_OUTS, 2 * COLS),
            buf(PAD_OUTS, 2 * COLS),
            buf(2, PAD_OUTS - CLS, COLS, dtype=F32),
            buf(5, 2, 8, COLS, dtype=F32),
            buf(nz, 8, COLS, dtype=F32),
            buf(2 * COLS, WIDTH, dtype=F32),
            buf(2, COLS, DEPTH, dtype=F32),
            buf(2, COLS, DEPTH, dtype=F32),
            pltpu.SemaphoreType.DMA((8,)),
            pltpu.SemaphoreType.REGULAR((max(nz // 2 - 1, 1),)),
            pltpu.SemaphoreType.REGULAR,
            pltpu.SemaphoreType.DMA((IN_FLIGHT + GROUPS,)),
            pltpu.SemaphoreType.DMA((RECEIVES,)),
            *per_stream,
        ],
        compiler_params=pltpu.CompilerParams(
            collective_id=0, has_side_effects=True, vmem_limit_bytes=56 * 2**20
        ),
        name="step",
    )(tower, cls_weight, box_weight, cls_bias, box_bias, labels, target_index, boxes)

    cls_grad, box_grad, loss, cls_bias_grad, box_bias_grad, tower_grad = pl.pallas_call(
        scale_kernel,
        out_shape=(
            jax.ShapeDtypeStruct((CLS, WIDTH), F32),
            jax.ShapeDtypeStruct((OUTS - CLS, WIDTH), F32),
            jax.ShapeDtypeStruct((1, 1), F32),
            jax.ShapeDtypeStruct((8, COLS), F32),
            jax.ShapeDtypeStruct((1, OUTS - CLS), F32),
            jax.ShapeDtypeStruct(tower.shape, BF16),
        ),
        in_specs=[vmem, vmem, vmem, vmem, vmem],
        out_specs=(hbm, vmem, vmem, vmem, vmem, hbm),
        scratch_shapes=[
            buf(4, BLOCK, WIDTH, dtype=F32),
            pltpu.SemaphoreType.DMA((5,)),
        ],
        compiler_params=pltpu.CompilerParams(vmem_limit_bytes=40 * 2**20),
        name="scale",
    )(r0, r1, q, s, tower_grad)
    return (
        loss.reshape(()),
        cls_grad,
        cls_bias_grad.reshape(-1)[:CLS],
        box_grad,
        box_bias_grad.reshape(-1),
        tower_grad,
    )


def solution(mesh):
    zl_count = mesh.shape["tile"] // (2 * RING)
    zh_count = mesh.shape["img"] // RING
    placed = (
        P("img", "tile", None, None),
        P(),
        P(),
        P(),
        P(),
        P("img", None, "tile", None),
        P("img", None, "tile", None),
        P("img", None, None),
    )
    return jax.shard_map(
        functools.partial(per_device, zl_count, zh_count),
        mesh=mesh,
        in_specs=placed,
        out_specs=(P(), P(), P(), P(), P(), P("img", "tile", None, None)),
        check_vma=False,
    )
```

```python
import functools

import jax
import jax.numpy as jnp
import numpy as np
from jax import lax
from jax.experimental import pallas as pl
from jax.experimental.pallas import tpu as pltpu
from jax.sharding import PartitionSpec as P

CLASSES = 80
ANCHORS = 9
STRIDE = 8
FOCAL_ALPHA = 0.25
NORM_EPS = 1e-06

RING = 4
IN_FLIGHT = 32
RECEIVES = 85
GROUPS = 18
CLS = ANCHORS * CLASSES
OUTS = CLS + 4 * ANCHORS
PAD_OUTS = 768
TAPS = 9
DEPTH = 256
WIDTH = TAPS * DEPTH
HALF = WIDTH // 2
COLS = 128
BLOCK = PAD_OUTS // (RING * RING)
STREAMS = ((0, 384), (384, 768), (768, 1152))
BF16 = jnp.bfloat16
F32 = jnp.float32
MESH = pl.DeviceIdType.MESH


def flip(i):
    return i + 1 - 2 * (i % 2)


class Links:
    def __init__(self, send, recv):
        self.send, self.recv = send, recv
        self.sends = self.recvs = 0
        self.sent, self.groups = [], []

    def make(self, src, dst, device, pair=None):
        send_id, recv_id = self.pair() if pair is None else pair
        return pltpu.make_async_remote_copy(
            src_ref=src,
            dst_ref=dst,
            send_sem=self.send.at[send_id],
            recv_sem=self.recv.at[recv_id],
            device_id=device,
            device_id_type=MESH,
        )

    def pair(self):
        self.sends += 1
        self.recvs += 1
        return IN_FLIGHT + self.sends - 1, self.recvs - 1

    def push(self, src, dst, device):
        slot = len(self.sent) % IN_FLIGHT
        if len(self.sent) >= IN_FLIGHT:
            self.sent[-IN_FLIGHT].wait_send()
        self.recvs += 1
        copy = self.make(src, dst, device, (slot, self.recvs - 1))
        copy.start()
        self.sent.append(copy)
        return copy

    def group(self, whole, device):
        pair = self.pair()
        both = self.make(whole, whole, device, pair)
        self.groups.append(both)

        def start(src, dst, to):
            self.make(src, dst, to, pair).start()

        return start, both.wait_recv

    def drain(self):
        for copy in self.sent[-IN_FLIGHT:]:
            copy.wait_send()
        for both in self.groups:
            both.wait_send()


def anchor_sizes():
    ids = np.arange(ANCHORS)
    base = np.float32(4.0 * STRIDE) * np.exp2((ids // 3).astype(np.float32) / np.float32(3.0))
    ratio = (ids % 3 - 1).astype(np.float32) / np.float32(2.0)
    return (base * np.exp2(-ratio)).astype(np.float32), (base * np.exp2(ratio)).astype(np.float32)


def box_terms(offsets, assigned, corners, first_row):
    shape = assigned.shape
    ids = lax.broadcasted_iota(jnp.int32, shape, 0)
    lanes = lax.broadcasted_iota(jnp.int32, shape, 1)
    widths, heights = anchor_sizes()
    anchor_w = jnp.zeros(shape, F32)
    anchor_h = jnp.zeros(shape, F32)
    for a in range(ANCHORS):
        anchor_w = jnp.where(ids == a, float(widths[a]), anchor_w)
        anchor_h = jnp.where(ids == a, float(heights[a]), anchor_h)
    second = (lanes >= COLS).astype(jnp.int32)
    centre_y = ((first_row + second).astype(F32) + 0.5) * STRIDE
    centre_x = ((lanes - COLS * second).astype(F32) + 0.5) * STRIDE
    true_left, true_top, true_right, true_bottom = corners
    positive = (assigned >= 0).astype(F32)

    def each(o0, o1, o2, o3):
        middle_x = centre_x + o0 * anchor_w
        middle_y = centre_y + o1 * anchor_h
        pred_width = anchor_w * jnp.exp(o2)
        pred_height = anchor_h * jnp.exp(o3)
        pred_left = middle_x - 0.5 * pred_width
        pred_right = middle_x + 0.5 * pred_width
        pred_top = middle_y - 0.5 * pred_height
        pred_bottom = middle_y + 0.5 * pred_height
        crossing_w = jnp.maximum(
            jnp.minimum(pred_right, true_right) - jnp.maximum(pred_left, true_left), 0.0
        )
        crossing_h = jnp.maximum(
            jnp.minimum(pred_bottom, true_bottom) - jnp.maximum(pred_top, true_top), 0.0
        )
        crossing = crossing_w * crossing_h
        union_area = (
            pred_width * pred_height
            + (true_right - true_left) * (true_bottom - true_top)
            - crossing
        )
        outer_w = jnp.maximum(pred_right, true_right) - jnp.minimum(pred_left, true_left)
        outer_h = jnp.maximum(pred_bottom, true_bottom) - jnp.minimum(pred_top, true_top)
        outer_area = outer_w * outer_h
        giou_value = crossing / union_area - (outer_area - union_area) / outer_area
        return positive * (1.0 - giou_value)

    values, pullback = jax.vjp(each, *offsets)
    return values, pullback(jnp.ones(shape, F32)), positive


def shifted(value, tap):
    if tap == 1:
        return value
    rows = lax.broadcasted_iota(jnp.int32, value.shape, 0)
    if tap == 0:
        return jnp.where(rows == 0, 0.0, pltpu.roll(value, 1, 0))
    return jnp.where(rows == COLS - 1, 0.0, pltpu.roll(value, COLS - 1, 0))


def step_kernel(
    zl_count, zh_count,
    tower_in, wc_in, wb_in, cls_bias_in, box_bias_in, labels_in, tindex_in, boxes_in,
    *refs,
):
    r_outs, (s_out, tg_out), refs = refs[: len(STREAMS)], refs[len(STREAMS) :][:2], refs[len(STREAMS) + 2 :]
    (
        tower, w, wb, cls_bias, box_bias, labels, tindex, boxes,
        wbs, bias_row, ext, patches, beside, outs, gf, glow, theirs, boxy,
        small_c, small_a, small_b, sz, dpatch, edge_s, edge_r,
        load_sem, ready, across_a, across_b, send, recv, *per_stream,
    ) = refs
    t = lax.axis_index("tile")
    m = lax.axis_index("img")
    tiles = zl_count * RING * 2
    nz = zl_count * zh_count
    c = t % 2
    y = (t // 2) % RING
    x = m // zh_count
    z = (m % zh_count) * zl_count + t // (2 * RING)

    def at(x_, y_, z_, c_):
        return {
            "tile": (z_ % zl_count) * (2 * RING) + y_ * 2 + c_,
            "img": x_ * zh_count + z_ // zl_count,
        }

    a = x + c * (y - x)
    b = y + c * (x - y)

    def ring(a_, b_):
        return at(a_ + c * (b_ - a_), b_ + c * (a_ - b_), z, c)

    sibling = at(x, y, z, 1 - c)
    outer = {"tile": t + 2 * c - 1, "img": m}
    has_outer = jnp.where(c == 0, t > 0, t < tiles - 1)
    links = Links(send, recv)

    barrier = pltpu.get_barrier_semaphore()

    def greet(device):
        pl.semaphore_signal(barrier, inc=1, device_id=device, device_id_type=MESH)

    greet(sibling)
    for near in (flip(a), 3 - a):
        greet(ring(near, b))
    for near in (flip(b), 3 - b):
        greet(ring(a, near))
    beside_z = (at(x, y, (z + 1) % nz, c), at(x, y, (z + nz - 1) % nz, c))
    for device in beside_z:
        greet(device)

    @pl.when(has_outer)
    def _():
        greet(outer)

    loads = [
        pltpu.make_async_copy(src, dst, load_sem.at[k])
        for k, (src, dst) in enumerate((
            (tindex_in, tindex), (boxes_in, boxes), (tower_in, tower), (wb_in, wb),
            (wc_in, w), (cls_bias_in, cls_bias), (box_bias_in, box_bias), (labels_in, labels),
        ))
    ]
    for load in loads:
        load.start()
    for load in loads[:4]:
        load.wait()

    wanted = jnp.concatenate([tindex[0, :, 0, :], tindex[0, :, 1, :]], axis=1)

    def pick(n, found):
        hit = wanted == n
        return tuple(jnp.where(hit, boxes[0, j, n], found[j]) for j in range(4))

    zero = jnp.zeros(wanted.shape, F32)
    corners = lax.fori_loop(0, boxes.shape[2], pick, (zero, zero, zero, zero))
    wbs[...] = jnp.zeros(wbs.shape, BF16)
    wbs[0 : 4 * ANCHORS, :] = wb[...]

    def fill(row, place, halves, put):
        value = row.astype(F32)
        for col_tap in range(3):
            piece = shifted(value, col_tap).astype(BF16)
            for here in range(2):
                row_tap = place - here
                if 0 <= row_tap <= 2:
                    for part in range(2):
                        k = (3 * row_tap + col_tap) * DEPTH + part * COLS
                        if k // HALF in halves:
                            put(
                                k // HALF,
                                slice(here * COLS, (here + 1) * COLS),
                                slice(k % HALF, k % HALF + COLS),
                                piece[:, part * COLS : (part + 1) * COLS],
                            )

    def put_own(half, rows, cols, value):
        patches[half, rows, cols] = value

    def put_beside(half, rows, cols, value):
        beside[rows, cols] = value

    for here in range(2):
        ext[1 + 2 * c + here] = tower[0, here]
        fill(tower[0, here], 1 + here, (0, 1), put_own)

    pl.semaphore_wait(barrier, 1 + 4 + 2 + has_outer.astype(jnp.int32))

    rounds = nz // 2 - 1

    def tell(k):
        if k < rounds:
            for device in beside_z:
                pl.semaphore_signal(ready.at[k], inc=1, device_id=device, device_id_type=MESH)

    def hear(k):
        if k < rounds:
            pl.semaphore_wait(ready.at[k], 2)
            tell(k + 1)

    halo = links.make(tower.at[0, c], ext.at[5 * (1 - c)], outer)

    @pl.when(has_outer)
    def _():
        halo.start()

    @pl.when(jnp.logical_not(has_outer))
    def _():
        ext[5 * c] = jnp.zeros(ext.shape[1:], BF16)

    rows_across = links.push(tower.at[0], ext.at[pl.ds(1 + 2 * c, 2)], sibling)
    tell(0)
    for near in (flip(a), 3 - a):
        pl.semaphore_signal(across_a, inc=1, device_id=ring(near, b), device_id_type=MESH)
    for near in (flip(b), 3 - b):
        pl.semaphore_signal(across_b, inc=1, device_id=ring(a, near), device_id_type=MESH)

    nt = (((1,), (1,)), ((), ()))

    def product(lhs, rhs):
        return lax.dot_general(lhs, rhs, nt, preferred_element_type=F32)

    def column(values):
        wide = jnp.broadcast_to(values, (8, values.shape[1]))
        return jnp.transpose(wide)[:, 0:1]

    edge = 3 * DEPTH
    outer_part = (
        (0, slice(0, COLS), slice(0, edge), slice(0, edge)),
        (1, slice(COLS, 2 * COLS), slice(HALF - edge, HALF), slice(WIDTH - edge, WIDTH)),
    )
    for load in loads[4:]:
        load.wait()
    bias_row[0:1, 0:CLS] = cls_bias[...].reshape(1, CLS)
    bias_row[0:1, CLS:OUTS] = box_bias[...].reshape(1, OUTS - CLS)
    bias_row[0:1, OUTS:PAD_OUTS] = jnp.zeros((1, PAD_OUTS - OUTS), F32)
    bias_col = column(bias_row[0:1, :])
    rows_across.wait_recv()
    for half in range(2):

        @pl.when(c == half)
        def _():
            part, positions, cols, _ = outer_part[half]
            patches[part, positions, cols] = jnp.zeros((COLS, edge), BF16)
            fill(ext[2 * half + 3 - 3 * half], 3 - 3 * half, (0, 1), put_own)

    both = ((w, slice(0, CLS)), (wbs, slice(CLS, PAD_OUTS)))
    for lhs, rows in both:
        outs[rows, :] = (
            product(lhs[:, 0:HALF], patches[0])
            + product(lhs[:, HALF:WIDTH], patches[1])
            + bias_col[rows]
        )

    @pl.when(has_outer)
    def _():
        halo.wait_recv()

    outer_across = links.push(ext.at[5 * c], ext.at[5 * c], sibling)
    for half in range(2):

        @pl.when(c == half)
        def _():
            part, positions, cols, weights = outer_part[half]
            fill(ext[5 * half], 3 * half, (0, 1), put_own)
            for lhs, rows in both:
                outs[rows, positions] += product(lhs[:, weights], patches[part, positions, cols])

    hear(0)

    class_ids = lax.broadcasted_iota(jnp.int32, (CLASSES, COLS), 0)

    def focal(anchor, total):
        rows = pl.ds(pl.multiple_of(anchor * CLASSES, CLASSES), CLASSES)
        for here in range(2):
            lanes = slice(here * COLS, (here + 1) * COLS)
            score = outs[rows, lanes]
            label = labels[0, anchor, here : here + 1, :]
            hit = jnp.broadcast_to(label, (CLASSES, COLS)) == class_ids
            counted = (label >= -1).astype(F32)
            side = jnp.where(hit, score, -score)
            small_e = jnp.exp(-jnp.abs(score))
            inverse = 1.0 / (1.0 + small_e)
            log_p = jnp.minimum(side, 0.0) - jnp.log1p(small_e)
            right = side >= 0
            p = jnp.where(right, inverse, small_e * inverse)
            miss = jnp.where(right, small_e * inverse, inverse)
            alpha = jnp.where(hit, FOCAL_ALPHA, FOCAL_ALPHA - 1.0) * counted
            weight = alpha * miss * miss
            grad = weight * (2.0 * p * log_p - miss)
            value = -jnp.abs(weight) * log_p
            gf[rows, lanes] = grad
            glow[rows, lanes] = grad.astype(BF16)
            total = total + jnp.sum(value.reshape(CLASSES // 8, 8, COLS), axis=0)
        return total

    focal_sum = lax.fori_loop(0, ANCHORS, focal, jnp.zeros((8, COLS), F32))

    assigned = jnp.concatenate([labels[0, :, 0, :], labels[0, :, 1, :]], axis=1)
    for here in range(2):
        boxy[here] = outs[CLS:PAD_OUTS, here * COLS : (here + 1) * COLS]
    offsets = [
        jnp.concatenate([boxy[here, pl.ds(j, ANCHORS, stride=4), :] for here in range(2)], axis=1)
        for j in range(4)
    ]
    giou, offset_grads, positive = box_terms(offsets, assigned, corners, 2 * t)
    boxy[...] = jnp.zeros(boxy.shape, F32)
    for here in range(2):
        lanes = slice(here * COLS, (here + 1) * COLS)
        for j in range(4):
            boxy[here, pl.ds(j, ANCHORS, stride=4), :] = offset_grads[j][:, lanes]
        gf[CLS:PAD_OUTS, lanes] = boxy[here]
    glow[CLS:PAD_OUTS, :] = gf[CLS:PAD_OUTS, :].astype(BF16)
    glow_across = links.push(glow, theirs, sibling)

    streams = []
    each = len(per_stream) // len(STREAMS)
    for k, (start, stop) in enumerate(STREAMS):
        streams.append((r_outs[k], start, stop, *per_stream[k * each : (k + 1) * each]))

    def own_part(k):
        _, start, stop, acc, *_ = streams[k]
        part = jnp.dot(glow[...], patches[c, :, start:stop], preferred_element_type=F32)
        acc[...] = part.reshape(acc.shape)

    own_part(0)
    hear(1)
    outer_across.wait_recv()
    for half in range(2):

        @pl.when(c == half)
        def _():
            for place in range(4):
                fill(ext[2 * (1 - half) + place], place, (half,), put_beside)

    glow_across.wait_recv()

    def wrap(i):
        return (i + RING) % RING

    far_first = sorted(range(1, nz), key=lambda k: -min(k, nz - k))
    groups = BLOCK // 8
    shared = []

    squares = []

    def stream(
        number, r, start, stop,
        acc, a1s, a1r, a2s, a2r, accb, b_s, b_r, zf, zs, zr, zg,
    ):
        width = stop - start
        if number:
            own_part(number)
        part = jnp.dot(theirs[...], beside[:, start:stop], preferred_element_type=F32)
        acc[...] += part.reshape(acc.shape)

        steps = ((flip(a), 3 - a), (3 - a, flip(a)))
        first = {}
        for which in (1, 0):
            for s in range(2):
                near, far = steps[s]
                back = (3 - near, flip(near))[s]
                quarter = back if which else near
                for j in range(2):
                    a1s[s, which, j] = acc[quarter, 2 * s + j].astype(BF16)
                first[s, which] = links.push(a1s.at[s, which], a1r.at[s, which], ring(near, b))
        yield

        second = []
        for s in range(2):
            near, far = steps[s]
            first[s, 1].wait_recv()
            for j in range(2):
                a2s[s, j] = (acc[far, 2 * s + j] + a1r[s, 1, j].astype(F32)).astype(BF16)
            second.append(links.push(a2s.at[s], a2r.at[s], ring(far, b)))
        yield

        for s in range(2):
            first[s, 0].wait_recv()
            second[s].wait_recv()
            for j in range(2):
                accb[2 * s + j] = (
                    acc[a, 2 * s + j] + a1r[s, 0, j].astype(F32) + a2r[s, j].astype(F32)
                )

        turn, arrived = links.group(b_r, ring(a, wrap(b + 1)))
        for k in (2, 1, 3):
            b_s[k - 1] = accb[wrap(b + k)].astype(BF16)
            turn(b_s.at[k - 1], b_r.at[k - 1], ring(a, wrap(b + k)))
        yield

        per = zf.shape[1] // 8
        zf[...] = jnp.zeros(zf.shape, F32)
        arrived()
        done = accb[b] + b_r[0].astype(F32) + b_r[1].astype(F32) + b_r[2].astype(F32)
        for k in range(width // COLS):
            for g in range(groups):
                n = k * groups + g
                zf[n // per, (n % per) * 8 : (n % per) * 8 + 8, :] = done[
                    g * 8 : g * 8 + 8, k * COLS : (k + 1) * COLS
                ]

        zs[...] = zf[...].astype(BF16)
        turn, arrived = links.group(zr.at[pl.ds(0, nz - 1)], beside_z[0])
        for k in far_first:
            turn(zs.at[(z + k) % nz], zr.at[z], at(x, y, (z + k) % nz, c))
        yield

        arrived()
        total = zf[z]
        for k in range(1, nz):
            total = total + zr[(z + nz - k) % nz].astype(F32)
        zg[z] = total.astype(BF16)
        squares.append(jnp.sum(total * total))
        turn, arrived = links.group(zg.at[pl.ds(0, nz - 1)], beside_z[0])
        for k in far_first:
            turn(zg.at[z], zg.at[z], at(x, y, (z + k) % nz, c))
        yield

        arrived()
        zf[...] = zg[...].astype(F32)
        for k in range(width // COLS):
            pieces = []
            for g in range(groups):
                n = k * groups + g
                pieces.append(zf[n // per, (n % per) * 8 : (n % per) * 8 + 8, :])
            r[c, a, b, :, k * COLS : (k + 1) * COLS] = jnp.concatenate(pieces, axis=0).astype(BF16)

        across, all_across = links.group(r.at[1 - c], sibling)
        shared.append(all_across)

        def share(a_, b_):
            across(r.at[c, a_, b_], r.at[c, a_, b_], sibling)

        def along_a(b_):
            block = r.at[c, a, b_]
            return (
                links.push(block, block, ring(wrap(a + 1), b)),
                links.push(block, block, ring(wrap(a - 1), b)),
            )

        block = r.at[c, a, b]
        wide = [along_a(b)]
        to = {k: links.push(block, block, ring(a, wrap(b + k))) for k in (1, 3, 2)}
        share(a, b)
        yield

        for k in (1, 3):
            to[k].wait_recv()
            wide.append(along_a(wrap(b - k)))
            share(a, wrap(b - k))
        yield

        to[2].wait_recv()
        wide.append(along_a(wrap(b + 2)))
        share(a, wrap(b + 2))
        yield

        order = (b, wrap(b - 1), wrap(b + 1), wrap(b + 2))
        rest = []
        for k, b_ in enumerate(order):
            wide[k][0].wait_recv()
            if k < 2:
                block = r.at[c, wrap(a - 1), b_]
                rest.append(links.push(block, block, ring(wrap(a + 1), b)))
            share(wrap(a - 1), b_)
            wide[k][1].wait_recv()
            if k >= 2:
                block = r.at[c, wrap(a + 1), b_]
                rest.append(links.push(block, block, ring(wrap(a - 1), b)))
            share(wrap(a + 1), b_)
            yield
        for k, b_ in enumerate(order):
            rest[k].wait_recv()
            share(wrap(a + 2), b_)
            yield

    going = [stream(k, *refs) for k, refs in enumerate(streams)]

    def step():
        for one in going:
            next(one, None)

    step()
    hear(2)

    tn = (((0,), (0,)), ((), ()))
    dpatch[...] = lax.dot_general(
        glow[0:CLS, :], w[...], tn, preferred_element_type=F32
    ) + lax.dot_general(glow[CLS:PAD_OUTS, :], wbs[...], tn, preferred_element_type=F32)

    def reach(row_tap, here):
        total = None
        for col_tap in range(3):
            k = (3 * row_tap + col_tap) * DEPTH
            piece = shifted(dpatch[here * COLS : (here + 1) * COLS, k : k + DEPTH], 2 - col_tap)
            total = piece if total is None else total + piece
        return total

    edge_s[0] = reach(0, 0)
    edge_s[1] = reach(2, 1)
    edge_out = links.make(edge_s.at[c], edge_r.at[1 - c], outer)
    edge_in = links.push(edge_s.at[1 - c], edge_r.at[c], sibling)

    @pl.when(has_outer)
    def _():
        edge_out.start()

    @pl.when(jnp.logical_not(has_outer))
    def _():
        edge_r[c] = jnp.zeros(edge_r.shape[1:], F32)

    sums = lax.dot_general(
        jnp.ones((8, 2 * COLS), F32), gf[...], nt,
        precision=lax.Precision.HIGHEST, preferred_element_type=F32,
    )
    lane = lax.broadcasted_iota(jnp.int32, (1, COLS), 1)
    mine = jnp.zeros((8, COLS), F32)
    rows8 = lax.broadcasted_iota(jnp.int32, (8, COLS), 0)
    for k in range(PAD_OUTS // COLS):
        mine = jnp.where(rows8 == k, sums[:, k * COLS : (k + 1) * COLS], mine)
    def add_up(stage):
        slots, here, devices = (
            (small_c, c, (sibling,)),
            (small_a, a, tuple(ring(wrap(a + k), b) for k in (2, 1, 3))),
            (small_b, b, tuple(ring(a, wrap(b + k)) for k in (2, 1, 3))),
            (sz, z, tuple(at(x, y, (z + k) % nz, c) for k in far_first)),
        )[stage]
        if stage == 0:
            total = mine
            scalars = (jnp.sum(focal_sum), jnp.sum(giou), jnp.sum(positive), sum(squares))
            for n, value in enumerate(scalars):
                total = jnp.where((rows8 == 6) & (lane == n), value, total)
        else:
            total = added()
        slots[here] = total
        count = len(devices)
        turn, arrived = links.group(slots.at[pl.ds(0, count)], devices[0])
        for device in devices:
            turn(slots.at[here], slots.at[here], device)

        def result():
            arrived()
            total = slots[0]
            for k in range(1, count + 1):
                total = total + slots[k]
            return total

        return result

    step()

    tg_own = (reach(1, 0) + reach(0, 1), reach(2, 0) + reach(1, 1))
    edge_in.wait_recv()

    @pl.when(has_outer)
    def _():
        edge_out.wait_recv()

    for here in range(2):
        tg_out[0, here] = (tg_own[here] + edge_r[here]).astype(BF16)

    pl.semaphore_wait(across_a, 2)
    pl.semaphore_wait(across_b, 2)
    step()
    step()
    step()
    added = add_up(0)
    step()
    added = add_up(1)
    step()
    added = add_up(2)
    step()
    step()
    added = add_up(3)
    for _ in range(2 * RING):
        step()
    s_out[...] = added()
    for all_across in shared:
        all_across()

    links.drain()

    @pl.when(has_outer)
    def _():
        halo.wait_send()
        edge_out.wait_send()


def scale_kernel(*refs):
    rs, refs = refs[: len(STREAMS)], refs[len(STREAMS) :]
    s, tg, cls_out, box_out, loss_out, cls_bias_out, box_bias_out, tg_out, *refs = refs
    stage, box_stage, loss, cls_bias, box_bias, sem, rest = refs
    others = [
        pltpu.make_async_copy(src, dst, rest.at[k])
        for k, (src, dst) in enumerate((
            (tg, tg_out), (box_stage, box_out), (loss, loss_out),
            (cls_bias, cls_bias_out), (box_bias, box_bias_out),
        ))
    ]
    others[0].start()
    rows8 = lax.broadcasted_iota(jnp.int32, (8, COLS), 0)
    bias = jnp.where(rows8 < PAD_OUTS // COLS, s[...], 0.0)
    total = s[6:7, 3:4] + jnp.sum(bias * bias, keepdims=True)
    scale = lax.rsqrt(total / (OUTS * (WIDTH + 1)) + NORM_EPS)

    def scaled(k, put):
        for h in range(2):
            for r, (start, stop) in zip(rs, STREAMS):
                put(
                    slice(h * HALF + start, h * HALF + stop),
                    r[h, k // RING, k % RING].astype(F32) * scale,
                )

    def chunk(k, carry):
        rows = pl.ds(pl.multiple_of(k * BLOCK, BLOCK), BLOCK)

        def put(cols, value):
            stage[rows, cols] = value

        scaled(k, put)
        pltpu.make_async_copy(stage.at[rows], cls_out.at[rows], sem).start()
        return carry

    def put_box(cols, value):
        box_stage[:, cols] = value[0 : OUTS - CLS]

    lax.fori_loop(0, CLS // BLOCK, chunk, 0)
    scaled(CLS // BLOCK, put_box)
    bias = bias * scale
    cls_bias[...] = bias
    at_row, at_lane = CLS // COLS, CLS % COLS
    box_bias[...] = pltpu.roll(bias, COLS - at_lane, 1)[at_row : at_row + 1, 0 : OUTS - CLS]
    loss[...] = (s[6:7, 0:1] + s[6:7, 1:2]) / s[6:7, 2:3]
    for copy in others[1:]:
        copy.start()
    pltpu.make_async_copy(stage, cls_out, sem).wait()
    for copy in others:
        copy.wait()


def per_device(
    zl_count, zh_count, tower, cls_weight, cls_bias, box_weight, box_bias, labels, target_index, boxes
):
    nz = zl_count * zh_count
    vmem = pl.BlockSpec(memory_space=pltpu.VMEM)
    hbm = pl.BlockSpec(memory_space=pl.ANY)

    def buf(*shape, dtype=BF16):
        return pltpu.VMEM(shape, dtype)

    per_stream = []
    for start, stop in STREAMS:
        width = stop - start
        per = -(-(BLOCK // 8 * (width // COLS)) // nz) * 8
        per_stream += [
            buf(RING, RING, BLOCK, width, dtype=F32),
            buf(2, 2, 2, BLOCK, width),
            buf(2, 2, 2, BLOCK, width),
            buf(2, 2, BLOCK, width),
            buf(2, 2, BLOCK, width),
            buf(RING, BLOCK, width, dtype=F32),
        ]
        per_stream += [buf(RING - 1, BLOCK, width)] * 2
        per_stream += [buf(nz, per, COLS, dtype=F32)] + [buf(nz, per, COLS)] * 3

    *rs, s, tower_grad = pl.pallas_call(
        functools.partial(step_kernel, zl_count, zh_count),
        out_shape=(
            *(buf(2, RING, RING, BLOCK, stop - start) for start, stop in STREAMS),
            buf(8, COLS, dtype=F32),
            buf(*tower.shape),
        ),
        in_specs=[hbm] * 8,
        out_specs=(vmem,) * (len(STREAMS) + 2),
        scratch_shapes=[
            buf(*tower.shape),
            buf(CLS, WIDTH),
            buf(*box_weight.shape),
            buf(*cls_bias.shape, dtype=F32),
            buf(*box_bias.shape, dtype=F32),
            buf(*labels.shape, dtype=jnp.int32),
            buf(*target_index.shape, dtype=jnp.int32),
            pltpu.SMEM(boxes.shape, F32),
            buf(PAD_OUTS - CLS, WIDTH),
            buf(8, PAD_OUTS, dtype=F32),
            buf(6, COLS, DEPTH),
            buf(2, 2 * COLS, HALF),
            buf(2 * COLS, HALF),
            buf(PAD_OUTS, 2 * COLS, dtype=F32),
            buf(PAD_OUTS, 2 * COLS, dtype=F32),
            buf(PAD_OUTS, 2 * COLS),
            buf(PAD_OUTS, 2 * COLS),
            buf(2, PAD_OUTS - CLS, COLS, dtype=F32),
            buf(2, 8, COLS, dtype=F32),
            buf(RING, 8, COLS, dtype=F32),
            buf(RING, 8, COLS, dtype=F32),
            buf(nz, 8, COLS, dtype=F32),
            buf(2 * COLS, WIDTH, dtype=F32),
            buf(2, COLS, DEPTH, dtype=F32),
            buf(2, COLS, DEPTH, dtype=F32),
            pltpu.SemaphoreType.DMA((8,)),
            pltpu.SemaphoreType.REGULAR((max(nz // 2 - 1, 1),)),
            pltpu.SemaphoreType.REGULAR,
            pltpu.SemaphoreType.REGULAR,
            pltpu.SemaphoreType.DMA((IN_FLIGHT + GROUPS,)),
            pltpu.SemaphoreType.DMA((RECEIVES,)),
            *per_stream,
        ],
        compiler_params=pltpu.CompilerParams(
            collective_id=0, has_side_effects=True, vmem_limit_bytes=56 * 2**20
        ),
        name="step",
    )(tower, cls_weight, box_weight, cls_bias, box_bias, labels, target_index, boxes)

    cls_grad, box_grad, loss, cls_bias_grad, box_bias_grad, tower_grad = pl.pallas_call(
        scale_kernel,
        out_shape=(
            jax.ShapeDtypeStruct((CLS, WIDTH), F32),
            jax.ShapeDtypeStruct((OUTS - CLS, WIDTH), F32),
            jax.ShapeDtypeStruct((1, 1), F32),
            jax.ShapeDtypeStruct((8, COLS), F32),
            jax.ShapeDtypeStruct((1, OUTS - CLS), F32),
            jax.ShapeDtypeStruct(tower.shape, BF16),
        ),
        in_specs=[vmem] * (len(STREAMS) + 2),
        out_specs=(hbm,) * 6,
        scratch_shapes=[
            buf(CLS, WIDTH, dtype=F32),
            buf(OUTS - CLS, WIDTH, dtype=F32),
            buf(1, 1, dtype=F32),
            buf(8, COLS, dtype=F32),
            buf(1, OUTS - CLS, dtype=F32),
            pltpu.SemaphoreType.DMA,
            pltpu.SemaphoreType.DMA((5,)),
        ],
        compiler_params=pltpu.CompilerParams(vmem_limit_bytes=40 * 2**20),
        name="scale",
    )(*rs, s, tower_grad)
    return (
        loss.reshape(()),
        cls_grad,
        cls_bias_grad.reshape(-1)[:CLS],
        box_grad,
        box_bias_grad.reshape(-1),
        tower_grad,
    )


def solution(mesh):
    zl_count = mesh.shape["tile"] // (2 * RING)
    zh_count = mesh.shape["img"] // RING
    placed = (
        P("img", "tile", None, None),
        P(),
        P(),
        P(),
        P(),
        P("img", None, "tile", None),
        P("img", None, "tile", None),
        P("img", None, None),
    )
    return jax.shard_map(
        functools.partial(per_device, zl_count, zh_count),
        mesh=mesh,
        in_specs=placed,
        out_specs=(P(), P(), P(), P(), P(), P("img", "tile", None, None)),
        check_vma=False,
    )
```

```python
import functools

import jax
import jax.numpy as jnp
import numpy as np
from jax import lax
from jax.experimental import pallas as pl
from jax.experimental.pallas import tpu as pltpu
from jax.sharding import PartitionSpec as P

CLASSES = 80
ANCHORS = 9
STRIDE = 8
FOCAL_ALPHA = 0.25
NORM_EPS = 1e-06

RING = 4
IN_FLIGHT = 16
RECEIVES = 55
APART = 5
CLS = ANCHORS * CLASSES
OUTS = CLS + 4 * ANCHORS
PAD_OUTS = 768
TAPS = 9
DEPTH = 256
WIDTH = TAPS * DEPTH
HALF = WIDTH // 2
COLS = 128
BLOCK = PAD_OUTS // (RING * RING)
STREAMS = ((0, 384), (384, 768), (768, 1152))
BF16 = jnp.bfloat16
F32 = jnp.float32
MESH = pl.DeviceIdType.MESH


def flip(i):
    return i + 1 - 2 * (i % 2)


class Links:
    def __init__(self, send, recv):
        self.send, self.recv = send, recv
        self.apart = self.recvs = 0
        self.ring, self.kept = [], []

    def make(self, src, dst, device, pair=None):
        send_id, recv_id = self.pair(True) if pair is None else pair
        return pltpu.make_async_remote_copy(
            src_ref=src,
            dst_ref=dst,
            send_sem=self.send.at[send_id],
            recv_sem=self.recv.at[recv_id],
            device_id=device,
            device_id_type=MESH,
        )

    def pair(self, apart):
        self.recvs += 1
        if apart:
            self.apart += 1
            return IN_FLIGHT + self.apart - 1, self.recvs - 1
        if len(self.ring) >= IN_FLIGHT:
            self.ring[-IN_FLIGHT].wait_send()
        return len(self.ring) % IN_FLIGHT, self.recvs - 1

    def push(self, src, dst, device):
        copy = self.make(src, dst, device, self.pair(False))
        copy.start()
        self.ring.append(copy)
        return copy

    def group(self, whole, device, apart=False):
        pair = self.pair(apart)
        both = self.make(whole, whole, device, pair)
        (self.kept if apart else self.ring).append(both)

        def start(src, dst, to):
            self.make(src, dst, to, pair).start()

        return start, both.wait_recv

    def drain(self):
        for both in self.ring[-IN_FLIGHT:] + self.kept:
            both.wait_send()


def anchor_sizes():
    ids = np.arange(ANCHORS)
    base = np.float32(4.0 * STRIDE) * np.exp2((ids // 3).astype(np.float32) / np.float32(3.0))
    ratio = (ids % 3 - 1).astype(np.float32) / np.float32(2.0)
    return (base * np.exp2(-ratio)).astype(np.float32), (base * np.exp2(ratio)).astype(np.float32)


def box_terms(offsets, assigned, corners, first_row):
    shape = assigned.shape
    ids = lax.broadcasted_iota(jnp.int32, shape, 0)
    lanes = lax.broadcasted_iota(jnp.int32, shape, 1)
    widths, heights = anchor_sizes()
    anchor_w = jnp.zeros(shape, F32)
    anchor_h = jnp.zeros(shape, F32)
    for a in range(ANCHORS):
        anchor_w = jnp.where(ids == a, float(widths[a]), anchor_w)
        anchor_h = jnp.where(ids == a, float(heights[a]), anchor_h)
    second = (lanes >= COLS).astype(jnp.int32)
    centre_y = ((first_row + second).astype(F32) + 0.5) * STRIDE
    centre_x = ((lanes - COLS * second).astype(F32) + 0.5) * STRIDE
    true_left, true_top, true_right, true_bottom = corners
    positive = (assigned >= 0).astype(F32)

    def each(o0, o1, o2, o3):
        middle_x = centre_x + o0 * anchor_w
        middle_y = centre_y + o1 * anchor_h
        pred_width = anchor_w * jnp.exp(o2)
        pred_height = anchor_h * jnp.exp(o3)
        pred_left = middle_x - 0.5 * pred_width
        pred_right = middle_x + 0.5 * pred_width
        pred_top = middle_y - 0.5 * pred_height
        pred_bottom = middle_y + 0.5 * pred_height
        crossing_w = jnp.maximum(
            jnp.minimum(pred_right, true_right) - jnp.maximum(pred_left, true_left), 0.0
        )
        crossing_h = jnp.maximum(
            jnp.minimum(pred_bottom, true_bottom) - jnp.maximum(pred_top, true_top), 0.0
        )
        crossing = crossing_w * crossing_h
        union_area = (
            pred_width * pred_height
            + (true_right - true_left) * (true_bottom - true_top)
            - crossing
        )
        outer_w = jnp.maximum(pred_right, true_right) - jnp.minimum(pred_left, true_left)
        outer_h = jnp.maximum(pred_bottom, true_bottom) - jnp.minimum(pred_top, true_top)
        outer_area = outer_w * outer_h
        giou_value = crossing / union_area - (outer_area - union_area) / outer_area
        return positive * (1.0 - giou_value)

    values, pullback = jax.vjp(each, *offsets)
    return values, pullback(jnp.ones(shape, F32)), positive


def shifted(value, tap):
    if tap == 1:
        return value
    rows = lax.broadcasted_iota(jnp.int32, value.shape, 0)
    if tap == 0:
        return jnp.where(rows == 0, 0.0, pltpu.roll(value, 1, 0))
    return jnp.where(rows == COLS - 1, 0.0, pltpu.roll(value, COLS - 1, 0))


def step_kernel(
    zl_count, zh_count,
    tower_in, wc_in, wb_in, cls_bias_in, box_bias_in, labels_in, tindex_in, boxes_in,
    *refs,
):
    r_outs, (s_out, tg_out), refs = refs[: len(STREAMS)], refs[len(STREAMS) :][:2], refs[len(STREAMS) + 2 :]
    (
        tower, w, wb, cls_bias, box_bias, labels, tindex, boxes,
        wbs, bias_row, ext, patches, beside, outs, gf, glow, theirs, boxy,
        small_c, small_a, small_b, sz, dpatch, edge_s, edge_r,
        load_sem, ready, across_a, across_b, send, recv, *per_stream,
    ) = refs
    t = lax.axis_index("tile")
    m = lax.axis_index("img")
    tiles = zl_count * RING * 2
    nz = zl_count * zh_count
    c = t % 2
    y = (t // 2) % RING
    x = m // zh_count
    z = (m % zh_count) * zl_count + t // (2 * RING)

    def at(x_, y_, z_, c_):
        return {
            "tile": (z_ % zl_count) * (2 * RING) + y_ * 2 + c_,
            "img": x_ * zh_count + z_ // zl_count,
        }

    a = x + c * (y - x)
    b = y + c * (x - y)

    def ring(a_, b_):
        return at(a_ + c * (b_ - a_), b_ + c * (a_ - b_), z, c)

    sibling = at(x, y, z, 1 - c)
    outer = {"tile": t + 2 * c - 1, "img": m}
    has_outer = jnp.where(c == 0, t > 0, t < tiles - 1)
    links = Links(send, recv)

    barrier = pltpu.get_barrier_semaphore()

    def greet(device):
        pl.semaphore_signal(barrier, inc=1, device_id=device, device_id_type=MESH)

    greet(sibling)
    for near in (flip(a), 3 - a):
        greet(ring(near, b))
    for near in (flip(b), 3 - b):
        greet(ring(a, near))
    beside_z = (at(x, y, (z + 1) % nz, c), at(x, y, (z + nz - 1) % nz, c))
    for device in beside_z:
        greet(device)

    @pl.when(has_outer)
    def _():
        greet(outer)

    loads = [
        pltpu.make_async_copy(src, dst, load_sem.at[k])
        for k, (src, dst) in enumerate((
            (tower_in, tower), (tindex_in, tindex), (boxes_in, boxes), (wb_in, wb),
            (wc_in, w), (cls_bias_in, cls_bias), (box_bias_in, box_bias), (labels_in, labels),
        ))
    ]
    for load in loads:
        load.start()
    def fill(row, place, halves, put):
        value = row.astype(F32)
        for col_tap in range(3):
            piece = shifted(value, col_tap).astype(BF16)
            for here in range(2):
                row_tap = place - here
                if 0 <= row_tap <= 2:
                    for part in range(2):
                        k = (3 * row_tap + col_tap) * DEPTH + part * COLS
                        if k // HALF in halves:
                            put(
                                k // HALF,
                                slice(here * COLS, (here + 1) * COLS),
                                slice(k % HALF, k % HALF + COLS),
                                piece[:, part * COLS : (part + 1) * COLS],
                            )

    def put_own(half, rows, cols, value):
        patches[half, rows, cols] = value

    def put_beside(half, rows, cols, value):
        beside[rows, cols] = value

    wbs[...] = jnp.zeros(wbs.shape, BF16)
    loads[0].wait()
    pl.semaphore_wait(barrier, 1 + 4 + 2 + has_outer.astype(jnp.int32))

    rounds = nz // 2 - 1

    def tell(k):
        if k < rounds:
            for device in beside_z:
                pl.semaphore_signal(ready.at[k], inc=1, device_id=device, device_id_type=MESH)

    def hear(k):
        if k < rounds:
            pl.semaphore_wait(ready.at[k], 2)
            tell(k + 1)

    halo = links.make(tower.at[0, c], ext.at[5 * (1 - c)], outer)

    @pl.when(has_outer)
    def _():
        halo.start()

    @pl.when(jnp.logical_not(has_outer))
    def _():
        ext[5 * c] = jnp.zeros(ext.shape[1:], BF16)

    rows_across = links.push(tower.at[0], ext.at[pl.ds(1 + 2 * c, 2)], sibling)
    tell(0)
    for near in (flip(a), 3 - a):
        pl.semaphore_signal(across_a, inc=1, device_id=ring(near, b), device_id_type=MESH)
    for near in (flip(b), 3 - b):
        pl.semaphore_signal(across_b, inc=1, device_id=ring(a, near), device_id_type=MESH)

    for here in range(2):
        ext[1 + 2 * c + here] = tower[0, here]
        fill(tower[0, here], 1 + here, (0, 1), put_own)

    for load in loads[1:4]:
        load.wait()

    wanted = jnp.concatenate([tindex[0, :, 0, :], tindex[0, :, 1, :]], axis=1)

    def pick(n, found):
        hit = wanted == n
        return tuple(jnp.where(hit, boxes[0, j, n], found[j]) for j in range(4))

    zero = jnp.zeros(wanted.shape, F32)
    corners = lax.fori_loop(0, boxes.shape[2], pick, (zero, zero, zero, zero), unroll=5)
    wbs[0 : 4 * ANCHORS, :] = wb[...]

    nt = (((1,), (1,)), ((), ()))

    def product(lhs, rhs):
        return lax.dot_general(lhs, rhs, nt, preferred_element_type=F32)

    def column(values):
        wide = jnp.broadcast_to(values, (8, values.shape[1]))
        return jnp.transpose(wide)[:, 0:1]

    edge = 3 * DEPTH
    outer_part = (
        (0, slice(0, COLS), slice(0, edge), slice(0, edge)),
        (1, slice(COLS, 2 * COLS), slice(HALF - edge, HALF), slice(WIDTH - edge, WIDTH)),
    )
    for load in loads[4:]:
        load.wait()
    bias_row[0:1, 0:CLS] = cls_bias[...].reshape(1, CLS)
    bias_row[0:1, CLS:OUTS] = box_bias[...].reshape(1, OUTS - CLS)
    bias_row[0:1, OUTS:PAD_OUTS] = jnp.zeros((1, PAD_OUTS - OUTS), F32)
    bias_col = column(bias_row[0:1, :])
    rows_across.wait_recv()
    for half in range(2):

        @pl.when(c == half)
        def _():
            part, positions, cols, _ = outer_part[half]
            patches[part, positions, cols] = jnp.zeros((COLS, edge), BF16)
            fill(ext[2 * half + 3 - 3 * half], 3 - 3 * half, (0, 1), put_own)

    both = ((w, slice(0, CLS)), (wbs, slice(CLS, PAD_OUTS)))
    for lhs, rows in both:
        outs[rows, :] = (
            product(lhs[:, 0:HALF], patches[0])
            + product(lhs[:, HALF:WIDTH], patches[1])
            + bias_col[rows]
        )

    @pl.when(has_outer)
    def _():
        halo.wait_recv()

    outer_across = links.push(ext.at[5 * c], ext.at[5 * c], sibling)
    for half in range(2):

        @pl.when(c == half)
        def _():
            part, positions, cols, weights = outer_part[half]
            fill(ext[5 * half], 3 * half, (0, 1), put_own)
            for lhs, rows in both:
                outs[rows, positions] += product(lhs[:, weights], patches[part, positions, cols])

    hear(0)

    class_ids = lax.broadcasted_iota(jnp.int32, (CLASSES, COLS), 0)

    def focal(anchor, total):
        rows = pl.ds(pl.multiple_of(anchor * CLASSES, CLASSES), CLASSES)
        for here in range(2):
            lanes = slice(here * COLS, (here + 1) * COLS)
            score = outs[rows, lanes]
            label = labels[0, anchor, here : here + 1, :]
            hit = jnp.broadcast_to(label, (CLASSES, COLS)) == class_ids
            counted = (label >= -1).astype(F32)
            side = jnp.where(hit, score, -score)
            small_e = jnp.exp(-jnp.abs(score))
            inverse = 1.0 / (1.0 + small_e)
            log_p = jnp.minimum(side, 0.0) - jnp.log1p(small_e)
            right = side >= 0
            p = jnp.where(right, inverse, small_e * inverse)
            miss = jnp.where(right, small_e * inverse, inverse)
            alpha = jnp.where(hit, FOCAL_ALPHA, FOCAL_ALPHA - 1.0) * counted
            weight = alpha * miss * miss
            grad = weight * (2.0 * p * log_p - miss)
            value = -jnp.abs(weight) * log_p
            gf[rows, lanes] = grad
            glow[rows, lanes] = grad.astype(BF16)
            total = total + jnp.sum(value.reshape(CLASSES // 8, 8, COLS), axis=0)
        return total

    glow_across, glow_arrived = links.group(theirs, sibling)

    def send_grads(start, stop):
        glow_across(glow.at[pl.ds(start, stop - start)], theirs.at[pl.ds(start, stop - start)], sibling)

    focal_sum = jnp.zeros((8, COLS), F32)
    for k in range(3):
        focal_sum = lax.fori_loop(3 * k, 3 * k + 3, focal, focal_sum)
        send_grads(3 * k * CLASSES, 3 * (k + 1) * CLASSES)

    assigned = jnp.concatenate([labels[0, :, 0, :], labels[0, :, 1, :]], axis=1)
    for here in range(2):
        boxy[here] = outs[CLS:PAD_OUTS, here * COLS : (here + 1) * COLS]
    offsets = [
        jnp.concatenate([boxy[here, pl.ds(j, ANCHORS, stride=4), :] for here in range(2)], axis=1)
        for j in range(4)
    ]
    giou, offset_grads, positive = box_terms(offsets, assigned, corners, 2 * t)
    boxy[...] = jnp.zeros(boxy.shape, F32)
    for here in range(2):
        lanes = slice(here * COLS, (here + 1) * COLS)
        for j in range(4):
            boxy[here, pl.ds(j, ANCHORS, stride=4), :] = offset_grads[j][:, lanes]
        gf[CLS:PAD_OUTS, lanes] = boxy[here]
    glow[CLS:PAD_OUTS, :] = gf[CLS:PAD_OUTS, :].astype(BF16)
    send_grads(CLS, PAD_OUTS)

    streams = []
    each = len(per_stream) // len(STREAMS)
    for k, (start, stop) in enumerate(STREAMS):
        streams.append((r_outs[k], start, stop, *per_stream[k * each : (k + 1) * each]))

    def own_part(k):
        _, start, stop, acc, *_ = streams[k]
        part = jnp.dot(glow[...], patches[c, :, start:stop], preferred_element_type=F32)
        acc[...] = part.reshape(acc.shape)

    own_part(0)
    hear(1)
    outer_across.wait_recv()
    for half in range(2):

        @pl.when(c == half)
        def _():
            for place in range(4):
                fill(ext[2 * (1 - half) + place], place, (half,), put_beside)

    glow_arrived()

    def wrap(i):
        return (i + RING) % RING

    far_first = sorted(range(1, nz), key=lambda k: -min(k, nz - k))
    groups = BLOCK // 8
    shared = []

    squares = []

    def stream(
        number, r, start, stop,
        acc, far_s, far_r, own_s, own_r, accb, b_s, b_r, zf, zs, zr, zg,
    ):
        width = stop - start
        if number:
            own_part(number)
        part = jnp.dot(theirs[...], beside[:, start:stop], preferred_element_type=F32)
        acc[...] += part.reshape(acc.shape)

        steps = ((flip(a), 3 - a), (3 - a, flip(a)))
        first = []
        for s in range(2):
            near, far = steps[s]
            for j in range(2):
                far_s[s, j] = acc[(3 - near, flip(near))[s], 2 * s + j].astype(BF16)
            first.append(links.push(far_s.at[s], far_r.at[s], ring(near, b)))
        turn, arrived = links.group(own_r, ring(flip(a), b))
        for s in range(2):
            near, far = steps[s]
            for j in range(2):
                own_s[s, j] = acc[near, 2 * s + j].astype(BF16)
            turn(own_s.at[s], own_r.at[s], ring(near, b))
        yield

        for s in range(2):
            near, far = steps[s]
            first[s].wait_recv()
            for j in range(2):
                own_s[2 + s, j] = (acc[far, 2 * s + j] + far_r[s, j].astype(F32)).astype(BF16)
            turn(own_s.at[2 + s], own_r.at[2 + s], ring(far, b))
        yield

        arrived()
        for s in range(2):
            for j in range(2):
                accb[2 * s + j] = (
                    acc[a, 2 * s + j] + own_r[s, j].astype(F32) + own_r[2 + s, j].astype(F32)
                )

        turn, arrived = links.group(b_r, ring(a, wrap(b + 1)))
        for k in (2, 1, 3):
            b_s[k - 1] = accb[wrap(b + k)].astype(BF16)
            turn(b_s.at[k - 1], b_r.at[k - 1], ring(a, wrap(b + k)))
        yield

        per = zf.shape[1] // 8
        zf[...] = jnp.zeros(zf.shape, F32)
        arrived()
        done = accb[b] + b_r[0].astype(F32) + b_r[1].astype(F32) + b_r[2].astype(F32)
        for k in range(width // COLS):
            for g in range(groups):
                n = k * groups + g
                zf[n // per, (n % per) * 8 : (n % per) * 8 + 8, :] = done[
                    g * 8 : g * 8 + 8, k * COLS : (k + 1) * COLS
                ]

        zs[...] = zf[...].astype(BF16)
        turn, arrived = links.group(zr.at[pl.ds(0, nz - 1)], beside_z[0])
        for k in far_first:
            turn(zs.at[(z + k) % nz], zr.at[z], at(x, y, (z + k) % nz, c))
        yield

        arrived()
        total = zf[z]
        for k in range(1, nz):
            total = total + zr[(z + nz - k) % nz].astype(F32)
        zg[z] = total.astype(BF16)
        squares.append(jnp.sum(total * total))
        turn, arrived = links.group(zg.at[pl.ds(0, nz - 1)], beside_z[0])
        for k in far_first:
            turn(zg.at[z], zg.at[z], at(x, y, (z + k) % nz, c))
        yield

        arrived()
        zf[...] = zg[...].astype(F32)
        for k in range(width // COLS):
            pieces = []
            for g in range(groups):
                n = k * groups + g
                pieces.append(zf[n // per, (n % per) * 8 : (n % per) * 8 + 8, :])
            r[c, a, b, :, k * COLS : (k + 1) * COLS] = jnp.concatenate(pieces, axis=0).astype(BF16)

        across, all_across = links.group(r.at[1 - c], sibling, apart=True)
        shared.append(all_across)

        def share(a_, b_):
            across(r.at[c, a_, b_], r.at[c, a_, b_], sibling)

        def along_a(b_):
            block = r.at[c, a, b_]
            turn, arrived = links.group(r.at[c, a, pl.ds(0, 2)], ring(wrap(a + 1), b))
            turn(block, block, ring(wrap(a + 1), b))
            turn(block, block, ring(wrap(a - 1), b))
            return arrived

        block = r.at[c, a, b]
        wide = [along_a(b)]
        turn, arrived = links.group(r.at[c, a, pl.ds(0, 2)], ring(a, wrap(b + 1)))
        for k in (1, 3):
            turn(block, block, ring(a, wrap(b + k)))
        share(a, b)
        yield

        arrived()
        turn, arrived = links.group(r.at[c, a, b], ring(a, wrap(b + 1)))
        for k, rows in ((1, slice(0, 32)), (3, slice(32, BLOCK))):
            block = r.at[c, a, wrap(b - k), rows]
            turn(block, block, ring(a, wrap(b + k)))
        for k in (1, 3):
            wide.append(along_a(wrap(b - k)))
            share(a, wrap(b - k))
        yield

        arrived()
        wide.append(along_a(wrap(b + 2)))
        share(a, wrap(b + 2))
        yield

        order = (b, wrap(b - 1), wrap(b + 1), wrap(b + 2))
        rest = []
        for k, b_ in enumerate(order):
            wide[k]()
            step = -1 if k < 2 else 1
            if k % 2 == 0:
                turn, arrived = links.group(r.at[c, a, pl.ds(0, 2)], ring(wrap(a - step), b))
                rest.append(arrived)
            block = r.at[c, wrap(a + step), b_]
            turn(block, block, ring(wrap(a - step), b))
            share(wrap(a - 1), b_)
            share(wrap(a + 1), b_)
            yield
        for k in range(2):
            rest[k]()
            for b_ in order[2 * k : 2 * k + 2]:
                share(wrap(a + 2), b_)
            yield

    going = [stream(k, *refs) for k, refs in enumerate(streams)]

    def step(*numbers):
        for k in numbers or range(len(going)):
            next(going[k], None)

    step()
    hear(2)

    tn = (((0,), (0,)), ((), ()))
    dpatch[...] = lax.dot_general(
        glow[0:CLS, :], w[...], tn, preferred_element_type=F32
    ) + lax.dot_general(glow[CLS:PAD_OUTS, :], wbs[...], tn, preferred_element_type=F32)

    def reach(row_tap, here):
        total = None
        for col_tap in range(3):
            k = (3 * row_tap + col_tap) * DEPTH
            piece = shifted(dpatch[here * COLS : (here + 1) * COLS, k : k + DEPTH], 2 - col_tap)
            total = piece if total is None else total + piece
        return total

    edge_s[0] = reach(0, 0)
    edge_s[1] = reach(2, 1)
    edge_out = links.make(edge_s.at[c], edge_r.at[1 - c], outer)
    edge_in = links.push(edge_s.at[1 - c], edge_r.at[c], sibling)

    @pl.when(has_outer)
    def _():
        edge_out.start()

    @pl.when(jnp.logical_not(has_outer))
    def _():
        edge_r[c] = jnp.zeros(edge_r.shape[1:], F32)

    sums = lax.dot_general(
        jnp.ones((8, 2 * COLS), F32), gf[...], nt,
        precision=lax.Precision.HIGHEST, preferred_element_type=F32,
    )
    lane = lax.broadcasted_iota(jnp.int32, (1, COLS), 1)
    mine = jnp.zeros((8, COLS), F32)
    rows8 = lax.broadcasted_iota(jnp.int32, (8, COLS), 0)
    for k in range(PAD_OUTS // COLS):
        mine = jnp.where(rows8 == k, sums[:, k * COLS : (k + 1) * COLS], mine)
    def add_up(stage):
        slots, here, devices = (
            (small_c, c, (sibling,)),
            (small_a, a, tuple(ring(wrap(a + k), b) for k in (2, 1, 3))),
            (small_b, b, tuple(ring(a, wrap(b + k)) for k in (2, 1, 3))),
            (sz, z, tuple(at(x, y, (z + k) % nz, c) for k in far_first)),
        )[stage]
        if stage == 0:
            total = mine
            scalars = (jnp.sum(focal_sum), jnp.sum(giou), jnp.sum(positive), sum(squares))
            for n, value in enumerate(scalars):
                total = jnp.where((rows8 == 6) & (lane == n), value, total)
        else:
            total = added()
        slots[here] = total
        count = len(devices)
        turn, arrived = links.group(slots.at[pl.ds(0, count)], devices[0])
        for device in devices:
            turn(slots.at[here], slots.at[here], device)

        def result():
            arrived()
            total = slots[0]
            for k in range(1, count + 1):
                total = total + slots[k]
            return total

        return result

    step()

    tg_own = (reach(1, 0) + reach(0, 1), reach(2, 0) + reach(1, 1))
    edge_in.wait_recv()

    @pl.when(has_outer)
    def _():
        edge_out.wait_recv()

    for here in range(2):
        tg_out[0, here] = (tg_own[here] + edge_r[here]).astype(BF16)

    pl.semaphore_wait(across_a, 2)
    pl.semaphore_wait(across_b, 2)
    step()
    step()
    step()
    added = add_up(0)
    step()
    added = add_up(1)
    step()
    added = add_up(2)
    step()
    step()
    added = add_up(3)
    for _ in range(RING + 2):
        step()
    s_out[...] = added()
    for all_across in shared:
        all_across()

    links.drain()

    @pl.when(has_outer)
    def _():
        halo.wait_send()
        edge_out.wait_send()


def scale_kernel(*refs):
    rs, refs = refs[: len(STREAMS)], refs[len(STREAMS) :]
    s, tg, cls_out, box_out, loss_out, cls_bias_out, box_bias_out, tg_out, *refs = refs
    stage, box_stage, loss, cls_bias, box_bias, sem, rest = refs
    others = [
        pltpu.make_async_copy(src, dst, rest.at[k])
        for k, (src, dst) in enumerate((
            (tg, tg_out), (box_stage, box_out), (loss, loss_out),
            (cls_bias, cls_bias_out), (box_bias, box_bias_out),
        ))
    ]
    others[0].start()
    rows8 = lax.broadcasted_iota(jnp.int32, (8, COLS), 0)
    bias = jnp.where(rows8 < PAD_OUTS // COLS, s[...], 0.0)
    total = s[6:7, 3:4] + jnp.sum(bias * bias, keepdims=True)
    scale = lax.rsqrt(total / (OUTS * (WIDTH + 1)) + NORM_EPS)

    def scaled(k, put):
        for h in range(2):
            for r, (start, stop) in zip(rs, STREAMS):
                put(
                    slice(h * HALF + start, h * HALF + stop),
                    r[h, k // RING, k % RING].astype(F32) * scale,
                )

    def chunk(k, carry):
        rows = pl.ds(pl.multiple_of(k * BLOCK, BLOCK), BLOCK)

        def put(cols, value):
            stage[rows, cols] = value

        scaled(k, put)
        pltpu.make_async_copy(stage.at[rows], cls_out.at[rows], sem).start()
        return carry

    def put_box(cols, value):
        box_stage[:, cols] = value[0 : OUTS - CLS]

    lax.fori_loop(0, CLS // BLOCK, chunk, 0)
    scaled(CLS // BLOCK, put_box)
    bias = bias * scale
    cls_bias[...] = bias
    at_row, at_lane = CLS // COLS, CLS % COLS
    box_bias[...] = pltpu.roll(bias, COLS - at_lane, 1)[at_row : at_row + 1, 0 : OUTS - CLS]
    loss[...] = (s[6:7, 0:1] + s[6:7, 1:2]) / s[6:7, 2:3]
    for copy in others[1:]:
        copy.start()
    pltpu.make_async_copy(stage, cls_out, sem).wait()
    for copy in others:
        copy.wait()


def per_device(
    zl_count, zh_count, tower, cls_weight, cls_bias, box_weight, box_bias, labels, target_index, boxes
):
    nz = zl_count * zh_count
    vmem = pl.BlockSpec(memory_space=pltpu.VMEM)
    hbm = pl.BlockSpec(memory_space=pl.ANY)

    def buf(*shape, dtype=BF16):
        return pltpu.VMEM(shape, dtype)

    per_stream = []
    for start, stop in STREAMS:
        width = stop - start
        per = -(-(BLOCK // 8 * (width // COLS)) // nz) * 8
        per_stream += [
            buf(RING, RING, BLOCK, width, dtype=F32),
            buf(2, 2, BLOCK, width),
            buf(2, 2, BLOCK, width),
            buf(4, 2, BLOCK, width),
            buf(4, 2, BLOCK, width),
            buf(RING, BLOCK, width, dtype=F32),
        ]
        per_stream += [buf(RING - 1, BLOCK, width)] * 2
        per_stream += [buf(nz, per, COLS, dtype=F32)] + [buf(nz, per, COLS)] * 3

    *rs, s, tower_grad = pl.pallas_call(
        functools.partial(step_kernel, zl_count, zh_count),
        out_shape=(
            *(buf(2, RING, RING, BLOCK, stop - start) for start, stop in STREAMS),
            buf(8, COLS, dtype=F32),
            buf(*tower.shape),
        ),
        in_specs=[hbm] * 8,
        out_specs=(vmem,) * (len(STREAMS) + 2),
        scratch_shapes=[
            buf(*tower.shape),
            buf(CLS, WIDTH),
            buf(*box_weight.shape),
            buf(*cls_bias.shape, dtype=F32),
            buf(*box_bias.shape, dtype=F32),
            buf(*labels.shape, dtype=jnp.int32),
            buf(*target_index.shape, dtype=jnp.int32),
            pltpu.SMEM(boxes.shape, F32),
            buf(PAD_OUTS - CLS, WIDTH),
            buf(8, PAD_OUTS, dtype=F32),
            buf(6, COLS, DEPTH),
            buf(2, 2 * COLS, HALF),
            buf(2 * COLS, HALF),
            buf(PAD_OUTS, 2 * COLS, dtype=F32),
            buf(PAD_OUTS, 2 * COLS, dtype=F32),
            buf(PAD_OUTS, 2 * COLS),
            buf(PAD_OUTS, 2 * COLS),
            buf(2, PAD_OUTS - CLS, COLS, dtype=F32),
            buf(2, 8, COLS, dtype=F32),
            buf(RING, 8, COLS, dtype=F32),
            buf(RING, 8, COLS, dtype=F32),
            buf(nz, 8, COLS, dtype=F32),
            buf(2 * COLS, WIDTH, dtype=F32),
            buf(2, COLS, DEPTH, dtype=F32),
            buf(2, COLS, DEPTH, dtype=F32),
            pltpu.SemaphoreType.DMA((8,)),
            pltpu.SemaphoreType.REGULAR((max(nz // 2 - 1, 1),)),
            pltpu.SemaphoreType.REGULAR,
            pltpu.SemaphoreType.REGULAR,
            pltpu.SemaphoreType.DMA((IN_FLIGHT + APART,)),
            pltpu.SemaphoreType.DMA((RECEIVES,)),
            *per_stream,
        ],
        compiler_params=pltpu.CompilerParams(
            collective_id=0, has_side_effects=True, vmem_limit_bytes=56 * 2**20
        ),
        name="step",
    )(tower, cls_weight, box_weight, cls_bias, box_bias, labels, target_index, boxes)

    cls_grad, box_grad, loss, cls_bias_grad, box_bias_grad, tower_grad = pl.pallas_call(
        scale_kernel,
        out_shape=(
            jax.ShapeDtypeStruct((CLS, WIDTH), F32),
            jax.ShapeDtypeStruct((OUTS - CLS, WIDTH), F32),
            jax.ShapeDtypeStruct((1, 1), F32),
            jax.ShapeDtypeStruct((8, COLS), F32),
            jax.ShapeDtypeStruct((1, OUTS - CLS), F32),
            jax.ShapeDtypeStruct(tower.shape, BF16),
        ),
        in_specs=[vmem] * (len(STREAMS) + 2),
        out_specs=(hbm,) * 6,
        scratch_shapes=[
            buf(CLS, WIDTH, dtype=F32),
            buf(OUTS - CLS, WIDTH, dtype=F32),
            buf(1, 1, dtype=F32),
            buf(8, COLS, dtype=F32),
            buf(1, OUTS - CLS, dtype=F32),
            pltpu.SemaphoreType.DMA,
            pltpu.SemaphoreType.DMA((5,)),
        ],
        compiler_params=pltpu.CompilerParams(vmem_limit_bytes=40 * 2**20),
        name="scale",
    )(*rs, s, tower_grad)
    return (
        loss.reshape(()),
        cls_grad,
        cls_bias_grad.reshape(-1)[:CLS],
        box_grad,
        box_bias_grad.reshape(-1),
        tower_grad,
    )


def solution(mesh):
    zl_count = mesh.shape["tile"] // (2 * RING)
    zh_count = mesh.shape["img"] // RING
    placed = (
        P("img", "tile", None, None),
        P(),
        P(),
        P(),
        P(),
        P("img", None, "tile", None),
        P("img", None, "tile", None),
        P("img", None, None),
    )
    return jax.shard_map(
        functools.partial(per_device, zl_count, zh_count),
        mesh=mesh,
        in_specs=placed,
        out_specs=(P(), P(), P(), P(), P(), P("img", "tile", None, None)),
        check_vma=False,
    )
```

```python
import functools

import jax
import jax.numpy as jnp
import numpy as np
from jax import lax
from jax.experimental import pallas as pl
from jax.experimental.pallas import tpu as pltpu
from jax.sharding import PartitionSpec as P

CLASSES = 80
ANCHORS = 9
STRIDE = 8
FOCAL_ALPHA = 0.25
NORM_EPS = 1e-06

RING = 4
IN_FLIGHT = 16
RECEIVES = 61
APART = 5
CLS = ANCHORS * CLASSES
OUTS = CLS + 4 * ANCHORS
PAD_OUTS = 768
TAPS = 9
DEPTH = 256
WIDTH = TAPS * DEPTH
HALF = WIDTH // 2
COLS = 128
BLOCK = PAD_OUTS // (RING * RING)
STREAMS = ((0, 384), (384, 768), (768, 1152))
BF16 = jnp.bfloat16
F32 = jnp.float32
MESH = pl.DeviceIdType.MESH


def flip(i):
    return i + 1 - 2 * (i % 2)


class Links:
    def __init__(self, send, recv):
        self.send, self.recv = send, recv
        self.apart = self.recvs = 0
        self.ring, self.kept = [], []

    def make(self, src, dst, device, pair=None):
        send_id, recv_id = self.pair(True) if pair is None else pair
        return pltpu.make_async_remote_copy(
            src_ref=src,
            dst_ref=dst,
            send_sem=self.send.at[send_id],
            recv_sem=self.recv.at[recv_id],
            device_id=device,
            device_id_type=MESH,
        )

    def pair(self, apart):
        self.recvs += 1
        if apart:
            self.apart += 1
            return IN_FLIGHT + self.apart - 1, self.recvs - 1
        if len(self.ring) >= IN_FLIGHT:
            self.ring[-IN_FLIGHT].wait_send()
        return len(self.ring) % IN_FLIGHT, self.recvs - 1

    def push(self, src, dst, device):
        copy = self.make(src, dst, device, self.pair(False))
        copy.start()
        self.ring.append(copy)
        return copy

    def group(self, whole, device, apart=False):
        pair = self.pair(apart)
        both = self.make(whole, whole, device, pair)
        (self.kept if apart else self.ring).append(both)

        def start(src, dst, to):
            self.make(src, dst, to, pair).start()

        return start, both.wait_recv

    def drain(self):
        for both in self.ring[-IN_FLIGHT:] + self.kept:
            both.wait_send()


def anchor_sizes():
    ids = np.arange(ANCHORS)
    base = np.float32(4.0 * STRIDE) * np.exp2((ids // 3).astype(np.float32) / np.float32(3.0))
    ratio = (ids % 3 - 1).astype(np.float32) / np.float32(2.0)
    return (base * np.exp2(-ratio)).astype(np.float32), (base * np.exp2(ratio)).astype(np.float32)


def box_terms(offsets, assigned, corners, first_row):
    shape = assigned.shape
    ids = lax.broadcasted_iota(jnp.int32, shape, 0)
    lanes = lax.broadcasted_iota(jnp.int32, shape, 1)
    widths, heights = anchor_sizes()
    anchor_w = jnp.zeros(shape, F32)
    anchor_h = jnp.zeros(shape, F32)
    for a in range(ANCHORS):
        anchor_w = jnp.where(ids == a, float(widths[a]), anchor_w)
        anchor_h = jnp.where(ids == a, float(heights[a]), anchor_h)
    second = (lanes >= COLS).astype(jnp.int32)
    centre_y = ((first_row + second).astype(F32) + 0.5) * STRIDE
    centre_x = ((lanes - COLS * second).astype(F32) + 0.5) * STRIDE
    true_left, true_top, true_right, true_bottom = corners
    positive = (assigned >= 0).astype(F32)

    def each(o0, o1, o2, o3):
        middle_x = centre_x + o0 * anchor_w
        middle_y = centre_y + o1 * anchor_h
        pred_width = anchor_w * jnp.exp(o2)
        pred_height = anchor_h * jnp.exp(o3)
        pred_left = middle_x - 0.5 * pred_width
        pred_right = middle_x + 0.5 * pred_width
        pred_top = middle_y - 0.5 * pred_height
        pred_bottom = middle_y + 0.5 * pred_height
        crossing_w = jnp.maximum(
            jnp.minimum(pred_right, true_right) - jnp.maximum(pred_left, true_left), 0.0
        )
        crossing_h = jnp.maximum(
            jnp.minimum(pred_bottom, true_bottom) - jnp.maximum(pred_top, true_top), 0.0
        )
        crossing = crossing_w * crossing_h
        union_area = (
            pred_width * pred_height
            + (true_right - true_left) * (true_bottom - true_top)
            - crossing
        )
        outer_w = jnp.maximum(pred_right, true_right) - jnp.minimum(pred_left, true_left)
        outer_h = jnp.maximum(pred_bottom, true_bottom) - jnp.minimum(pred_top, true_top)
        outer_area = outer_w * outer_h
        giou_value = crossing / union_area - (outer_area - union_area) / outer_area
        return positive * (1.0 - giou_value)

    values, pullback = jax.vjp(each, *offsets)
    return values, pullback(jnp.ones(shape, F32)), positive


def shifted(value, tap):
    if tap == 1:
        return value
    rows = lax.broadcasted_iota(jnp.int32, value.shape, 0)
    if tap == 0:
        return jnp.where(rows == 0, 0.0, pltpu.roll(value, 1, 0))
    return jnp.where(rows == COLS - 1, 0.0, pltpu.roll(value, COLS - 1, 0))


def step_kernel(
    zl_count, zh_count,
    tower_in, wc_in, wb_in, cls_bias_in, box_bias_in, labels_in, tindex_in, boxes_in,
    *refs,
):
    r_outs, (s_out, tg_out), refs = refs[: len(STREAMS)], refs[len(STREAMS) :][:2], refs[len(STREAMS) + 2 :]
    (
        tower, w, wb, cls_bias, box_bias, labels, tindex, boxes,
        wbs, bias_row, ext, patches, beside, outs, gf, glow, theirs, boxy,
        small_c, small_a, small_b, sz, dpatch, edge_s, edge_r,
        load_sem, ready, across_a, across_b, send, recv, *per_stream,
    ) = refs
    t = lax.axis_index("tile")
    m = lax.axis_index("img")
    tiles = zl_count * RING * 2
    nz = zl_count * zh_count
    c = t % 2
    y = (t // 2) % RING
    x = m // zh_count
    z = (m % zh_count) * zl_count + t // (2 * RING)

    def at(x_, y_, z_, c_):
        return {
            "tile": (z_ % zl_count) * (2 * RING) + y_ * 2 + c_,
            "img": x_ * zh_count + z_ // zl_count,
        }

    a = x + c * (y - x)
    b = y + c * (x - y)

    def ring(a_, b_):
        return at(a_ + c * (b_ - a_), b_ + c * (a_ - b_), z, c)

    sibling = at(x, y, z, 1 - c)
    outer = {"tile": t + 2 * c - 1, "img": m}
    has_outer = jnp.where(c == 0, t > 0, t < tiles - 1)
    links = Links(send, recv)

    barrier = pltpu.get_barrier_semaphore()

    def greet(device):
        pl.semaphore_signal(barrier, inc=1, device_id=device, device_id_type=MESH)

    greet(sibling)
    for near in (flip(a), 3 - a):
        greet(ring(near, b))
    for near in (flip(b), 3 - b):
        greet(ring(a, near))
    beside_z = (at(x, y, (z + 1) % nz, c), at(x, y, (z + nz - 1) % nz, c))
    for device in beside_z:
        greet(device)

    @pl.when(has_outer)
    def _():
        greet(outer)

    loads = [
        pltpu.make_async_copy(src, dst, load_sem.at[k])
        for k, (src, dst) in enumerate((
            (tower_in, tower), (tindex_in, tindex), (boxes_in, boxes), (wb_in, wb),
            (wc_in, w), (cls_bias_in, cls_bias), (box_bias_in, box_bias), (labels_in, labels),
        ))
    ]
    for load in loads:
        load.start()
    def fill(row, place, halves, put):
        value = row.astype(F32)
        for col_tap in range(3):
            piece = shifted(value, col_tap).astype(BF16)
            for here in range(2):
                row_tap = place - here
                if 0 <= row_tap <= 2:
                    for part in range(2):
                        k = (3 * row_tap + col_tap) * DEPTH + part * COLS
                        if k // HALF in halves:
                            put(
                                k // HALF,
                                slice(here * COLS, (here + 1) * COLS),
                                slice(k % HALF, k % HALF + COLS),
                                piece[:, part * COLS : (part + 1) * COLS],
                            )

    def put_own(half, rows, cols, value):
        patches[half, rows, cols] = value

    def put_beside(half, rows, cols, value):
        beside[rows, cols] = value

    wbs[...] = jnp.zeros(wbs.shape, BF16)
    loads[0].wait()
    pl.semaphore_wait(barrier, 1 + 4 + 2 + has_outer.astype(jnp.int32))

    rounds = nz // 2 - 1

    def tell(k):
        if k < rounds:
            for device in beside_z:
                pl.semaphore_signal(ready.at[k], inc=1, device_id=device, device_id_type=MESH)

    def hear(k):
        if k < rounds:
            pl.semaphore_wait(ready.at[k], 2)
            tell(k + 1)

    halo = links.make(tower.at[0, c], ext.at[5 * (1 - c)], outer)

    @pl.when(has_outer)
    def _():
        halo.start()

    @pl.when(jnp.logical_not(has_outer))
    def _():
        ext[5 * c] = jnp.zeros(ext.shape[1:], BF16)

    rows_across = links.push(tower.at[0], ext.at[pl.ds(1 + 2 * c, 2)], sibling)
    tell(0)
    for near in (flip(a), 3 - a):
        pl.semaphore_signal(across_a, inc=1, device_id=ring(near, b), device_id_type=MESH)
    for near in (flip(b), 3 - b):
        pl.semaphore_signal(across_b, inc=1, device_id=ring(a, near), device_id_type=MESH)

    for here in range(2):
        ext[1 + 2 * c + here] = tower[0, here]
        fill(tower[0, here], 1 + here, (0, 1), put_own)

    for load in loads[1:4]:
        load.wait()

    wanted = jnp.concatenate([tindex[0, :, 0, :], tindex[0, :, 1, :]], axis=1)

    def pick(n, found):
        hit = wanted == n
        return tuple(jnp.where(hit, boxes[0, j, n], found[j]) for j in range(4))

    zero = jnp.zeros(wanted.shape, F32)
    corners = lax.fori_loop(0, boxes.shape[2], pick, (zero, zero, zero, zero), unroll=5)
    wbs[0 : 4 * ANCHORS, :] = wb[...]

    nt = (((1,), (1,)), ((), ()))

    def product(lhs, rhs):
        return lax.dot_general(lhs, rhs, nt, preferred_element_type=F32)

    def column(values):
        wide = jnp.broadcast_to(values, (8, values.shape[1]))
        return jnp.transpose(wide)[:, 0:1]

    edge = 3 * DEPTH
    outer_part = (
        (0, slice(0, COLS), slice(0, edge), slice(0, edge)),
        (1, slice(COLS, 2 * COLS), slice(HALF - edge, HALF), slice(WIDTH - edge, WIDTH)),
    )
    for load in loads[4:]:
        load.wait()
    bias_row[0:1, 0:CLS] = cls_bias[...].reshape(1, CLS)
    bias_row[0:1, CLS:OUTS] = box_bias[...].reshape(1, OUTS - CLS)
    bias_row[0:1, OUTS:PAD_OUTS] = jnp.zeros((1, PAD_OUTS - OUTS), F32)
    bias_col = column(bias_row[0:1, :])
    rows_across.wait_recv()
    for half in range(2):

        @pl.when(c == half)
        def _():
            part, positions, cols, _ = outer_part[half]
            patches[part, positions, cols] = jnp.zeros((COLS, edge), BF16)
            fill(ext[2 * half + 3 - 3 * half], 3 - 3 * half, (0, 1), put_own)

    both = ((w, slice(0, CLS)), (wbs, slice(CLS, PAD_OUTS)))
    for lhs, rows in both:
        outs[rows, :] = (
            product(lhs[:, 0:HALF], patches[0])
            + product(lhs[:, HALF:WIDTH], patches[1])
            + bias_col[rows]
        )

    @pl.when(has_outer)
    def _():
        halo.wait_recv()

    outer_across = links.push(ext.at[5 * c], ext.at[5 * c], sibling)
    for half in range(2):

        @pl.when(c == half)
        def _():
            part, positions, cols, weights = outer_part[half]
            fill(ext[5 * half], 3 * half, (0, 1), put_own)
            for lhs, rows in both:
                outs[rows, positions] += product(lhs[:, weights], patches[part, positions, cols])

    hear(0)

    class_ids = lax.broadcasted_iota(jnp.int32, (CLASSES, COLS), 0)

    def focal(anchor, total):
        rows = pl.ds(pl.multiple_of(anchor * CLASSES, CLASSES), CLASSES)
        for here in range(2):
            lanes = slice(here * COLS, (here + 1) * COLS)
            score = outs[rows, lanes]
            label = labels[0, anchor, here : here + 1, :]
            hit = jnp.broadcast_to(label, (CLASSES, COLS)) == class_ids
            counted = (label >= -1).astype(F32)
            side = jnp.where(hit, score, -score)
            small_e = jnp.exp(-jnp.abs(score))
            inverse = 1.0 / (1.0 + small_e)
            log_p = jnp.minimum(side, 0.0) - jnp.log1p(small_e)
            right = side >= 0
            p = jnp.where(right, inverse, small_e * inverse)
            miss = jnp.where(right, small_e * inverse, inverse)
            alpha = jnp.where(hit, FOCAL_ALPHA, FOCAL_ALPHA - 1.0) * counted
            weight = alpha * miss * miss
            grad = weight * (2.0 * p * log_p - miss)
            value = -jnp.abs(weight) * log_p
            gf[rows, lanes] = grad
            glow[rows, lanes] = grad.astype(BF16)
            total = total + jnp.sum(value.reshape(CLASSES // 8, 8, COLS), axis=0)
        return total

    glow_across, glow_arrived = links.group(theirs, sibling)

    def send_grads(start, stop):
        glow_across(glow.at[pl.ds(start, stop - start)], theirs.at[pl.ds(start, stop - start)], sibling)

    focal_sum = jnp.zeros((8, COLS), F32)
    for k in range(3):
        focal_sum = lax.fori_loop(3 * k, 3 * k + 3, focal, focal_sum)
        send_grads(3 * k * CLASSES, 3 * (k + 1) * CLASSES)

    assigned = jnp.concatenate([labels[0, :, 0, :], labels[0, :, 1, :]], axis=1)
    for here in range(2):
        boxy[here] = outs[CLS:PAD_OUTS, here * COLS : (here + 1) * COLS]
    offsets = [
        jnp.concatenate([boxy[here, pl.ds(j, ANCHORS, stride=4), :] for here in range(2)], axis=1)
        for j in range(4)
    ]
    giou, offset_grads, positive = box_terms(offsets, assigned, corners, 2 * t)
    boxy[...] = jnp.zeros(boxy.shape, F32)
    for here in range(2):
        lanes = slice(here * COLS, (here + 1) * COLS)
        for j in range(4):
            boxy[here, pl.ds(j, ANCHORS, stride=4), :] = offset_grads[j][:, lanes]
        gf[CLS:PAD_OUTS, lanes] = boxy[here]
    glow[CLS:PAD_OUTS, :] = gf[CLS:PAD_OUTS, :].astype(BF16)
    send_grads(CLS, PAD_OUTS)

    streams = []
    each = len(per_stream) // len(STREAMS)
    for k, (start, stop) in enumerate(STREAMS):
        streams.append((r_outs[k], start, stop, *per_stream[k * each : (k + 1) * each]))

    def own_part(k):
        _, start, stop, acc, *_ = streams[k]
        part = jnp.dot(glow[...], patches[c, :, start:stop], preferred_element_type=F32)
        acc[...] = part.reshape(acc.shape)

    own_part(0)
    hear(1)
    outer_across.wait_recv()
    for half in range(2):

        @pl.when(c == half)
        def _():
            for place in range(4):
                fill(ext[2 * (1 - half) + place], place, (half,), put_beside)

    glow_arrived()

    def wrap(i):
        return (i + RING) % RING

    far_first = sorted(range(1, nz), key=lambda k: -min(k, nz - k))
    groups = BLOCK // 8
    shared = []

    squares = []

    def stream(
        number, r, start, stop,
        acc, far_s, far_r, own_s, own_r, accb, b_s, b_r, zf, zs, zr, zg,
    ):
        width = stop - start
        if number:
            own_part(number)

        steps = ((flip(a), 3 - a), (3 - a, flip(a)))
        first = []
        for s in range(2):
            near, far = steps[s]
            back = (3 - near, flip(near))[s]
            rows = pl.ds(pl.multiple_of((back * RING + 2 * s) * BLOCK, 2 * BLOCK), 2 * BLOCK)
            part = jnp.dot(theirs[rows, :], beside[:, start:stop], preferred_element_type=F32)
            for j in range(2):
                far_s[s, j] = (acc[back, 2 * s + j] + part[j * BLOCK : (j + 1) * BLOCK]).astype(BF16)
            first.append(links.push(far_s.at[s], far_r.at[s], ring(near, b)))
        part = jnp.dot(theirs[...], beside[:, start:stop], preferred_element_type=F32)
        acc[...] += part.reshape(acc.shape)
        turn, arrived = links.group(own_r, ring(flip(a), b))
        for s in range(2):
            near, far = steps[s]
            for j in range(2):
                own_s[s, j] = acc[near, 2 * s + j].astype(BF16)
            turn(own_s.at[s], own_r.at[s], ring(near, b))
        yield

        for s in range(2):
            near, far = steps[s]
            first[s].wait_recv()
            for j in range(2):
                own_s[2 + s, j] = (acc[far, 2 * s + j] + far_r[s, j].astype(F32)).astype(BF16)
            turn(own_s.at[2 + s], own_r.at[2 + s], ring(far, b))
        yield

        arrived()
        for s in range(2):
            for j in range(2):
                accb[2 * s + j] = (
                    acc[a, 2 * s + j] + own_r[s, j].astype(F32) + own_r[2 + s, j].astype(F32)
                )

        turn, arrived = links.group(b_r, ring(a, wrap(b + 1)))
        for k in (2, 1, 3):
            b_s[k - 1] = accb[wrap(b + k)].astype(BF16)
            turn(b_s.at[k - 1], b_r.at[k - 1], ring(a, wrap(b + k)))
        yield

        per = zf.shape[1] // 8
        zf[...] = jnp.zeros(zf.shape, F32)
        arrived()
        done = accb[b] + b_r[0].astype(F32) + b_r[1].astype(F32) + b_r[2].astype(F32)
        for k in range(width // COLS):
            for g in range(groups):
                n = k * groups + g
                zf[n // per, (n % per) * 8 : (n % per) * 8 + 8, :] = done[
                    g * 8 : g * 8 + 8, k * COLS : (k + 1) * COLS
                ]

        zs[...] = zf[...].astype(BF16)
        turn, arrived = links.group(zr.at[pl.ds(0, nz - 1)], beside_z[0])
        for k in far_first:
            turn(zs.at[(z + k) % nz], zr.at[z], at(x, y, (z + k) % nz, c))
        yield

        arrived()
        total = zf[z]
        for k in range(1, nz):
            total = total + zr[(z + nz - k) % nz].astype(F32)
        zg[z] = total.astype(BF16)
        squares.append(jnp.sum(total * total))
        turn, arrived = links.group(zg.at[pl.ds(0, nz - 1)], beside_z[0])
        for k in far_first:
            turn(zg.at[z], zg.at[z], at(x, y, (z + k) % nz, c))
        yield

        arrived()
        zf[...] = zg[...].astype(F32)
        for k in range(width // COLS):
            pieces = []
            for g in range(groups):
                n = k * groups + g
                pieces.append(zf[n // per, (n % per) * 8 : (n % per) * 8 + 8, :])
            r[c, a, b, :, k * COLS : (k + 1) * COLS] = jnp.concatenate(pieces, axis=0).astype(BF16)

        across, all_across = links.group(r.at[1 - c], sibling, apart=True)
        shared.append(all_across)

        def share(a_, b_):
            across(r.at[c, a_, b_], r.at[c, a_, b_], sibling)

        def along_a(b_):
            block = r.at[c, a, b_]
            turn, arrived = links.group(r.at[c, a, pl.ds(0, 2)], ring(wrap(a + 1), b))
            turn(block, block, ring(wrap(a + 1), b))
            turn(block, block, ring(wrap(a - 1), b))
            return arrived

        block = r.at[c, a, b]
        wide = [along_a(b)]
        turn, arrived = links.group(r.at[c, a, pl.ds(0, 2)], ring(a, wrap(b + 1)))
        for k in (1, 3):
            turn(block, block, ring(a, wrap(b + k)))
        share(a, b)
        yield

        arrived()
        turn, arrived = links.group(r.at[c, a, b], ring(a, wrap(b + 1)))
        for k, rows in ((1, slice(0, 32)), (3, slice(32, BLOCK))):
            block = r.at[c, a, wrap(b - k), rows]
            turn(block, block, ring(a, wrap(b + k)))
        for k in (1, 3):
            wide.append(along_a(wrap(b - k)))
            share(a, wrap(b - k))
        yield

        arrived()
        wide.append(along_a(wrap(b + 2)))
        share(a, wrap(b + 2))
        yield

        order = (b, wrap(b - 1), wrap(b + 1), wrap(b + 2))
        rest = []
        for k, b_ in enumerate(order):
            wide[k]()
            step = -1 if k < 2 else 1
            block = r.at[c, wrap(a + step), b_]
            rest.append(links.push(block, block, ring(wrap(a - step), b)))
            share(wrap(a - 1), b_)
            share(wrap(a + 1), b_)
            yield
        for copy, b_ in zip(rest, order):
            copy.wait_recv()
            share(wrap(a + 2), b_)
            yield

    going = [stream(k, *refs) for k, refs in enumerate(streams)]

    def step(*numbers):
        for k in numbers or range(len(going)):
            next(going[k], None)

    step()
    hear(2)

    tn = (((0,), (0,)), ((), ()))
    dpatch[...] = lax.dot_general(
        glow[0:CLS, :], w[...], tn, preferred_element_type=F32
    ) + lax.dot_general(glow[CLS:PAD_OUTS, :], wbs[...], tn, preferred_element_type=F32)

    def reach(row_tap, here):
        total = None
        for col_tap in range(3):
            k = (3 * row_tap + col_tap) * DEPTH
            piece = shifted(dpatch[here * COLS : (here + 1) * COLS, k : k + DEPTH], 2 - col_tap)
            total = piece if total is None else total + piece
        return total

    edge_s[0] = reach(0, 0)
    edge_s[1] = reach(2, 1)
    edge_out = links.make(edge_s.at[c], edge_r.at[1 - c], outer)
    edge_in = links.push(edge_s.at[1 - c], edge_r.at[c], sibling)

    @pl.when(has_outer)
    def _():
        edge_out.start()

    @pl.when(jnp.logical_not(has_outer))
    def _():
        edge_r[c] = jnp.zeros(edge_r.shape[1:], F32)

    sums = lax.dot_general(
        jnp.ones((8, 2 * COLS), F32), gf[...], nt,
        precision=lax.Precision.HIGHEST, preferred_element_type=F32,
    )
    lane = lax.broadcasted_iota(jnp.int32, (1, COLS), 1)
    mine = jnp.zeros((8, COLS), F32)
    rows8 = lax.broadcasted_iota(jnp.int32, (8, COLS), 0)
    for k in range(PAD_OUTS // COLS):
        mine = jnp.where(rows8 == k, sums[:, k * COLS : (k + 1) * COLS], mine)
    def add_up(stage):
        slots, here, devices = (
            (small_c, c, (sibling,)),
            (small_a, a, tuple(ring(wrap(a + k), b) for k in (2, 1, 3))),
            (small_b, b, tuple(ring(a, wrap(b + k)) for k in (2, 1, 3))),
            (sz, z, tuple(at(x, y, (z + k) % nz, c) for k in far_first)),
        )[stage]
        if stage == 0:
            total = mine
            scalars = (jnp.sum(focal_sum), jnp.sum(giou), jnp.sum(positive), sum(squares))
            for n, value in enumerate(scalars):
                total = jnp.where((rows8 == 6) & (lane == n), value, total)
        else:
            total = added()
        slots[here] = total
        count = len(devices)
        turn, arrived = links.group(slots.at[pl.ds(0, count)], devices[0])
        for device in devices:
            turn(slots.at[here], slots.at[here], device)

        def result():
            arrived()
            total = slots[0]
            for k in range(1, count + 1):
                total = total + slots[k]
            return total

        return result

    step()

    tg_own = (reach(1, 0) + reach(0, 1), reach(2, 0) + reach(1, 1))
    edge_in.wait_recv()

    @pl.when(has_outer)
    def _():
        edge_out.wait_recv()

    for here in range(2):
        tg_out[0, here] = (tg_own[here] + edge_r[here]).astype(BF16)

    pl.semaphore_wait(across_a, 2)
    pl.semaphore_wait(across_b, 2)
    step()
    step()
    step()
    added = add_up(0)
    step()
    added = add_up(1)
    step()
    added = add_up(2)
    step()
    step()
    added = add_up(3)
    for _ in range(2 * RING):
        step()
    s_out[...] = added()
    for all_across in shared:
        all_across()

    links.drain()

    @pl.when(has_outer)
    def _():
        halo.wait_send()
        edge_out.wait_send()


def scale_kernel(*refs):
    rs, refs = refs[: len(STREAMS)], refs[len(STREAMS) :]
    s, tg, cls_out, box_out, loss_out, cls_bias_out, box_bias_out, tg_out, *refs = refs
    stage, box_stage, loss, cls_bias, box_bias, sem, rest = refs
    others = [
        pltpu.make_async_copy(src, dst, rest.at[k])
        for k, (src, dst) in enumerate((
            (tg, tg_out), (box_stage, box_out), (loss, loss_out),
            (cls_bias, cls_bias_out), (box_bias, box_bias_out),
        ))
    ]
    others[0].start()
    rows8 = lax.broadcasted_iota(jnp.int32, (8, COLS), 0)
    bias = jnp.where(rows8 < PAD_OUTS // COLS, s[...], 0.0)
    total = s[6:7, 3:4] + jnp.sum(bias * bias, keepdims=True)
    scale = lax.rsqrt(total / (OUTS * (WIDTH + 1)) + NORM_EPS)

    def scaled(k, put):
        for h in range(2):
            for r, (start, stop) in zip(rs, STREAMS):
                put(
                    slice(h * HALF + start, h * HALF + stop),
                    r[h, k // RING, k % RING].astype(F32) * scale,
                )

    def chunk(k, carry):
        rows = pl.ds(pl.multiple_of(k * BLOCK, BLOCK), BLOCK)

        def put(cols, value):
            stage[rows, cols] = value

        scaled(k, put)
        pltpu.make_async_copy(stage.at[rows], cls_out.at[rows], sem).start()
        return carry

    def put_box(cols, value):
        box_stage[:, cols] = value[0 : OUTS - CLS]

    lax.fori_loop(0, CLS // BLOCK, chunk, 0)
    scaled(CLS // BLOCK, put_box)
    bias = bias * scale
    cls_bias[...] = bias
    at_row, at_lane = CLS // COLS, CLS % COLS
    box_bias[...] = pltpu.roll(bias, COLS - at_lane, 1)[at_row : at_row + 1, 0 : OUTS - CLS]
    loss[...] = (s[6:7, 0:1] + s[6:7, 1:2]) / s[6:7, 2:3]
    for copy in others[1:]:
        copy.start()
    pltpu.make_async_copy(stage, cls_out, sem).wait()
    for copy in others:
        copy.wait()


def per_device(
    zl_count, zh_count, tower, cls_weight, cls_bias, box_weight, box_bias, labels, target_index, boxes
):
    nz = zl_count * zh_count
    vmem = pl.BlockSpec(memory_space=pltpu.VMEM)
    hbm = pl.BlockSpec(memory_space=pl.ANY)

    def buf(*shape, dtype=BF16):
        return pltpu.VMEM(shape, dtype)

    per_stream = []
    for start, stop in STREAMS:
        width = stop - start
        per = -(-(BLOCK // 8 * (width // COLS)) // nz) * 8
        per_stream += [
            buf(RING, RING, BLOCK, width, dtype=F32),
            buf(2, 2, BLOCK, width),
            buf(2, 2, BLOCK, width),
            buf(4, 2, BLOCK, width),
            buf(4, 2, BLOCK, width),
            buf(RING, BLOCK, width, dtype=F32),
        ]
        per_stream += [buf(RING - 1, BLOCK, width)] * 2
        per_stream += [buf(nz, per, COLS, dtype=F32)] + [buf(nz, per, COLS)] * 3

    *rs, s, tower_grad = pl.pallas_call(
        functools.partial(step_kernel, zl_count, zh_count),
        out_shape=(
            *(buf(2, RING, RING, BLOCK, stop - start) for start, stop in STREAMS),
            buf(8, COLS, dtype=F32),
            buf(*tower.shape),
        ),
        in_specs=[hbm] * 8,
        out_specs=(vmem,) * (len(STREAMS) + 2),
        scratch_shapes=[
            buf(*tower.shape),
            buf(CLS, WIDTH),
            buf(*box_weight.shape),
            buf(*cls_bias.shape, dtype=F32),
            buf(*box_bias.shape, dtype=F32),
            buf(*labels.shape, dtype=jnp.int32),
            buf(*target_index.shape, dtype=jnp.int32),
            pltpu.SMEM(boxes.shape, F32),
            buf(PAD_OUTS - CLS, WIDTH),
            buf(8, PAD_OUTS, dtype=F32),
            buf(6, COLS, DEPTH),
            buf(2, 2 * COLS, HALF),
            buf(2 * COLS, HALF),
            buf(PAD_OUTS, 2 * COLS, dtype=F32),
            buf(PAD_OUTS, 2 * COLS, dtype=F32),
            buf(PAD_OUTS, 2 * COLS),
            buf(PAD_OUTS, 2 * COLS),
            buf(2, PAD_OUTS - CLS, COLS, dtype=F32),
            buf(2, 8, COLS, dtype=F32),
            buf(RING, 8, COLS, dtype=F32),
            buf(RING, 8, COLS, dtype=F32),
            buf(nz, 8, COLS, dtype=F32),
            buf(2 * COLS, WIDTH, dtype=F32),
            buf(2, COLS, DEPTH, dtype=F32),
            buf(2, COLS, DEPTH, dtype=F32),
            pltpu.SemaphoreType.DMA((8,)),
            pltpu.SemaphoreType.REGULAR((max(nz // 2 - 1, 1),)),
            pltpu.SemaphoreType.REGULAR,
            pltpu.SemaphoreType.REGULAR,
            pltpu.SemaphoreType.DMA((IN_FLIGHT + APART,)),
            pltpu.SemaphoreType.DMA((RECEIVES,)),
            *per_stream,
        ],
        compiler_params=pltpu.CompilerParams(
            collective_id=0, has_side_effects=True, vmem_limit_bytes=56 * 2**20
        ),
        name="step",
    )(tower, cls_weight, box_weight, cls_bias, box_bias, labels, target_index, boxes)

    cls_grad, box_grad, loss, cls_bias_grad, box_bias_grad, tower_grad = pl.pallas_call(
        scale_kernel,
        out_shape=(
            jax.ShapeDtypeStruct((CLS, WIDTH), F32),
            jax.ShapeDtypeStruct((OUTS - CLS, WIDTH), F32),
            jax.ShapeDtypeStruct((1, 1), F32),
            jax.ShapeDtypeStruct((8, COLS), F32),
            jax.ShapeDtypeStruct((1, OUTS - CLS), F32),
            jax.ShapeDtypeStruct(tower.shape, BF16),
        ),
        in_specs=[vmem] * (len(STREAMS) + 2),
        out_specs=(hbm,) * 6,
        scratch_shapes=[
            buf(CLS, WIDTH, dtype=F32),
            buf(OUTS - CLS, WIDTH, dtype=F32),
            buf(1, 1, dtype=F32),
            buf(8, COLS, dtype=F32),
            buf(1, OUTS - CLS, dtype=F32),
            pltpu.SemaphoreType.DMA,
            pltpu.SemaphoreType.DMA((5,)),
        ],
        compiler_params=pltpu.CompilerParams(vmem_limit_bytes=40 * 2**20),
        name="scale",
    )(*rs, s, tower_grad)
    return (
        loss.reshape(()),
        cls_grad,
        cls_bias_grad.reshape(-1)[:CLS],
        box_grad,
        box_bias_grad.reshape(-1),
        tower_grad,
    )


def solution(mesh):
    zl_count = mesh.shape["tile"] // (2 * RING)
    zh_count = mesh.shape["img"] // RING
    placed = (
        P("img", "tile", None, None),
        P(),
        P(),
        P(),
        P(),
        P("img", None, "tile", None),
        P("img", None, "tile", None),
        P("img", None, None),
    )
    return jax.shard_map(
        functools.partial(per_device, zl_count, zh_count),
        mesh=mesh,
        in_specs=placed,
        out_specs=(P(), P(), P(), P(), P(), P("img", "tile", None, None)),
        check_vma=False,
    )
```
